256 devices in a mesh: gz: 8 (over z), xy: 32 (over x, y, core).
Axes of the slice: x: 4, y: 4, z: 8, core: 2. Of those that a mesh axis runs over, the one named last changes fastest.
Arguments:
- volume: float32 [128, 1536, 128], P('gz', 'xy'), may hold values from 0 to 1
- measured: float32 [2, 5, 160, 1536], P(None, None, 'gz', 'xy'), may hold values from 0 to 1
- view_order: int32 [48], replicated, may hold values from 0 to 47, each once
Outputs:
- volume_out: float32 [128, 1536, 128], P('gz', 'xy')
- residual: float32 [5, 160, 1536], P(None, 'gz', 'xy')
The draws below stay inside these ranges and needn't reach their ends.
Inputs may be any that keep to these rules, and one draw needn't show every extreme that they name: `view_order`: A permutation of the numbers 0 to 47.
All inputs are finite; a program needn't handle non-finite values.
Results may differ from the reference program's by a relative error of at most 0.00078.
Values may be sent and summed in bfloat16 or wider, within the bound.
A program may use at most 64 MiB of HBM per device.

```python
import math
import jax
import jax.numpy as jnp
from jax import lax

X_DEV = 48
NY = 128
VIEWS = 5
SUBSETS = 2
ANGLES = 48
NX = 1536
NZ = 128
DR = 160
DC = 1536
N_XY = 32


def levels(own_key, extent, shards, smallest, top_value):
    def one(dim, parts):
        heights = jax.random.uniform(jax.random.fold_in(jax.random.fold_in(own_key, 6), dim), (parts,), jnp.float32, smallest / len(shards), top_value / len(shards))
        return jnp.repeat(jnp.exp(heights), extent[dim] // parts).reshape((-1,) + (1,) * (len(extent) - dim - 1))

    level = one(*shards[0])
    for cut in shards[1:]:
        level = level * one(*cut)
    return level


def setup_inputs(seed: int = 0) -> dict:
    seeds = jax.random.split(jax.random.key(seed), 4)
    return {
        "volume": jnp.clip(1.0 * jax.random.uniform(seeds[0], (NZ, NX, NY), jnp.float32) ** levels(seeds[0], (NZ, NX, NY), ((0, 8), (1, 32)), -0.2, 0.2), 0.0, 1.0),
        "measured": jnp.clip(1.0 * jax.random.uniform(seeds[1], (SUBSETS, VIEWS, DR, DC), jnp.float32) ** levels(seeds[1], (SUBSETS, VIEWS, DR, DC), ((2, 8), (3, 32)), -0.2, 0.2), 0.0, 1.0),
        "view_order": jax.random.permutation(seeds[2], ANGLES).astype(jnp.int32),
    }


def column_weights(view_angle, x_first, x_count, nx_all, ny_all, dc_all):
    x_coords = jnp.asarray(x_first).astype(jnp.float32) + jnp.arange(x_count, dtype=jnp.float32) - (nx_all - 1) / 2.0
    y_coords = jnp.arange(ny_all, dtype=jnp.float32) - (ny_all - 1) / 2.0
    cosine = jnp.cos(view_angle)
    sine_value = jnp.sin(view_angle)
    along_axis = x_coords[:, None] * cosine + y_coords[None, :] * sine_value
    depth_axis = y_coords[None, :] * cosine - x_coords[:, None] * sine_value
    source = 2.0 * nx_all
    position = (dc_all - 1) / 2.0 + 0.9 * (dc_all / nx_all) * along_axis * source / (source + depth_axis)
    position = position.reshape(x_count // 8, 8, ny_all // 16, 16).transpose(0, 2, 1, 3).reshape(-1, 128)
    lowest = jnp.min(position, axis=1)
    first_block = jnp.clip(jnp.floor(lowest / 64.0), 0, dc_all // 64 - 2).astype(jnp.int32)
    columns = (first_block * 64)[:, None] + jnp.arange(128, dtype=jnp.int32)[None, :]
    weights = jnp.maximum(0.0, 1.0 - jnp.abs(position[:, :, None] - columns[:, None, :].astype(position.dtype)))
    return weights.astype(jnp.bfloat16), first_block


def place_blocks(values, first_block, block_count):
    block_ids = jnp.arange(block_count, dtype=jnp.int32)
    low_onehot = (first_block[:, None] == block_ids[None, :]).astype(values.dtype)
    high_onehot = (first_block[:, None] + 1 == block_ids[None, :]).astype(values.dtype)
    result = jnp.einsum('sb,skc->kbc', low_onehot, values[:, :, :64], precision=lax.Precision.HIGHEST)
    result = result + jnp.einsum('sb,skc->kbc', high_onehot, values[:, :, 64:], precision=lax.Precision.HIGHEST)
    return result.reshape(values.shape[1], block_count * 64)


def row_weights(row_ids, slice_ids, dr_all, nz_all):
    position = (dr_all - 1) / 2.0 + 0.96 * (dr_all / nz_all) * (slice_ids.astype(jnp.float32) - (nz_all - 1) / 2.0)
    inside = ((row_ids >= 0) & (row_ids < dr_all)).astype(jnp.float32)
    hat = jnp.maximum(0.0, 1.0 - jnp.abs(position[None, :] - row_ids[:, None].astype(jnp.float32)) / 2.0)
    return hat * inside[:, None]


def reference(volume, measured, view_order):
    block_count = DC // 64
    tiled = volume.reshape(NZ, N_XY, X_DEV // 8, 8, NY // 16, 16).transpose(1, 2, 4, 0, 3, 5).reshape(N_XY, -1, NZ, 128)
    axial_weights = row_weights(jnp.arange(DR, dtype=jnp.int32), jnp.arange(NZ, dtype=jnp.int32), DR, NZ)
    slice_total = jnp.sum(axial_weights, axis=0)
    ray_rows = jnp.sum(axial_weights, axis=1)
    strip_ids = jnp.arange(N_XY, dtype=jnp.int32)
    residual = jnp.zeros((VIEWS, DR, DC), jnp.float32)
    for subset in range(SUBSETS):
        chosen = view_order[subset * VIEWS:(subset + 1) * VIEWS]
        angles = 2.0 * math.pi * chosen.astype(jnp.float32) / ANGLES

        def forward(totals, item):
            tiles, strip_index = item
            placed_sum, column_sum = totals
            tiles_rounded = lax.optimization_barrier(tiles.astype(jnp.bfloat16)).astype(jnp.float32)
            new_placed = []
            new_columns = []
            for view_index in range(VIEWS):
                weights, first_block = column_weights(angles[view_index], strip_index * X_DEV, X_DEV, NX, NY, DC)
                weights = lax.optimization_barrier(weights).astype(jnp.float32)
                column_sums = jnp.einsum('szv,svc->szc', tiles_rounded, weights, precision=lax.Precision.HIGHEST)
                new_placed.append(place_blocks(column_sums, first_block, block_count))
                new_columns.append(place_blocks(jnp.sum(weights, axis=1)[:, None, :], first_block, block_count)[0])
            return (placed_sum + jnp.stack(new_placed), column_sum + jnp.stack(new_columns)), None

        start = (jnp.zeros((VIEWS, NZ, DC), jnp.float32), jnp.zeros((VIEWS, DC), jnp.float32))
        (placed, column_total), leftover = lax.scan(forward, start, (tiled, strip_ids))
        projection = jnp.einsum('rz,vzc->vrc', axial_weights, placed, precision=lax.Precision.HIGHEST)
        ray_sums = ray_rows[None, :, None] * column_total[:, None, :]
        residual = measured[subset] - projection / jnp.maximum(ray_sums, 1.0)
        rounded = lax.optimization_barrier(residual.astype(jnp.bfloat16)).astype(jnp.float32)
        smeared = jnp.einsum('rz,vrc->vzc', axial_weights, rounded, precision=lax.Precision.HIGHEST).astype(jnp.bfloat16)
        smeared = lax.optimization_barrier(smeared).astype(jnp.float32)

        def backward(item):
            tiles, strip_index = item
            back_total = jnp.zeros(tiles.shape, jnp.float32)
            norm_total = jnp.zeros(tiles.shape, jnp.float32)
            for view_index in range(VIEWS):
                weights, first_block = column_weights(angles[view_index], strip_index * X_DEV, X_DEV, NX, NY, DC)
                weights = lax.optimization_barrier(weights).astype(jnp.float32)
                pieces = smeared[view_index].reshape(NZ, block_count, 64)
                window = jnp.concatenate((jnp.take(pieces, first_block, axis=1), jnp.take(pieces, first_block + 1, axis=1)), axis=2)
                back_total = back_total + jnp.einsum('zsc,svc->szv', window, weights, precision=lax.Precision.HIGHEST)
                norm_total = norm_total + slice_total[None, :, None] * jnp.sum(weights, axis=2)[:, None, :]
            return tiles + back_total / jnp.maximum(norm_total, 1.0)

        tiled = lax.map(backward, (tiled, strip_ids))
    volume_out = tiled.reshape(N_XY, X_DEV // 8, NY // 16, NZ, 8, 16).transpose(3, 0, 1, 4, 2, 5).reshape(NZ, NX, NY)
    return volume_out, residual
```

```python
import functools
import math

import jax
import jax.numpy as jnp
from jax import lax
from jax.experimental import pallas as pl
from jax.experimental.pallas import tpu as pltpu
from jax.sharding import PartitionSpec as P

Z_DEV = 16
X_DEV = 48
COLS_DEV = 48
NY = 128
VIEWS = 5
SUBSETS = 2
ANGLES = 48
ROWS_DEV = 20
HALF = X_DEV // 2
WIN = 48
GROUPS = 5
OWNERS = VIEWS * GROUPS
MESH = pl.DeviceIdType.MESH
HIGHEST = lax.Precision.HIGHEST
F32 = jnp.float32
BF16 = jnp.bfloat16


def iota(shape, dim):
    return lax.broadcasted_iota(jnp.int32, shape, dim)


def kernel(
    gz, xy, view_ref, vol_ref, meas_ref, out_ref, resid_ref,
    it, up, ws, shift, trig, weights, data, window, ones_window,
    send_m, recv_m, meas_rows, send_a, recv_a, send_t, recv_t,
    starts, total, total_t, res, send_c, recv_c, send_d, recv_d, turned,
    sem_vol, sem_ms, sem_mr, sem_as, sem_ar, sem_ah, sem_ts, sem_tr, sem_cs, sem_cr, sem_ch, sem_ds, sem_dr,
):
    g = lax.axis_index("gz")
    j = lax.axis_index("xy")
    nx_all, ny_all, dc_all = X_DEV * xy, NY, COLS_DEV * xy
    dr_all, nz_all = ROWS_DEV * gz, Z_DEV * gz
    owner = j < OWNERS
    own_view = lax.rem(lax.div(j, GROUPS), VIEWS)
    own_group = lax.rem(j, GROUPS)
    first_group = jnp.logical_and(owner, own_group == 0)
    last_group = jnp.logical_and(owner, own_group == GROUPS - 1)
    below, above = g > 0, g < gz - 1

    vol_copy = pltpu.make_async_copy(vol_ref, it, sem_vol)
    vol_copy.start()

    barrier = pltpu.get_barrier_semaphore()

    def greet(plane, device):
        pl.semaphore_signal(barrier, inc=1, device_id=(plane, device), device_id_type=MESH)

    def greet_plane(i, carry):
        @pl.when(i != j)
        def _():
            greet(g, i)

        @pl.when(jnp.logical_and(below, jnp.logical_or(first_group, jnp.logical_and(i < OWNERS, lax.rem(i, GROUPS) == GROUPS - 1))))
        def _():
            greet(g - 1, i)

        @pl.when(jnp.logical_and(above, jnp.logical_or(last_group, jnp.logical_and(i < OWNERS, lax.rem(i, GROUPS) == 0))))
        def _():
            greet(g + 1, i)

        return carry

    lax.fori_loop(0, xy, greet_plane, 0)
    greeted = (
        xy - 1
        + jnp.where(below, jnp.where(first_group, xy, VIEWS), 0)
        + jnp.where(above, jnp.where(last_group, xy, VIEWS), 0)
    )

    lane = iota((8, 128), 1)
    sub = iota((8, 128), 0)
    lane_f = lane.astype(F32)
    sub_f = sub.astype(F32)
    band = lane // 16
    source = 2.0 * nx_all
    scale = 0.9 * (dc_all / nx_all)
    middle = (dc_all - 1) / 2.0
    x_first = (j * X_DEV).astype(F32)

    def project(x, y, cosine, sine):
        along = x * cosine + y * sine
        depth = y * cosine - x * sine
        return middle + scale * along * source / (source + depth)

    def hat(row, slice_id):
        position = (dr_all - 1) / 2.0 + 0.96 * (dr_all / nz_all) * (slice_id - (nz_all - 1) / 2.0)
        return jnp.maximum(0.0, 1.0 - jnp.abs(position - row) / 2.0)

    def rounded(x):
        return x.astype(BF16).astype(F32)

    def geometry(s):
        for v in range(VIEWS):
            number = jnp.full((8, 128), view_ref[s * VIEWS + v], jnp.int32).astype(F32)
            angle = 2.0 * math.pi * number / ANGLES
            cosine, sine = jnp.cos(angle), jnp.sin(angle)
            trig[s, v, 0] = cosine
            trig[s, v, 1] = sine
            y_low = (band * 16).astype(F32) - (ny_all - 1) / 2.0
            base = []
            for h in range(2):
                x_low = (x_first + HALF * h) - (nx_all - 1) / 2.0
                corners = [
                    project(x, y, cosine, sine)
                    for x in (x_low, x_low + (HALF - 1))
                    for y in (y_low, y_low + 15.0)
                ]
                lowest = jnp.minimum(jnp.minimum(corners[0], corners[1]), jnp.minimum(corners[2], corners[3]))
                start = jnp.floor((lowest - 0.03125) * 0.125) * 8.0
                base.append(start)
                shift[s, v, h] = (start - 256.0 * jnp.floor(start * (1.0 / 256.0))).astype(jnp.int32)
            for block in range(X_DEV // 8):
                x = (x_first + (8.0 * block + sub_f)) - (nx_all - 1) / 2.0
                y = lane_f - (ny_all - 1) / 2.0
                u = project(x, y, cosine, sine)
                up[s, v, 8 * block : 8 * block + 8, :] = u - base[block // (HALF // 8)]
                low = jnp.floor(u)
                both = rounded(jnp.maximum(0.0, 1.0 - jnp.abs(u - low))) + rounded(
                    jnp.maximum(0.0, 1.0 - jnp.abs(u - (low + 1.0)))
                )
                rows = slice(8 * block, 8 * block + 8)
                ws[s, rows, :] = both if v == 0 else ws[s, rows, :] + both

    window_ids = iota((WIN, 128), 0).astype(F32)

    def make_weights(s):
        def one(x, carry):
            columns = pl.ds(pl.multiple_of(x * 128, 128), 128)
            for h in range(2):
                for v in range(VIEWS):
                    u = up[s, v, pl.ds(HALF * h + x, 1), :]
                    w = jnp.maximum(0.0, 1.0 - jnp.abs(u - window_ids))
                    weights[2 * s + h, v * WIN : (v + 1) * WIN, columns] = w.astype(BF16)
            return carry

        lax.fori_loop(0, HALF, one, 0)

    band_masks = [(iota((16, 128), 1) // 16 == q).astype(F32).astype(BF16) for q in range(8)]

    def spread(values, h, x):
        columns = pl.ds(pl.multiple_of(x * 128, 128), 128)
        values = values.astype(BF16)
        for q in range(8):
            data[h, 16 * q : 16 * q + 16, columns] = values * band_masks[q]

    row_local = (iota((56, 128), 0) // 8) * 4 + iota((56, 128), 0) % 4 - 4
    row_all = g * ROWS_DEV + row_local
    inside = jnp.logical_and(row_all >= 0, row_all < dr_all)
    slice_all = (g * Z_DEV + iota((56, 128), 1) % 16).astype(F32)
    row_hat = jnp.where(inside, hat(row_all.astype(F32), slice_all), 0.0)
    in_low = iota((56, 128), 0) % 8 < 4
    hat_low = jnp.where(in_low, row_hat, 0.0)
    hat_high = jnp.where(in_low, 0.0, row_hat)

    slices = (g * Z_DEV + iota((16, 128), 0)).astype(F32)
    slice_total = jnp.zeros((16, 1), F32)
    for part in range(-(-dr_all // 128)):
        rows = 128 * part + iota((16, 128), 1)
        weight = jnp.where(rows < dr_all, hat(rows.astype(F32), slices), 0.0)
        slice_total = slice_total + jnp.sum(weight, axis=1, keepdims=True)
    slice_total = jnp.broadcast_to(slice_total, (16, 128))
    own_row = (g * ROWS_DEV + own_group * 4 + sub % 4).astype(F32)
    ray_row = jnp.zeros((8, 1), F32)
    for part in range(-(-nz_all // 128)):
        ids = 128 * part + lane
        weight = jnp.where(ids < nz_all, hat(own_row, ids.astype(F32)), 0.0)
        ray_row = ray_row + jnp.sum(weight, axis=1, keepdims=True)
    ray_row = jnp.broadcast_to(ray_row, (8, 128))
    column_ids = [(256 * m + 128 * (sub // 4) + lane).astype(F32) for m in range(dc_all // 256)]

    def to_owners(src, dst, send_sem, recv_sem):
        def one(o, carry):
            @pl.when(o != j)
            def _():
                pltpu.make_async_remote_copy(
                    src_ref=src(o), dst_ref=dst, send_sem=send_sem, recv_sem=recv_sem,
                    device_id=(g, o), device_id_type=MESH,
                ).start()

            @pl.when(o == j)
            def _():
                pltpu.make_async_copy(src(o), dst, recv_sem).start()

            return carry

        lax.fori_loop(0, OWNERS, one, 0)

    def sent_to_owners(ref, sem):
        @pl.when(owner)
        def _():
            pltpu.make_async_copy(ref.at[0 : OWNERS - 1], ref.at[0 : OWNERS - 1], sem).wait()

        @pl.when(jnp.logical_not(owner))
        def _():
            pltpu.make_async_copy(ref.at[0:OWNERS], ref.at[0:OWNERS], sem).wait()

    def arrived(ref, sem):
        pltpu.make_async_copy(ref, ref, sem).wait()

    geometry(0)

    for v in range(VIEWS):
        for k in range(GROUPS):
            for s in range(SUBSETS):
                send_m[v * GROUPS + k, 4 * s : 4 * s + 4, 0:COLS_DEV] = meas_ref[s, v, 4 * k : 4 * k + 4, :]
    turn = lax.rem(j * COLS_DEV, 128)
    for o in range(OWNERS):
        send_m[o] = pltpu.roll(send_m[o], turn, 1)

    make_weights(0)

    def fill_ones(x, carry):
        columns = pl.ds(pl.multiple_of(x * 128, 128), 128)
        for h in range(2):
            for q in range(8):
                first = iota((16, 128), 0) == 0
                row = jnp.where(jnp.logical_and(first, iota((16, 128), 1) // 16 == q), 1.0, 0.0)
                data[h, 128 + 16 * q : 128 + 16 * q + 16, columns] = row.astype(BF16)
        return carry

    lax.fori_loop(0, HALF, fill_ones, 0)
    vol_copy.wait()

    def fill_data(x, carry):
        for h in range(2):
            spread(it[pl.ds(HALF * h + x, 16, stride=X_DEV), :], h, x)
        return carry

    lax.fori_loop(0, HALF, fill_data, 0)

    pl.semaphore_wait(barrier, greeted)
    to_owners(lambda o: send_m.at[o], recv_m.at[j], sem_ms, sem_mr)

    def forward(s):
        for h in range(2):
            sums = lax.dot_general(
                weights[2 * s + h], data[h], (((1,), (1,)), ((), ())), preferred_element_type=F32
            )
            for v in range(VIEWS):
                offset = shift[s, v, h]
                for part, target in ((0, window), (1, ones_window)):
                    rows = [
                        sums[v * WIN + 8 * i : v * WIN + 8 * i + 8, 128 * part : 128 * part + 128]
                        for i in range(WIN // 8)
                    ] + [None] * (32 - WIN // 8)
                    for bit in (8, 16, 32, 64, 128):
                        moved = (offset & bit) != 0
                        step = bit // 8
                        new = []
                        for i in range(32):
                            old, other = rows[i], rows[(i - step) % 32]
                            if old is None and other is None:
                                new.append(None)
                            elif old is None:
                                new.append(jnp.where(moved, other, 0.0))
                            elif other is None:
                                new.append(jnp.where(moved, 0.0, old))
                            else:
                                new.append(jnp.where(moved, other, old))
                        rows = new
                    for i in range(32):
                        at = slice(256 * v + 8 * i, 256 * v + 8 * i + 8)
                        target[at, :] = rows[i] if h == 0 else target[at, :] + rows[i]
        for v in range(VIEWS):
            totals = lax.dot_general(
                jnp.ones((8, 128), F32), ones_window[256 * v : 256 * v + 256, :],
                (((1,), (1,)), ((), ())), precision=HIGHEST, preferred_element_type=F32,
            )
            message = jnp.where(sub < 4, totals[:, 0:128], totals[:, 128:256])
            low = lax.dot_general(
                hat_low, window[256 * v : 256 * v + 128, :],
                (((1,), (1,)), ((), ())), precision=HIGHEST, preferred_element_type=F32,
            )
            high = lax.dot_general(
                hat_high, window[256 * v + 128 : 256 * v + 256, :],
                (((1,), (1,)), ((), ())), precision=HIGHEST, preferred_element_type=F32,
            )
            rows = low + high
            send_t[s, v] = message
            for k in range(GROUPS + 2):
                send_a[s, k, v] = rows[8 * k : 8 * k + 8, :]
        to_owners(
            lambda o: send_a.at[s, 1 + lax.rem(o, GROUPS), lax.div(o, GROUPS)],
            recv_a.at[s, 0, j], sem_as.at[s], sem_ar.at[s],
        )
        to_owners(lambda o: send_t.at[s, lax.div(o, GROUPS)], recv_t.at[s, j], sem_ts.at[s], sem_tr.at[s])

        def beside(v, carry):
            for there, plane, slot, device in (
                (below, g - 1, 0, GROUPS * v + GROUPS - 1),
                (above, g + 1, GROUPS + 1, GROUPS * v),
            ):
                @pl.when(there)
                def _():
                    pltpu.make_async_remote_copy(
                        src_ref=send_a.at[s, slot, v], dst_ref=recv_a.at[s, 1, j],
                        send_sem=sem_as.at[2 + s], recv_sem=sem_ah.at[s],
                        device_id=(plane, device), device_id_type=MESH,
                    ).start()

            return carry

        lax.fori_loop(0, VIEWS, beside, 0)

    has_beside = jnp.logical_or(jnp.logical_and(first_group, below), jnp.logical_and(last_group, above))

    def prepare_owner():
        arrived(recv_m, sem_mr)
        for block in range(dc_all // 128):
            first, last = 128 * block, 128 * block + 128
            value = jnp.zeros((8, 128), F32)
            for i in range(first // COLS_DEV, min(xy, -(-last // COLS_DEV))):
                low, high = max(COLS_DEV * i, first) - first, min(COLS_DEV * (i + 1), last) - first
                value = jnp.where(jnp.logical_and(lane >= low, lane < high), recv_m[i], value)
            at = 4 * (block % 2)
            for s in range(SUBSETS):
                meas_rows[s, block // 2, at : at + 4, :] = value[4 * s : 4 * s + 4, :]

    def window_starts(s):
        cosine, sine = trig[s, own_view, 0], trig[s, own_view, 1]

        def one(i, carry):
            x = jnp.full((8, 128), i * X_DEV, jnp.int32).astype(F32) + ((X_DEV - 1) / 2.0 - (nx_all - 1) / 2.0)
            starts[i] = jnp.floor(project(x, 0.0, cosine, sine)) - 128.0
            return carry

        lax.fori_loop(0, xy, one, 0)

    blocks = dc_all // 256

    def owner_work(s):
        arrived(recv_a.at[s, 0], sem_ar.at[s])
        arrived(recv_t.at[s], sem_tr.at[s])
        zero = tuple(jnp.zeros((8, 128), F32) for _ in range(2 * blocks))

        def add(i, sums):
            start = starts[i]
            message, column = recv_a[s, 0, i], recv_t[s, i]
            new = list(sums)
            for m in range(blocks):
                away = column_ids[m] - start
                hit = jnp.logical_and(away >= 0.0, away < 256.0)
                new[m] = new[m] + jnp.where(hit, message, 0.0)
                new[blocks + m] = new[blocks + m] + jnp.where(hit, column, 0.0)
            return tuple(new)

        sums = lax.fori_loop(0, xy, add, zero)
        for m in range(blocks):
            total[m] = sums[m]
            total_t[m] = sums[blocks + m]

        @pl.when(has_beside)
        def _():
            arrived(recv_a.at[s, 1], sem_ah.at[s])

            def add_beside(i, sums):
                start = starts[i]
                message = recv_a[s, 1, i]
                new = []
                for m in range(blocks):
                    away = column_ids[m] - start
                    hit = jnp.logical_and(away >= 0.0, away < 256.0)
                    new.append(sums[m] + jnp.where(hit, message, 0.0))
                return tuple(new)

            sums = lax.fori_loop(0, xy, add_beside, zero[:blocks])
            for m in range(blocks):
                total[m] = total[m] + sums[m]

        residuals = []
        for m in range(blocks):
            residual = meas_rows[s, m] - total[m] / jnp.maximum(ray_row * total_t[m], 1.0)
            res[m] = residual
            residuals.append(rounded(residual))

        def give(i, carry):
            start = starts[i]
            message = residuals[blocks - 1]
            for m in range(blocks - 2, -1, -1):
                message = jnp.where(column_ids[m] >= start, residuals[m], message)
            send_c[s, i] = message
            return carry

        lax.fori_loop(0, xy, give, 0)

        def send(i, carry):
            slot = recv_c.at[s, 1 + own_group, own_view]

            @pl.when(i != j)
            def _():
                pltpu.make_async_remote_copy(
                    src_ref=send_c.at[s, i], dst_ref=slot, send_sem=sem_cs.at[s], recv_sem=sem_cr.at[s],
                    device_id=(g, i), device_id_type=MESH,
                ).start()

            @pl.when(i == j)
            def _():
                pltpu.make_async_copy(send_c.at[s, i], slot, sem_cr.at[s]).start()

            @pl.when(jnp.logical_and(first_group, below))
            def _():
                pltpu.make_async_remote_copy(
                    src_ref=send_c.at[s, i], dst_ref=recv_c.at[s, GROUPS + 1, own_view],
                    send_sem=sem_cs.at[2 + s], recv_sem=sem_ch.at[s, 1],
                    device_id=(g - 1, i), device_id_type=MESH,
                ).start()

            @pl.when(jnp.logical_and(last_group, above))
            def _():
                pltpu.make_async_remote_copy(
                    src_ref=send_c.at[s, i], dst_ref=recv_c.at[s, 0, own_view],
                    send_sem=sem_cs.at[2 + s], recv_sem=sem_ch.at[s, 0],
                    device_id=(g + 1, i), device_id_type=MESH,
                ).start()

            return carry

        lax.fori_loop(0, xy, send, 0)

    def owner_give_residual():
        residuals = [res[m] for m in range(blocks)]

        def give(i, carry):
            start = jnp.full((8, 128), i * COLS_DEV, jnp.int32).astype(F32)
            message = residuals[blocks - 1]
            for m in range(blocks - 2, -1, -1):
                message = jnp.where(column_ids[m] >= start, residuals[m], message)
            send_d[i] = message
            return carry

        lax.fori_loop(0, xy, give, 0)

        def send(i, carry):
            @pl.when(i != j)
            def _():
                pltpu.make_async_remote_copy(
                    src_ref=send_d.at[i], dst_ref=recv_d.at[j], send_sem=sem_ds, recv_sem=sem_dr,
                    device_id=(g, i), device_id_type=MESH,
                ).start()

            @pl.when(i == j)
            def _():
                pltpu.make_async_copy(send_d.at[i], recv_d.at[j], sem_dr).start()

            return carry

        lax.fori_loop(0, xy, send, 0)

    def backward(s):
        @pl.when(jnp.logical_not(below))
        def _():
            recv_c[s, 0] = jnp.zeros((VIEWS, 8, 128), F32)

        @pl.when(jnp.logical_not(above))
        def _():
            recv_c[s, GROUPS + 1] = jnp.zeros((VIEWS, 8, 128), F32)

        arrived(recv_c.at[s, 1 : GROUPS + 1], sem_cr.at[s])

        @pl.when(below)
        def _():
            arrived(recv_c.at[s, 0], sem_ch.at[s, 0])

        @pl.when(above)
        def _():
            arrived(recv_c.at[s, GROUPS + 1], sem_ch.at[s, 1])

        hats = jnp.concatenate([hat_low, hat_high], axis=1)
        for v in range(VIEWS):
            rows = jnp.concatenate([recv_c[s, k, v] for k in range(GROUPS + 2)], axis=0)
            smeared = rounded(
                lax.dot_general(
                    rows, hats, (((0,), (0,)), ((), ())), precision=HIGHEST, preferred_element_type=F32
                )
            )
            whole = [smeared[8 * i : 8 * i + 8, 128 * p : 128 * p + 128] for p in range(2) for i in range(16)]
            for h in range(2):
                offset = shift[s, v, h]
                now = whole
                for bit in (128, 64, 32, 16, 8):
                    step = bit // 8
                    moved = (offset & bit) != 0
                    now = [
                        jnp.where(moved, now[(i + step) % 32], now[i]) for i in range(WIN // 8 + step - 1)
                    ]
                for i in range(WIN // 8):
                    turned[h, v * WIN + 8 * i : v * WIN + 8 * i + 8, :] = now[i]
        sides = [jnp.transpose(turned[h]).astype(BF16) for h in range(2)]
        last = s == SUBSETS - 1

        def one(pair, carry):
            for h in range(2):
                columns = pl.ds(pl.multiple_of(pair * 256, 256), 256)
                back = lax.dot_general(
                    sides[h], weights[2 * s + h, :, columns], (((1,), (0,)), ((), ())),
                    preferred_element_type=F32,
                )
                for part in range(2):
                    x = 2 * pair + part
                    mine = back[112:128, 128 * part : 128 * part + 128]
                    for q in range(6, -1, -1):
                        mine = jnp.where(
                            jnp.concatenate([band, band], axis=0) == q,
                            back[16 * q : 16 * q + 16, 128 * part : 128 * part + 128], mine,
                        )
                    norm = slice_total * ws[s, pl.ds(HALF * h + x, 1), :]
                    at = pl.ds(HALF * h + x, 16, stride=X_DEV)
                    new = it[at, :] + mine / jnp.maximum(norm, 1.0)
                    if last:
                        out_ref[at, :] = new
                    else:
                        it[at, :] = new
                        spread(new, h, x)
            return carry

        lax.fori_loop(0, HALF // 2, one, 0)

    forward(0)

    @pl.when(owner)
    def _():
        prepare_owner()
        window_starts(0)
        owner_work(0)

    geometry(1)
    make_weights(1)
    backward(0)
    forward(1)

    @pl.when(owner)
    def _():
        window_starts(1)
        owner_work(1)
        owner_give_residual()

    backward(1)

    arrived(recv_d, sem_dr)
    begin = j * COLS_DEV
    turn_back = lax.rem(128 - lax.rem(begin, 128), 128)
    odd = lax.rem(lax.div(begin, 128), 2) == 1
    keep = lane < 128 - lax.rem(begin, 128)
    from_low = jnp.logical_xor(keep, odd)
    for v in range(VIEWS):
        for k in range(GROUPS):
            message = pltpu.roll(recv_d[v * GROUPS + k], turn_back, 1)
            other = pltpu.roll(message, 4, 0)
            value = jnp.where(from_low, message, other)
            resid_ref[v, 4 * k : 4 * k + 4, :] = value[0:4, 0:COLS_DEV]

    sent_to_owners(send_m, sem_ms)
    for s in range(SUBSETS):
        flat = recv_a.at[s, 0]
        sent_to_owners(flat, sem_as.at[s])
        sent_to_owners(flat, sem_ts.at[s])

        @pl.when(below)
        def _():
            arrived(send_a.at[s, 0], sem_as.at[2 + s])

        @pl.when(above)
        def _():
            arrived(send_a.at[s, GROUPS + 1], sem_as.at[2 + s])

        @pl.when(owner)
        def _():
            arrived(send_c.at[s, 0 : xy - 1], sem_cs.at[s])

            @pl.when(has_beside)
            def _():
                arrived(send_c.at[s], sem_cs.at[2 + s])

    @pl.when(owner)
    def _():
        arrived(send_d.at[0 : xy - 1], sem_ds)


def local(gz, xy, volume, measured, view_order):
    blocks = COLS_DEV * xy // 256
    dma = pltpu.SemaphoreType.DMA
    vmem = pltpu.VMEM
    out, resid = pl.pallas_call(
        functools.partial(kernel, gz, xy),
        out_shape=(
            jax.ShapeDtypeStruct((Z_DEV * X_DEV, NY), F32),
            jax.ShapeDtypeStruct((VIEWS, ROWS_DEV, COLS_DEV), F32),
        ),
        in_specs=[
            pl.BlockSpec(memory_space=pltpu.SMEM),
            pl.BlockSpec(memory_space=pl.ANY),
            pl.BlockSpec(memory_space=pltpu.VMEM),
        ],
        out_specs=(pl.BlockSpec(memory_space=pltpu.VMEM), pl.BlockSpec(memory_space=pltpu.VMEM)),
        scratch_shapes=[
            vmem((Z_DEV * X_DEV, NY), F32),
            vmem((SUBSETS, VIEWS, X_DEV, NY), F32),
            vmem((SUBSETS, X_DEV, NY), F32),
            vmem((SUBSETS, VIEWS, 2, 8, 128), jnp.int32),
            vmem((SUBSETS, VIEWS, 2, 8, 128), F32),
            vmem((2 * SUBSETS, VIEWS * WIN, HALF * NY), BF16),
            vmem((2, 256, HALF * NY), BF16),
            vmem((VIEWS * 256, 128), F32),
            vmem((VIEWS * 256, 128), F32),
            vmem((OWNERS, 8, 128), F32),
            vmem((xy, 8, 128), F32),
            vmem((SUBSETS, blocks, 8, 128), F32),
            vmem((SUBSETS, GROUPS + 2, VIEWS, 8, 128), F32),
            vmem((SUBSETS, 2, xy, 8, 128), F32),
            vmem((SUBSETS, VIEWS, 8, 128), F32),
            vmem((SUBSETS, xy, 8, 128), F32),
            vmem((xy, 8, 128), F32),
            vmem((blocks, 8, 128), F32),
            vmem((blocks, 8, 128), F32),
            vmem((blocks, 8, 128), F32),
            vmem((SUBSETS, xy, 8, 128), F32),
            vmem((SUBSETS, GROUPS + 2, VIEWS, 8, 128), F32),
            vmem((xy, 8, 128), F32),
            vmem((OWNERS, 8, 128), F32),
            vmem((2, VIEWS * WIN, 128), F32),
            dma(()), dma(()), dma(()), dma((4,)), dma((2,)), dma((2,)), dma((2,)), dma((2,)),
            dma((4,)), dma((2,)), dma((2, 2)), dma(()), dma(()),
        ],
        compiler_params=pltpu.CompilerParams(collective_id=0, has_side_effects=True),
    )(view_order, volume.reshape(Z_DEV * X_DEV, NY), measured)
    return out.reshape(Z_DEV, X_DEV, NY), resid


def solution(mesh):
    in_specs = (P("gz", "xy", None), P(None, None, "gz", "xy"), P())
    out_specs = (P("gz", "xy", None), P(None, "gz", "xy"))
    body = functools.partial(local, mesh.shape["gz"], mesh.shape["xy"])
    return jax.shard_map(body, mesh=mesh, in_specs=in_specs, out_specs=out_specs, check_vma=False)
```

```python
import functools
import math

import jax
import jax.numpy as jnp
from jax import lax
from jax.experimental import pallas as pl
from jax.experimental.pallas import tpu as pltpu
from jax.sharding import PartitionSpec as P

Z_DEV = 16
X_DEV = 48
COLS_DEV = 48
NY = 128
VIEWS = 5
SUBSETS = 2
ANGLES = 48
ROWS_DEV = 20
HALF = X_DEV // 2
WIN = 48
GROUPS = 3
SLOTS = 7
SIZES = (7, 7, 6)
OWNERS = VIEWS * GROUPS
MESSAGES = ((-1, GROUPS - 1), (0, 0), (0, 1), (0, 2), (1, 0))
KINDS = len(MESSAGES)
MESH = pl.DeviceIdType.MESH
F32 = jnp.float32
BF16 = jnp.bfloat16


def iota(shape, dim):
    return lax.broadcasted_iota(jnp.int32, shape, dim)


def kernel(
    gz, xy, view_hbm, vol_ref, meas_hbm, out_ref, resid_ref,
    views, it, meas, up, ws, shift, trig, weights, data, window, mixer, smearer,
    send_m, recv_m, meas_rows, send_a, recv_a, starts, total, send_c, recv_c, send_d, recv_d, turned,
    sem_view, sem_vol, sem_meas, sem_ms, sem_mr, sem_as, sem_ar, sem_ah, sem_cs, sem_cr, sem_ch, sem_ds, sem_dr,
):
    g = lax.axis_index("gz")
    j = lax.axis_index("xy")
    nx_all, ny_all, dc_all = X_DEV * xy, NY, COLS_DEV * xy
    dr_all, nz_all = ROWS_DEV * gz, Z_DEV * gz
    blocks = dc_all // 128
    chip = lax.div(j, 2)
    owner = jnp.logical_and(lax.rem(j, 2) == 1, chip < OWNERS)
    own_view = lax.rem(lax.div(chip, GROUPS), VIEWS)
    own_group = lax.rem(chip, GROUPS)
    first_group = jnp.logical_and(owner, own_group == 0)
    last_group = jnp.logical_and(owner, own_group == GROUPS - 1)
    below, above = g > 0, g < gz - 1
    give_down = jnp.logical_and(first_group, below)
    give_up = jnp.logical_and(last_group, above)
    has_beside = jnp.logical_or(give_down, give_up)

    view_copy = pltpu.make_async_copy(view_hbm, views, sem_view)
    vol_copy = pltpu.make_async_copy(vol_ref, it, sem_vol)
    meas_copy = pltpu.make_async_copy(meas_hbm, meas, sem_meas)
    view_copy.start()
    vol_copy.start()
    meas_copy.start()

    barrier = pltpu.get_barrier_semaphore()

    def greet(plane, device):
        pl.semaphore_signal(barrier, inc=1, device_id=(plane, device), device_id_type=MESH)

    def greet_all(plane):
        for i in range(xy):
            greet(plane, i)

    def next_owner(t):
        return 2 * lax.rem(chip + t, OWNERS) + 1

    def next_device(t):
        return lax.rem(j + t, xy)

    with jax.named_scope("greet"):
        @pl.when(owner)
        def _():
            for t in range(1, xy):
                greet(g, next_device(t))

        @pl.when(jnp.logical_not(owner))
        def _():
            for t in range(OWNERS):
                greet(g, next_owner(t))

        @pl.when(give_down)
        def _():
            greet_all(g - 1)

        @pl.when(jnp.logical_and(below, jnp.logical_not(first_group)))
        def _():
            for v in range(VIEWS):
                greet(g - 1, 2 * (GROUPS * v + GROUPS - 1) + 1)

        @pl.when(give_up)
        def _():
            greet_all(g + 1)

        @pl.when(jnp.logical_and(above, jnp.logical_not(last_group)))
        def _():
            for v in range(VIEWS):
                greet(g + 1, 2 * GROUPS * v + 1)

    greeted = (
        jnp.where(owner, xy - 1, OWNERS)
        + jnp.where(below, jnp.where(first_group, xy, VIEWS), 0)
        + jnp.where(above, jnp.where(last_group, xy, VIEWS), 0)
    )

    lane = iota((8, 128), 1)
    sub = iota((8, 128), 0)
    lane_f = lane.astype(F32)
    sub_f = sub.astype(F32)
    band = lane // 16
    source = 2.0 * nx_all
    scale = 0.9 * (dc_all / nx_all)
    middle = (dc_all - 1) / 2.0
    x_first = (j * X_DEV).astype(F32)

    def project(x, y, cosine, sine):
        along = x * cosine + y * sine
        depth = y * cosine - x * sine
        return middle + scale * along * source / (source + depth)

    def hat(row, slice_id):
        position = (dr_all - 1) / 2.0 + 0.96 * (dr_all / nz_all) * (slice_id - (nz_all - 1) / 2.0)
        return jnp.maximum(0.0, 1.0 - jnp.abs(position - row) / 2.0)

    def rounded(x):
        return x.astype(BF16).astype(F32)

    def in_two(x):
        high = rounded(x)
        return high, x - high

    def geometry(s):
        for v in range(VIEWS):
            number = jnp.full((8, 128), views[s * VIEWS + v], jnp.int32).astype(F32)
            angle = 2.0 * math.pi * number / ANGLES
            cosine, sine = jnp.cos(angle), jnp.sin(angle)
            trig[s, v, 0] = cosine
            trig[s, v, 1] = sine
            y_low = (band * 16).astype(F32) - (ny_all - 1) / 2.0
            base = []
            for h in range(2):
                x_low = (x_first + HALF * h) - (nx_all - 1) / 2.0
                corners = [
                    project(x, y, cosine, sine)
                    for x in (x_low, x_low + (HALF - 1))
                    for y in (y_low, y_low + 15.0)
                ]
                lowest = jnp.minimum(jnp.minimum(corners[0], corners[1]), jnp.minimum(corners[2], corners[3]))
                start = jnp.floor((lowest - 0.03125) * 0.125) * 8.0
                base.append(start)
                shift[s, v, h] = (start - 256.0 * jnp.floor(start * (1.0 / 256.0))).astype(jnp.int32)
            for block in range(X_DEV // 8):
                x = (x_first + (8.0 * block + sub_f)) - (nx_all - 1) / 2.0
                y = lane_f - (ny_all - 1) / 2.0
                u = project(x, y, cosine, sine)
                up[s, v, 8 * block : 8 * block + 8, :] = u - base[block // (HALF // 8)]
                low = jnp.floor(u)
                both = rounded(jnp.maximum(0.0, 1.0 - jnp.abs(u - low))) + rounded(
                    jnp.maximum(0.0, 1.0 - jnp.abs(u - (low + 1.0)))
                )
                rows = slice(8 * block, 8 * block + 8)
                ws[s, rows, :] = both if v == 0 else ws[s, rows, :] + both

    window_ids = iota((WIN, 128), 0).astype(F32)

    def make_weights(s):
        def one(x, carry):
            columns = pl.ds(pl.multiple_of(x * 128, 128), 128)
            for h in range(2):
                for v in range(VIEWS):
                    u = up[s, v, pl.ds(HALF * h + x, 1), :]
                    w = jnp.maximum(0.0, 1.0 - jnp.abs(u - window_ids))
                    weights[2 * s + h, v * WIN : (v + 1) * WIN, columns] = w.astype(BF16)
            return carry

        lax.fori_loop(0, HALF, one, 0)

    band_masks = [(iota((16, 128), 1) // 16 == q).astype(F32).astype(BF16) for q in range(8)]

    def spread(values, h, x):
        columns = pl.ds(pl.multiple_of(x * 128, 128), 128)
        values = values.astype(BF16)
        for q in range(8):
            data[h, 16 * q : 16 * q + 16, columns] = values * band_masks[q]

    def row_tables():
        shape = (128, 128)
        at = iota(shape, 0)
        kind, half, slot = at // 16, (at // 8) % 2, at % 8
        row = jnp.where(kind == 0, slot + (SLOTS * MESSAGES[0][1] - ROWS_DEV), SLOTS * (kind - 1) + slot)
        row = jnp.where(kind == KINDS - 1, slot + ROWS_DEV, row)
        size = jnp.where(jnp.logical_or(kind == 0, kind == GROUPS), SIZES[-1], SLOTS)
        row_all = g * ROWS_DEV + row
        inside = jnp.logical_and(jnp.logical_and(row_all >= 0, row_all < dr_all), slot < size)
        inside = jnp.logical_and(inside, kind < KINDS)
        slice_all = (g * Z_DEV + iota(shape, 1) % 16).astype(F32)
        row_hat = jnp.where(inside, hat(row_all.astype(F32), slice_all), 0.0)
        own = jnp.logical_and(jnp.logical_and(kind >= 1, kind <= GROUPS), slot == 7)
        counts = jnp.where(jnp.logical_and(own, iota(shape, 1) % 16 < 2), 1.0, 0.0)
        count = 16 * KINDS
        for b in range(2):
            mine = half == b
            high, low = in_two(jnp.where(mine, row_hat, 0.0))
            ones = jnp.where(mine, counts, 0.0)
            smearer[0:128, 128 * b : 128 * b + 128] = high.astype(BF16)
            smearer[128:256, 128 * b : 128 * b + 128] = low.astype(BF16)
            for part, first, second in ((0, high, low), (1, high, low), (2, ones, jnp.zeros(shape, F32))):
                columns = slice(384 * b + 128 * part, 384 * b + 128 * part + 128)
                mixer[0:count, columns] = first[0:count].astype(BF16)
                mixer[count : 2 * count, columns] = second[0:count].astype(BF16)

    slices = (g * Z_DEV + iota((16, 128), 0)).astype(F32)
    slice_total = jnp.zeros((16, 1), F32)
    for part in range(-(-dr_all // 128)):
        rows = 128 * part + iota((16, 128), 1)
        weight = jnp.where(rows < dr_all, hat(rows.astype(F32), slices), 0.0)
        slice_total = slice_total + jnp.sum(weight, axis=1, keepdims=True)
    slice_total = jnp.broadcast_to(slice_total, (16, 128))
    own_row = (g * ROWS_DEV + own_group * SLOTS + sub).astype(F32)
    ray_row = jnp.zeros((8, 1), F32)
    for part in range(-(-nz_all // 128)):
        ids = 128 * part + lane
        weight = jnp.where(ids < nz_all, hat(own_row, ids.astype(F32)), 0.0)
        ray_row = ray_row + jnp.sum(weight, axis=1, keepdims=True)
    ray_row = jnp.broadcast_to(ray_row, (8, 128))
    own_slot = sub < jnp.where(own_group == GROUPS - 1, SIZES[-1], SLOTS)
    column_ids = [(128 * m + lane).astype(F32) for m in range(blocks)]

    def remote(src, dst, send_sem, recv_sem, plane, device):
        pltpu.make_async_remote_copy(
            src_ref=src, dst_ref=dst, send_sem=send_sem, recv_sem=recv_sem,
            device_id=(plane, device), device_id_type=MESH,
        ).start()

    def arrived(ref, sem):
        pltpu.make_async_copy(ref, ref, sem).wait()

    def to_owners(src, dst, send_sem, recv_sem):
        for t in range(1, OWNERS):
            device = next_owner(t)
            remote(src(lax.div(device, 2)), dst, send_sem, recv_sem, g, device)

        @pl.when(jnp.logical_not(owner))
        def _():
            device = next_owner(0)
            remote(src(lax.div(device, 2)), dst, send_sem, recv_sem, g, device)

    def with_owners(ref, sem):
        @pl.when(owner)
        def _():
            arrived(ref.at[0 : OWNERS - 1], sem)

        @pl.when(jnp.logical_not(owner))
        def _():
            arrived(ref.at[0:OWNERS], sem)

    def table(x, carry):
        columns = pl.ds(pl.multiple_of(x * 128, 128), 128)
        for h in range(2):
            for q in range(8):
                pair = iota((16, 128), 0) < 2
                row = jnp.where(jnp.logical_and(pair, iota((16, 128), 1) // 16 == q), 1.0, 0.0)
                data[h, 128 + 16 * q : 128 + 16 * q + 16, columns] = row.astype(BF16)
        return carry

    def fill_data(x, carry):
        for h in range(2):
            spread(it[pl.ds(HALF * h + x, 16, stride=X_DEV), :], h, x)
        return carry

    view_copy.wait()
    with jax.named_scope("geom0"):
        geometry(0)
    with jax.named_scope("mw0"):
        make_weights(0)
    with jax.named_scope("tables"):
        row_tables()
        lax.fori_loop(0, HALF, table, 0)
    with jax.named_scope("fill"):
        vol_copy.wait()
        lax.fori_loop(0, HALF, fill_data, 0)

    with jax.named_scope("measured"):
        meas_copy.wait()
        turn = lax.rem(j * COLS_DEV, 128)
        for v in range(VIEWS):
            for k in range(GROUPS):
                o = GROUPS * v + k
                send_m[o] = jnp.zeros((16, 128), F32)
                for s in range(SUBSETS):
                    for slot in range(SIZES[k]):
                        send_m[o, 8 * s + slot, 0:COLS_DEV] = meas[v, SLOTS * k + slot, s, :]
        for o in range(OWNERS):
            send_m[o] = pltpu.roll(send_m[o], turn, 1)

    with jax.named_scope("barrier"):
        pl.semaphore_wait(barrier, greeted)

    def send_measured():
        to_owners(lambda o: send_m.at[o], recv_m.at[j], sem_ms, sem_mr)

        @pl.when(owner)
        def _():
            recv_m[j] = send_m[chip]

    def forward(s):
        with jax.named_scope("f_dot"):
            sums = [
                lax.dot_general(
                    weights[2 * s + h], data[h], (((1,), (1,)), ((), ())), preferred_element_type=F32
                )
                for h in range(2)
            ]
        with jax.named_scope("f_place"):
            for v in range(VIEWS):
                for part in range(2):
                    halves = []
                    for h in range(2):
                        offset = shift[s, v, h]
                        rows = [
                            sums[h][v * WIN + 8 * i : v * WIN + 8 * i + 8, 128 * part : 128 * part + 128]
                            for i in range(WIN // 8)
                        ] + [None] * (32 - WIN // 8)
                        for bit in (8, 16, 32, 64, 128):
                            moved = (offset & bit) != 0
                            step = bit // 8
                            new = []
                            for i in range(32):
                                old, other = rows[i], rows[(i - step) % 32]
                                if old is None and other is None:
                                    new.append(None)
                                elif old is None:
                                    new.append(jnp.where(moved, other, 0.0))
                                elif other is None:
                                    new.append(jnp.where(moved, 0.0, old))
                                else:
                                    new.append(jnp.where(moved, other, old))
                            rows = new
                        halves.append(rows)
                    for i in range(16):
                        for b in range(2):
                            value = halves[0][16 * b + i] + halves[1][16 * b + i]
                            at = slice(128 * v + 8 * i, 128 * v + 8 * i + 8)
                            high, low = in_two(value)
                            if part == 0:
                                window[at, 384 * b : 384 * b + 128] = high
                                window[at, 384 * b + 128 : 384 * b + 256] = low
                            else:
                                window[at, 384 * b + 256 : 384 * b + 384] = jnp.where(lane % 16 == 0, high, low)
        with jax.named_scope("f_mix"):
            mixed = lax.dot_general(
                mixer[...], window[...].astype(BF16), (((1,), (1,)), ((), ())), preferred_element_type=F32
            )
            count = 16 * KINDS
            for v in range(VIEWS):
                for k in range(KINDS):
                    columns = slice(128 * v, 128 * v + 128)
                    send_a[s, k, v] = (
                        mixed[16 * k : 16 * k + 16, columns] + mixed[count + 16 * k : count + 16 * k + 16, columns]
                    )
        with jax.named_scope("f_send"):
            for there, plane, slot, group in ((below, g - 1, 0, GROUPS - 1), (above, g + 1, KINDS - 1, 0)):
                @pl.when(there)
                def _():
                    for v in range(VIEWS):
                        remote(
                            send_a.at[s, slot, v], recv_a.at[s, 1, j], sem_as.at[2 + s], sem_ah.at[s],
                            plane, 2 * (GROUPS * v + group) + 1,
                        )
            to_owners(
                lambda o: send_a.at[s, 1 + lax.rem(o, GROUPS), lax.div(o, GROUPS)],
                recv_a.at[s, 0, j], sem_as.at[s], sem_ar.at[s],
            )

            @pl.when(owner)
            def _():
                recv_a[s, 0, j] = send_a[s, 1 + own_group, own_view]

    def prepare_owner():
        arrived(recv_m.at[0 : xy - 1], sem_mr)
        for block in range(blocks):
            first, last = 128 * block, 128 * block + 128
            for s in range(SUBSETS):
                value = jnp.zeros((8, 128), F32)
                for i in range(first // COLS_DEV, min(xy, -(-last // COLS_DEV))):
                    low, high = max(COLS_DEV * i, first) - first, min(COLS_DEV * (i + 1), last) - first
                    piece = recv_m[i, 8 * s : 8 * s + 8, :]
                    value = jnp.where(jnp.logical_and(lane >= low, lane < high), piece, value)
                meas_rows[s, block] = value

    def window_starts(s):
        cosine, sine = trig[s, own_view, 0], trig[s, own_view, 1]

        def one(i, carry):
            x = jnp.full((8, 128), i * X_DEV, jnp.int32).astype(F32) + ((X_DEV - 1) / 2.0 - (nx_all - 1) / 2.0)
            starts[s, i] = jnp.floor(project(x, 0.0, cosine, sine)) - 128.0
            return carry

        lax.fori_loop(0, xy, one, 0)

    def owner_work(s):
        with jax.named_scope("wait_a"):
            arrived(recv_a.at[s, 0, 0 : xy - 1], sem_ar.at[s])

        def adder(source):
            def add(i, sums):
                start = starts[s, i]
                parts = recv_a[s, source, i, 0:8, :], recv_a[s, source, i, 8:16, :]
                new = []
                for m in range(blocks):
                    away = column_ids[m] - start
                    hit = jnp.logical_and(away >= 0.0, away < 256.0)
                    new.append(sums[m] + jnp.where(hit, parts[m % 2], 0.0))
                return tuple(new)

            return lax.fori_loop(0, xy, add, tuple(jnp.zeros((8, 128), F32) for _ in range(blocks)))

        with jax.named_scope("o_add"):
            sums = adder(0)
            for m in range(blocks):
                total[m] = sums[m]

        @pl.when(has_beside)
        def _():
            with jax.named_scope("wait_h"):
                arrived(recv_a.at[s, 1], sem_ah.at[s])
            with jax.named_scope("o_addh"):
                sums = adder(1)
                for m in range(blocks):
                    total[m] = total[m] + sums[m]

        with jax.named_scope("o_give"):
            residuals = []
            for m in range(blocks):
                value = total[m]
                columns = jnp.broadcast_to(value[7:8, :], (8, 128))
                residual = meas_rows[s, m] - value / jnp.maximum(ray_row * columns, 1.0)
                residual = jnp.where(own_slot, residual, 0.0)
                total[m] = residual
                residuals.append(rounded(residual))

            def give(i, carry):
                start = starts[s, i]
                parts = []
                for b in range(2):
                    message = residuals[blocks - 2 + b]
                    for m in range(blocks - 4 + b, -1, -2):
                        message = jnp.where(column_ids[m] >= start, residuals[m], message)
                    parts.append(message)
                send_c[s, i] = jnp.concatenate(parts, axis=0).astype(BF16)
                return carry

            lax.fori_loop(0, xy, give, 0)

        with jax.named_scope("o_send"):
            @pl.when(give_down)
            def _():
                for t in range(xy):
                    i = next_device(t)
                    remote(
                        send_c.at[s, i], recv_c.at[s, OWNERS + VIEWS + own_view],
                        sem_cs.at[2 + s], sem_ch.at[s, 1], g - 1, i,
                    )

            @pl.when(give_up)
            def _():
                for t in range(xy):
                    i = next_device(t)
                    remote(
                        send_c.at[s, i], recv_c.at[s, OWNERS + own_view], sem_cs.at[2 + s], sem_ch.at[s, 0], g + 1, i
                    )

            for t in range(1, xy):
                i = next_device(t)
                remote(send_c.at[s, i], recv_c.at[s, chip], sem_cs.at[s], sem_cr.at[s], g, i)
            recv_c[s, chip] = send_c[s, j]

    def owner_give_residual():
        for i in range(xy):
            first = COLS_DEV * i // 128
            message = total[first]
            if first + 1 < blocks:
                message = jnp.where(lane >= COLS_DEV * i % 128, message, total[first + 1])
            send_d[i] = message
        for t in range(1, xy):
            i = next_device(t)
            remote(send_d.at[i], recv_d.at[chip], sem_ds, sem_dr, g, i)
        recv_d[chip] = send_d[j]

    def backward(s):
        @pl.when(jnp.logical_not(below))
        def _():
            recv_c[s, OWNERS : OWNERS + VIEWS] = jnp.zeros((VIEWS, 16, 128), BF16)

        @pl.when(jnp.logical_not(above))
        def _():
            recv_c[s, OWNERS + VIEWS : OWNERS + 2 * VIEWS] = jnp.zeros((VIEWS, 16, 128), BF16)

        with jax.named_scope("wait_c"):
            with_owners(recv_c.at[s], sem_cr.at[s])

        with jax.named_scope("wait_ch"):
            @pl.when(below)
            def _():
                arrived(recv_c.at[s, OWNERS : OWNERS + VIEWS], sem_ch.at[s, 0])

            @pl.when(above)
            def _():
                arrived(recv_c.at[s, OWNERS + VIEWS : OWNERS + 2 * VIEWS], sem_ch.at[s, 1])

        with jax.named_scope("b_smear"):
            columns = []
            for v in range(VIEWS):
                from_rows = [OWNERS + v] + [GROUPS * v + k for k in range(GROUPS)] + [OWNERS + VIEWS + v]
                rows = jnp.concatenate(
                    [recv_c[s, at].astype(F32) for at in from_rows] + [jnp.zeros((128 - 16 * KINDS, 128), F32)],
                    axis=0,
                )
                flipped = jnp.transpose(rows).astype(BF16)
                columns.append(jnp.concatenate([flipped, flipped], axis=1))
            smeared = rounded(
                lax.dot_general(
                    jnp.concatenate(columns, axis=0), smearer[...], (((1,), (0,)), ((), ())),
                    preferred_element_type=F32,
                )
            )
            for v in range(VIEWS):
                whole = [
                    smeared[128 * v + 8 * i : 128 * v + 8 * i + 8, 128 * p : 128 * p + 128]
                    for p in range(2)
                    for i in range(16)
                ]
                for h in range(2):
                    offset = shift[s, v, h]
                    now = whole
                    for bit in (128, 64, 32, 16, 8):
                        step = bit // 8
                        moved = (offset & bit) != 0
                        now = [
                            jnp.where(moved, now[(i + step) % 32], now[i]) for i in range(WIN // 8 + step - 1)
                        ]
                    for i in range(WIN // 8):
                        turned[h, v * WIN + 8 * i : v * WIN + 8 * i + 8, :] = now[i]
        with jax.named_scope("b_turn"):
            sides = [jnp.transpose(turned[h]).astype(BF16) for h in range(2)]
        last = s == SUBSETS - 1
        per_step = 4

        def one(step, carry):
            for h in range(2):
                columns = pl.ds(pl.multiple_of(step * (128 * per_step), 128 * per_step), 128 * per_step)
                back = lax.dot_general(
                    sides[h], weights[2 * s + h, :, columns], (((1,), (0,)), ((), ())),
                    preferred_element_type=F32,
                )
                for part in range(per_step):
                    x = per_step * step + part
                    mine = back[112:128, 128 * part : 128 * part + 128]
                    for q in range(6, -1, -1):
                        mine = jnp.where(
                            jnp.concatenate([band, band], axis=0) == q,
                            back[16 * q : 16 * q + 16, 128 * part : 128 * part + 128], mine,
                        )
                    norm = slice_total * ws[s, pl.ds(HALF * h + x, 1), :]
                    at = pl.ds(HALF * h + x, 16, stride=X_DEV)
                    new = it[at, :] + mine / jnp.maximum(norm, 1.0)
                    if last:
                        out_ref[at, :] = new
                    else:
                        it[at, :] = new
                        spread(new, h, x)
            return carry

        with jax.named_scope("b_loop"):
            lax.fori_loop(0, HALF // per_step, one, 0)

    with jax.named_scope("send_m"):
        send_measured()
    forward(0)

    @pl.when(owner)
    def _():
        with jax.named_scope("prep"):
            prepare_owner()
            window_starts(0)
        owner_work(0)

    with jax.named_scope("gw1"):
        geometry(1)
        make_weights(1)

    @pl.when(owner)
    def _():
        window_starts(1)

    backward(0)
    forward(1)

    @pl.when(owner)
    def _():
        owner_work(1)
        with jax.named_scope("give"):
            owner_give_residual()

    backward(1)

    with jax.named_scope("tail"):
        with_owners(recv_d, sem_dr)
        turn_back = lax.rem(128 - lax.rem(j * COLS_DEV, 128), 128)
        for v in range(VIEWS):
            for k in range(GROUPS):
                message = pltpu.roll(recv_d[GROUPS * v + k], turn_back, 1)
                resid_ref[v, SLOTS * k : SLOTS * k + SIZES[k], :] = message[0 : SIZES[k], 0:COLS_DEV]

        with_owners(send_m, sem_ms)
        for s in range(SUBSETS):
            with_owners(recv_a.at[s, 0], sem_as.at[s])

            @pl.when(below)
            def _():
                arrived(send_a.at[s, 0], sem_as.at[2 + s])

            @pl.when(above)
            def _():
                arrived(send_a.at[s, KINDS - 1], sem_as.at[2 + s])

            @pl.when(owner)
            def _():
                arrived(send_c.at[s, 0 : xy - 1], sem_cs.at[s])

                @pl.when(has_beside)
                def _():
                    arrived(send_c.at[s], sem_cs.at[2 + s])

        @pl.when(owner)
        def _():
            arrived(send_d.at[0 : xy - 1], sem_ds)


def local(gz, xy, volume, measured, view_order):
    blocks = COLS_DEV * xy // 128
    dma = pltpu.SemaphoreType.DMA
    vmem = pltpu.VMEM
    out, resid = pl.pallas_call(
        functools.partial(kernel, gz, xy),
        out_shape=(
            jax.ShapeDtypeStruct((Z_DEV * X_DEV, NY), F32),
            jax.ShapeDtypeStruct((VIEWS, ROWS_DEV, COLS_DEV), F32),
        ),
        in_specs=[pl.BlockSpec(memory_space=pl.ANY)] * 3,
        out_specs=(pl.BlockSpec(memory_space=pltpu.VMEM), pl.BlockSpec(memory_space=pltpu.VMEM)),
        scratch_shapes=[
            pltpu.SMEM((ANGLES,), jnp.int32),
            vmem((Z_DEV * X_DEV, NY), F32),
            vmem((VIEWS, ROWS_DEV, SUBSETS, COLS_DEV), F32),
            vmem((SUBSETS, VIEWS, X_DEV, NY), F32),
            vmem((SUBSETS, X_DEV, NY), F32),
            vmem((SUBSETS, VIEWS, 2, 8, 128), jnp.int32),
            vmem((SUBSETS, VIEWS, 2, 8, 128), F32),
            vmem((2 * SUBSETS, VIEWS * WIN, HALF * NY), BF16),
            vmem((2, 256, HALF * NY), BF16),
            vmem((VIEWS * 128, 768), F32),
            vmem((32 * KINDS, 768), BF16),
            vmem((256, 256), BF16),
            vmem((OWNERS, 16, 128), F32),
            vmem((xy, 16, 128), F32),
            vmem((SUBSETS, blocks, 8, 128), F32),
            vmem((SUBSETS, KINDS, VIEWS, 16, 128), F32),
            vmem((SUBSETS, 2, xy, 16, 128), F32),
            vmem((SUBSETS, xy, 8, 128), F32),
            vmem((blocks, 8, 128), F32),
            vmem((SUBSETS, xy, 16, 128), BF16),
            vmem((SUBSETS, OWNERS + 2 * VIEWS, 16, 128), BF16),
            vmem((xy, 8, 128), F32),
            vmem((OWNERS, 8, 128), F32),
            vmem((2, VIEWS * WIN, 128), F32),
            dma(()), dma(()), dma(()), dma(()), dma(()), dma((4,)), dma((2,)), dma((2,)),
            dma((4,)), dma((2,)), dma((2, 2)), dma(()), dma(()),
        ],
        compiler_params=pltpu.CompilerParams(collective_id=0, has_side_effects=True),
    )(view_order, volume.reshape(Z_DEV * X_DEV, NY), measured.transpose(1, 2, 0, 3))
    return out.reshape(Z_DEV, X_DEV, NY), resid


def solution(mesh):
    in_specs = (P("gz", "xy", None), P(None, None, "gz", "xy"), P())
    out_specs = (P("gz", "xy", None), P(None, "gz", "xy"))
    body = functools.partial(local, mesh.shape["gz"], mesh.shape["xy"])
    return jax.shard_map(body, mesh=mesh, in_specs=in_specs, out_specs=out_specs, check_vma=False)
```

```python
import functools
import math

import jax
import jax.numpy as jnp
from jax import lax
from jax.experimental import pallas as pl
from jax.experimental.pallas import tpu as pltpu
from jax.sharding import PartitionSpec as P

Z_DEV = 16
X_DEV = 48
COLS_DEV = 48
NY = 128
VIEWS = 5
SUBSETS = 2
ANGLES = 48
ROWS_DEV = 20
HALF = X_DEV // 2
WIN = 48
GROUPS = 3
SLOTS = 7
SIZES = (7, 7, 6)
OWNERS = VIEWS * GROUPS
EDGE = 4
EDGE_SLOT = ROWS_DEV - EDGE - SLOTS * (GROUPS - 1)
ROWS = 16 * GROUPS + 16
MESH = pl.DeviceIdType.MESH
F32 = jnp.float32
BF16 = jnp.bfloat16


def iota(shape, dim):
    return lax.broadcasted_iota(jnp.int32, shape, dim)


def kernel(
    gz, xy, view_hbm, vol_ref, meas_hbm, out_ref, resid_ref,
    views, it, meas, low_id, low_w, high_w, ws, shift, trig, weights, data, window, counted, counted_ahead, count_rows, mixer, smearer,
    send_m, recv_m, meas_rows, send_a, recv_a, send_e, recv_e, starts, total, send_c, recv_c, send_f, recv_f,
    send_d, recv_d, turned,
    sem_view, sem_vol, sem_meas, sem_ms, sem_mr, sem_as, sem_ar, sem_ah, sem_cs, sem_cr, sem_ch, sem_ds, sem_dr,
):
    g = lax.axis_index("gz")
    j = lax.axis_index("xy")
    nx_all, ny_all, dc_all = X_DEV * xy, NY, COLS_DEV * xy
    dr_all, nz_all = ROWS_DEV * gz, Z_DEV * gz
    blocks = dc_all // 128
    chip = lax.div(j, 2)
    owner = jnp.logical_and(lax.rem(j, 2) == 1, chip < OWNERS)
    own_view = lax.rem(lax.div(chip, GROUPS), VIEWS)
    own_group = lax.rem(chip, GROUPS)
    first_group = jnp.logical_and(owner, own_group == 0)
    last_group = jnp.logical_and(owner, own_group == GROUPS - 1)
    below, above = g > 0, g < gz - 1
    give_down = jnp.logical_and(first_group, below)
    give_up = jnp.logical_and(last_group, above)
    has_beside = jnp.logical_or(give_down, give_up)

    view_copy = pltpu.make_async_copy(view_hbm, views, sem_view)
    vol_copy = pltpu.make_async_copy(vol_ref, it, sem_vol)
    meas_copy = pltpu.make_async_copy(meas_hbm, meas, sem_meas)
    view_copy.start()
    vol_copy.start()
    meas_copy.start()

    barrier = pltpu.get_barrier_semaphore()

    def greet(plane, device):
        pl.semaphore_signal(barrier, inc=1, device_id=(plane, device), device_id_type=MESH)

    def greet_all(plane):
        for i in range(xy):
            greet(plane, i)

    def next_owner(t):
        return 2 * lax.rem(chip + t, OWNERS) + 1

    def next_device(t):
        return lax.rem(j + t, xy)

    with jax.named_scope("greet"):
        @pl.when(owner)
        def _():
            for t in range(1, xy):
                greet(g, next_device(t))

        @pl.when(jnp.logical_not(owner))
        def _():
            for t in range(OWNERS):
                greet(g, next_owner(t))

        @pl.when(give_down)
        def _():
            greet_all(g - 1)

        @pl.when(jnp.logical_and(below, jnp.logical_not(first_group)))
        def _():
            for v in range(VIEWS):
                greet(g - 1, 2 * (GROUPS * v + GROUPS - 1) + 1)

        @pl.when(give_up)
        def _():
            greet_all(g + 1)

        @pl.when(jnp.logical_and(above, jnp.logical_not(last_group)))
        def _():
            for v in range(VIEWS):
                greet(g + 1, 2 * GROUPS * v + 1)

    greeted = (
        jnp.where(owner, xy - 1, OWNERS)
        + jnp.where(below, jnp.where(first_group, xy, VIEWS), 0)
        + jnp.where(above, jnp.where(last_group, xy, VIEWS), 0)
    )

    lane = iota((8, 128), 1)
    sub = iota((8, 128), 0)
    lane_f = lane.astype(F32)
    sub_f = sub.astype(F32)
    band = lane // 16
    source = 2.0 * nx_all
    scale = 0.9 * (dc_all / nx_all)
    middle = (dc_all - 1) / 2.0
    x_first = (j * X_DEV).astype(F32)

    def project(x, y, cosine, sine):
        along = x * cosine + y * sine
        depth = y * cosine - x * sine
        return middle + scale * along * source / (source + depth)

    def hat(row, slice_id):
        position = (dr_all - 1) / 2.0 + 0.96 * (dr_all / nz_all) * (slice_id - (nz_all - 1) / 2.0)
        return jnp.maximum(0.0, 1.0 - jnp.abs(position - row) / 2.0)

    def rounded(x):
        return x.astype(BF16).astype(F32)

    def in_two(x):
        high = rounded(x)
        return high, x - high

    def geometry(s):
        for v in range(VIEWS):
            number = jnp.full((8, 128), views[s * VIEWS + v], jnp.int32).astype(F32)
            angle = 2.0 * math.pi * number / ANGLES
            cosine, sine = jnp.cos(angle), jnp.sin(angle)
            trig[s, v, 0] = cosine
            trig[s, v, 1] = sine
            y_low = (band * 16).astype(F32) - (ny_all - 1) / 2.0
            base = []
            for h in range(2):
                x_low = (x_first + HALF * h) - (nx_all - 1) / 2.0
                corners = [
                    project(x, y, cosine, sine)
                    for x in (x_low, x_low + (HALF - 1))
                    for y in (y_low, y_low + 15.0)
                ]
                lowest = jnp.minimum(jnp.minimum(corners[0], corners[1]), jnp.minimum(corners[2], corners[3]))
                start = jnp.floor((lowest - 0.03125) * 0.125) * 8.0
                base.append(start)
                shift[s, v, h] = (start - 256.0 * jnp.floor(start * (1.0 / 256.0))).astype(jnp.int32)
            for block in range(X_DEV // 8):
                x = (x_first + (8.0 * block + sub_f)) - (nx_all - 1) / 2.0
                y = lane_f - (ny_all - 1) / 2.0
                u = project(x, y, cosine, sine)
                low = jnp.floor(u)
                first = rounded(jnp.maximum(0.0, 1.0 - jnp.abs(u - low)))
                second = rounded(jnp.maximum(0.0, 1.0 - jnp.abs(u - (low + 1.0))))
                both = first + second
                rows = slice(8 * block, 8 * block + 8)
                low_id[s, v, rows, :] = low - base[block // (HALF // 8)]
                low_w[s, v, rows, :] = first
                high_w[s, v, rows, :] = second
                ws[s, rows, :] = both if v == 0 else ws[s, rows, :] + both

    window_ids = [(iota((16, 128), 0) + 16 * t).astype(F32).astype(BF16) for t in range(WIN // 16)]
    window_ids_less = [(iota((16, 128), 0) + (16 * t - 1)).astype(F32).astype(BF16) for t in range(WIN // 16)]

    def make_weights(s):
        def one(x, carry):
            columns = pl.ds(pl.multiple_of(x * 128, 128), 128)
            for h in range(2):
                for v in range(VIEWS):
                    row = pl.ds(HALF * h + x, 1)
                    at, first, second = (
                        jnp.broadcast_to(ref[s, v, row, :], (16, 128)).astype(BF16) for ref in (low_id, low_w, high_w)
                    )
                    for t in range(WIN // 16):
                        w = jnp.where(window_ids[t] == at, first, jnp.zeros_like(first))
                        w = jnp.where(window_ids_less[t] == at, second, w)
                        weights[2 * s + h, v * WIN + 16 * t : v * WIN + 16 * t + 16, columns] = w
            return carry

        lax.fori_loop(0, HALF, one, 0)

    band_masks = [(iota((16, 128), 1) // 16 == q).astype(F32).astype(BF16) for q in range(8)]

    def spread(values, h, x):
        columns = pl.ds(pl.multiple_of(x * 128, 128), 128)
        values = values.astype(BF16)
        for q in range(8):
            data[h, 16 * q : 16 * q + 16, columns] = values * band_masks[q]

    def row_tables():
        shape = (ROWS, 128)
        at = iota(shape, 0)
        own = at < 16 * GROUPS
        half = jnp.where(own, (at // 8) % 2, (at // 4) % 2)
        slot = jnp.where(own, at % 8, at % 4)
        edge = jnp.where(at < 16 * GROUPS + 8, -EDGE, ROWS_DEV)
        row = slot + jnp.where(own, SLOTS * (at // 16), edge)
        size = jnp.where(at // 16 == GROUPS - 1, SIZES[-1], SLOTS)
        row_all = g * ROWS_DEV + row
        inside = jnp.logical_and(jnp.logical_and(row_all >= 0, row_all < dr_all), slot < size)
        slice_all = (g * Z_DEV + iota(shape, 1) % 16).astype(F32)
        row_hat = jnp.where(inside, hat(row_all.astype(F32), slice_all), 0.0)
        counts = jnp.where(jnp.logical_and(jnp.logical_and(own, slot == 7), iota(shape, 1) % 16 < 2), 1.0, 0.0)
        for b in range(2):
            mine = half == b
            high, low = in_two(jnp.where(mine, row_hat, 0.0))
            smearer[0:ROWS, 128 * b : 128 * b + 128] = high.astype(BF16)
            smearer[ROWS : 2 * ROWS, 128 * b : 128 * b + 128] = low.astype(BF16)
            for part in range(2):
                columns = slice(256 * b + 128 * part, 256 * b + 128 * part + 128)
                mixer[0:ROWS, columns] = high.astype(BF16)
                mixer[ROWS : 2 * ROWS, columns] = low.astype(BF16)
            count_rows[:, 128 * b : 128 * b + 128] = jnp.where(mine, counts, 0.0).astype(BF16)

    slices = (g * Z_DEV + iota((16, 128), 0)).astype(F32)
    slice_total = jnp.zeros((16, 1), F32)
    for part in range(-(-dr_all // 128)):
        rows = 128 * part + iota((16, 128), 1)
        weight = jnp.where(rows < dr_all, hat(rows.astype(F32), slices), 0.0)
        slice_total = slice_total + jnp.sum(weight, axis=1, keepdims=True)
    slice_total = jnp.broadcast_to(slice_total, (16, 128))
    own_row = (g * ROWS_DEV + own_group * SLOTS + sub).astype(F32)
    ray_row = jnp.zeros((8, 1), F32)
    for part in range(-(-nz_all // 128)):
        ids = 128 * part + lane
        weight = jnp.where(ids < nz_all, hat(own_row, ids.astype(F32)), 0.0)
        ray_row = ray_row + jnp.sum(weight, axis=1, keepdims=True)
    ray_row = jnp.broadcast_to(ray_row, (8, 128))
    own_slot = sub < jnp.where(own_group == GROUPS - 1, SIZES[-1], SLOTS)
    column_ids = [(128 * m + lane).astype(F32) for m in range(blocks)]

    def remote(src, dst, send_sem, recv_sem, plane, device):
        pltpu.make_async_remote_copy(
            src_ref=src, dst_ref=dst, send_sem=send_sem, recv_sem=recv_sem,
            device_id=(plane, device), device_id_type=MESH,
        ).start()

    def arrived(ref, sem):
        pltpu.make_async_copy(ref, ref, sem).wait()

    def to_owners(src, dst, send_sem, recv_sem):
        for t in range(1, OWNERS):
            device = next_owner(t)
            remote(src(lax.div(device, 2)), dst, send_sem, recv_sem, g, device)

        @pl.when(jnp.logical_not(owner))
        def _():
            device = next_owner(0)
            remote(src(lax.div(device, 2)), dst, send_sem, recv_sem, g, device)

    def with_owners(ref, sem):
        @pl.when(owner)
        def _():
            arrived(ref.at[0 : OWNERS - 1], sem)

        @pl.when(jnp.logical_not(owner))
        def _():
            arrived(ref.at[0:OWNERS], sem)

    def table(x, carry):
        columns = pl.ds(pl.multiple_of(x * 128, 128), 128)
        for h in range(2):
            for q in range(8):
                pair = iota((16, 128), 0) < 2
                row = jnp.where(jnp.logical_and(pair, iota((16, 128), 1) // 16 == q), 1.0, 0.0)
                data[h, 128 + 16 * q : 128 + 16 * q + 16, columns] = row.astype(BF16)
        return carry

    def fill_data(x, carry):
        for h in range(2):
            spread(it[pl.ds(HALF * h + x, 16, stride=X_DEV), :], h, x)
        return carry

    view_copy.wait()
    with jax.named_scope("geom0"):
        geometry(0)
    with jax.named_scope("mw0"):
        make_weights(0)
    with jax.named_scope("tables"):
        row_tables()
        lax.fori_loop(0, HALF, table, 0)
    with jax.named_scope("fill"):
        vol_copy.wait()
        lax.fori_loop(0, HALF, fill_data, 0)

    with jax.named_scope("measured"):
        meas_copy.wait()
        turn = lax.rem(j * COLS_DEV, 128)
        for v in range(VIEWS):
            for k in range(GROUPS):
                o = GROUPS * v + k
                send_m[o] = jnp.zeros((16, 128), F32)
                for s in range(SUBSETS):
                    for slot in range(SIZES[k]):
                        send_m[o, 8 * s + slot, 0:COLS_DEV] = meas[v, SLOTS * k + slot, s, :]
        for o in range(OWNERS):
            send_m[o] = pltpu.roll(send_m[o], turn, 1)

    with jax.named_scope("barrier"):
        pl.semaphore_wait(barrier, greeted)

    def send_measured():
        to_owners(lambda o: send_m.at[o], recv_m.at[j], sem_ms, sem_mr)

        @pl.when(owner)
        def _():
            recv_m[j] = send_m[chip]

    def placed(sums, s, v, part):
        halves = []
        for h in range(2):
            offset = shift[s, v, h]
            rows = [
                sums[h][v * WIN + 8 * i : v * WIN + 8 * i + 8, 128 * part : 128 * part + 128] for i in range(WIN // 8)
            ] + [None] * (32 - WIN // 8)
            for bit in (8, 16, 32, 64, 128):
                moved = (offset & bit) != 0
                step = bit // 8
                new = []
                for i in range(32):
                    old, other = rows[i], rows[(i - step) % 32]
                    if old is None and other is None:
                        new.append(None)
                    elif old is None:
                        new.append(jnp.where(moved, other, 0.0))
                    elif other is None:
                        new.append(jnp.where(moved, 0.0, old))
                    else:
                        new.append(jnp.where(moved, other, old))
                rows = new
            halves.append(rows)
        return [a + b for a, b in zip(*halves)]

    def pairs(pieces):
        for i in range(0, 32, 2):
            yield i // 16, 8 * (i % 16), jnp.concatenate([pieces[i], pieces[i + 1]], axis=0)

    def band_sums(s, part):
        rows = slice(0, 256) if part is None else slice(128 * part, 128 * part + 128)
        return [
            lax.dot_general(
                weights[2 * s + h], data[h, rows, :], (((1,), (1,)), ((), ())), preferred_element_type=F32
            )
            for h in range(2)
        ]

    first_lane = iota((16, 128), 1) % 16 == 0

    def count_columns(s, sums, part):
        for v in range(VIEWS):
            for b, at, value in pairs(placed(sums, s, v, part)):
                high, low = in_two(value)
                counted[128 * v + at : 128 * v + at + 16, 128 * b : 128 * b + 128] = jnp.where(
                    first_lane, high, low
                ).astype(BF16)
        return lax.dot_general(
            count_rows[...], counted[...], (((1,), (1,)), ((), ())), preferred_element_type=F32
        )

    def forward(s, counts):
        with jax.named_scope("f_dot"):
            sums = band_sums(s, None if counts is None else 0)
        with jax.named_scope("f_place"):
            for v in range(VIEWS):
                for b, at, value in pairs(placed(sums, s, v, 0)):
                    high, low = in_two(value)
                    rows = slice(128 * v + at, 128 * v + at + 16)
                    window[rows, 256 * b : 256 * b + 128] = high.astype(BF16)
                    window[rows, 256 * b + 128 : 256 * b + 256] = low.astype(BF16)
        with jax.named_scope("f_mix"):
            if counts is None:
                counts = count_columns(s, sums, 1)
            mixed = lax.dot_general(
                mixer[...], window[...], (((1,), (1,)), ((), ())), preferred_element_type=F32
            )
            mixed = mixed[0:ROWS] + mixed[ROWS : 2 * ROWS] + counts
            for v in range(VIEWS):
                columns = slice(128 * v, 128 * v + 128)
                for k in range(GROUPS):
                    send_a[s, k, v] = mixed[16 * k : 16 * k + 16, columns]
                for e in range(2):
                    at = 16 * GROUPS + 8 * e
                    send_e[s, e, v] = mixed[at : at + 8, columns]
        with jax.named_scope("f_send"):
            for there, plane, e, group in ((below, g - 1, 0, GROUPS - 1), (above, g + 1, 1, 0)):
                @pl.when(there)
                def _():
                    for v in range(VIEWS):
                        remote(
                            send_e.at[s, e, v], recv_e.at[s, j], sem_as.at[2 + s], sem_ah.at[s],
                            plane, 2 * (GROUPS * v + group) + 1,
                        )
            to_owners(
                lambda o: send_a.at[s, lax.rem(o, GROUPS), lax.div(o, GROUPS)],
                recv_a.at[s, j], sem_as.at[s], sem_ar.at[s],
            )

            @pl.when(owner)
            def _():
                recv_a[s, j] = send_a[s, own_group, own_view]

    def prepare_owner():
        arrived(recv_m.at[0 : xy - 1], sem_mr)
        for block in range(blocks):
            first, last = 128 * block, 128 * block + 128
            for s in range(SUBSETS):
                value = jnp.zeros((8, 128), F32)
                for i in range(first // COLS_DEV, min(xy, -(-last // COLS_DEV))):
                    low, high = max(COLS_DEV * i, first) - first, min(COLS_DEV * (i + 1), last) - first
                    piece = recv_m[i, 8 * s : 8 * s + 8, :]
                    value = jnp.where(jnp.logical_and(lane >= low, lane < high), piece, value)
                meas_rows[s, block] = value

    def window_starts(s):
        cosine, sine = trig[s, own_view, 0], trig[s, own_view, 1]

        def one(i, carry):
            x = jnp.full((8, 128), i * X_DEV, jnp.int32).astype(F32) + ((X_DEV - 1) / 2.0 - (nx_all - 1) / 2.0)
            starts[s, i] = jnp.floor(project(x, 0.0, cosine, sine)) - 128.0
            return carry

        lax.fori_loop(0, xy, one, 0)

    def reach(i):
        far = max(abs(X_DEV * i - (nx_all - 1) / 2.0), abs(X_DEV * i + X_DEV - 1 - (nx_all - 1) / 2.0))
        radius = math.hypot(far, (ny_all - 1) / 2.0)
        span = scale * radius / math.sqrt(1.0 - (radius / source) ** 2) + 2.0
        return max(0, int((middle - span) // 128)), min(blocks - 1, int((middle + span) // 128))

    edge_ids = [(256 * m + 128 * (sub // EDGE) + lane).astype(F32) for m in range(blocks // 2)]
    edge_slot = jnp.where(last_group, EDGE_SLOT, 0)

    def within(ids, start):
        return jnp.abs(ids - (start + 127.5)) < 128.0

    def choose(ids, values, candidates, start):
        message = None
        for m in reversed(candidates):
            message = values[m] if message is None else jnp.where(ids[m] >= start, values[m], message)
        return jnp.zeros((8, 128), F32) if message is None else message

    def owner_work(s):
        with jax.named_scope("wait_a"):
            arrived(recv_a.at[s, 0 : xy - 1], sem_ar.at[s])
        with jax.named_scope("o_add"):
            sums = [jnp.zeros((8, 128), F32)] * blocks
            for i in range(xy):
                start = starts[s, i]
                parts = recv_a[s, i, 0:8, :], recv_a[s, i, 8:16, :]
                for m in range(reach(i)[0], reach(i)[1] + 1):
                    sums[m] = sums[m] + jnp.where(within(column_ids[m], start), parts[m % 2], 0.0)
            for m in range(blocks):
                total[m] = sums[m]

        @pl.when(has_beside)
        def _():
            with jax.named_scope("wait_h"):
                arrived(recv_e.at[s], sem_ah.at[s])
            with jax.named_scope("o_addh"):
                sums = [jnp.zeros((8, 128), F32)] * (blocks // 2)
                for i in range(xy):
                    start = starts[s, i]
                    message = recv_e[s, i]
                    for m in range(reach(i)[0] // 2, reach(i)[1] // 2 + 1):
                        sums[m] = sums[m] + jnp.where(within(edge_ids[m], start), message, 0.0)
                for m in range(blocks // 2):
                    low = jnp.where(sub < EDGE, sums[m], 0.0)
                    total[2 * m] = total[2 * m] + pltpu.roll(low, edge_slot, 0)
                    total[2 * m + 1] = total[2 * m + 1] + pltpu.roll(sums[m] - low, edge_slot + EDGE, 0)

        with jax.named_scope("o_give"):
            residuals = []
            for m in range(blocks):
                value = total[m]
                columns = jnp.broadcast_to(value[7:8, :], (8, 128))
                residual = meas_rows[s, m] - value / jnp.maximum(ray_row * columns, 1.0)
                residual = jnp.where(own_slot, residual, 0.0)
                total[m] = residual
                residuals.append(rounded(residual))
            for i in range(xy):
                start = starts[s, i]
                parts = []
                for b in range(2):
                    candidates = [m for m in range(reach(i)[0], reach(i)[1] + 1) if m % 2 == b]
                    parts.append(choose(column_ids, residuals, candidates, start))
                send_c[s, i] = jnp.concatenate(parts, axis=0).astype(BF16)

        with jax.named_scope("o_send"):
            for t in range(1, xy):
                i = next_device(t)
                remote(send_c.at[s, i], recv_c.at[s, chip], sem_cs.at[s], sem_cr.at[s], g, i)
            recv_c[s, chip] = send_c[s, j]

        @pl.when(has_beside)
        def _():
            with jax.named_scope("o_giveh"):
                back = lax.rem(8 - edge_slot, 8)
                edges = [
                    jnp.where(
                        sub < EDGE,
                        pltpu.roll(rounded(total[2 * m]), back, 0),
                        pltpu.roll(rounded(total[2 * m + 1]), lax.rem(back + EDGE, 8), 0),
                    )
                    for m in range(blocks // 2)
                ]
                for i in range(xy):
                    candidates = list(range(reach(i)[0] // 2, reach(i)[1] // 2 + 1))
                    send_f[s, i] = choose(edge_ids, edges, candidates, starts[s, i]).astype(BF16)
            with jax.named_scope("o_sendh"):
                plane = jnp.where(last_group, g + 1, g - 1)
                slot = jnp.where(last_group, 0, 1)
                for t in range(xy):
                    i = next_device(t)
                    remote(
                        send_f.at[s, i], recv_f.at[s, slot, own_view], sem_cs.at[2 + s], sem_ch.at[s, slot], plane, i
                    )

    def owner_give_residual():
        for i in range(xy):
            first = COLS_DEV * i // 128
            message = total[first]
            if first + 1 < blocks:
                message = jnp.where(lane >= COLS_DEV * i % 128, message, total[first + 1])
            send_d[i] = message
        for t in range(1, xy):
            i = next_device(t)
            remote(send_d.at[i], recv_d.at[chip], sem_ds, sem_dr, g, i)
        recv_d[chip] = send_d[j]

    def backward(s):
        @pl.when(jnp.logical_not(below))
        def _():
            recv_f[s, 0] = jnp.zeros((VIEWS, 8, 128), BF16)

        @pl.when(jnp.logical_not(above))
        def _():
            recv_f[s, 1] = jnp.zeros((VIEWS, 8, 128), BF16)

        with jax.named_scope("wait_c"):
            with_owners(recv_c.at[s], sem_cr.at[s])

        with jax.named_scope("wait_ch"):
            @pl.when(below)
            def _():
                arrived(recv_f.at[s, 0], sem_ch.at[s, 0])

            @pl.when(above)
            def _():
                arrived(recv_f.at[s, 1], sem_ch.at[s, 1])

        with jax.named_scope("b_smear"):
            columns = []
            for v in range(VIEWS):
                rows = [recv_c[s, GROUPS * v + k].astype(F32) for k in range(GROUPS)]
                rows = rows + [recv_f[s, e, v].astype(F32) for e in range(2)]
                columns.append(jnp.transpose(jnp.concatenate(rows + rows, axis=0)).astype(BF16))
            smeared = rounded(
                lax.dot_general(
                    jnp.concatenate(columns, axis=0), smearer[...], (((1,), (0,)), ((), ())),
                    preferred_element_type=F32,
                )
            )
            for v in range(VIEWS):
                whole = [
                    smeared[128 * v + 8 * i : 128 * v + 8 * i + 8, 128 * p : 128 * p + 128]
                    for p in range(2)
                    for i in range(16)
                ]
                for h in range(2):
                    offset = shift[s, v, h]
                    now = whole
                    for bit in (128, 64, 32, 16, 8):
                        step = bit // 8
                        moved = (offset & bit) != 0
                        now = [
                            jnp.where(moved, now[(i + step) % 32], now[i]) for i in range(WIN // 8 + step - 1)
                        ]
                    for i in range(WIN // 8):
                        turned[h, v * WIN + 8 * i : v * WIN + 8 * i + 8, :] = now[i]
        with jax.named_scope("b_turn"):
            sides = [jnp.transpose(turned[h]).astype(BF16) for h in range(2)]
        last = s == SUBSETS - 1
        per_step = 4

        def one(step, carry):
            for h in range(2):
                columns = pl.ds(pl.multiple_of(step * (128 * per_step), 128 * per_step), 128 * per_step)
                back = lax.dot_general(
                    sides[h], weights[2 * s + h, :, columns], (((1,), (0,)), ((), ())),
                    preferred_element_type=F32,
                )
                for part in range(per_step):
                    x = per_step * step + part
                    mine = back[112:128, 128 * part : 128 * part + 128]
                    for q in range(6, -1, -1):
                        mine = jnp.where(
                            jnp.concatenate([band, band], axis=0) == q,
                            back[16 * q : 16 * q + 16, 128 * part : 128 * part + 128], mine,
                        )
                    norm = slice_total * ws[s, pl.ds(HALF * h + x, 1), :]
                    at = pl.ds(HALF * h + x, 16, stride=X_DEV)
                    new = it[at, :] + mine / jnp.maximum(norm, 1.0)
                    if last:
                        out_ref[at, :] = new
                    else:
                        it[at, :] = new
                        spread(new, h, x)
            return carry

        with jax.named_scope("b_loop"):
            lax.fori_loop(0, HALF // per_step, one, 0)

    with jax.named_scope("send_m"):
        send_measured()
    forward(0, None)

    @pl.when(owner)
    def _():
        with jax.named_scope("prep"):
            prepare_owner()
            window_starts(0)
        owner_work(0)

    with jax.named_scope("gw1"):
        geometry(1)
        make_weights(1)
        counted_ahead[...] = count_columns(1, band_sums(1, 1), 0)

    @pl.when(owner)
    def _():
        window_starts(1)

    backward(0)
    forward(1, counted_ahead[...])

    @pl.when(owner)
    def _():
        owner_work(1)
        with jax.named_scope("give"):
            owner_give_residual()

    backward(1)

    with jax.named_scope("tail"):
        with_owners(recv_d, sem_dr)
        turn_back = lax.rem(128 - lax.rem(j * COLS_DEV, 128), 128)
        for v in range(VIEWS):
            for k in range(GROUPS):
                message = pltpu.roll(recv_d[GROUPS * v + k], turn_back, 1)
                resid_ref[v, SLOTS * k : SLOTS * k + SIZES[k], :] = message[0 : SIZES[k], 0:COLS_DEV]

        with_owners(send_m, sem_ms)
        for s in range(SUBSETS):
            with_owners(recv_a.at[s], sem_as.at[s])

            @pl.when(below)
            def _():
                arrived(send_e.at[s, 0], sem_as.at[2 + s])

            @pl.when(above)
            def _():
                arrived(send_e.at[s, 1], sem_as.at[2 + s])

            @pl.when(owner)
            def _():
                arrived(send_c.at[s, 0 : xy - 1], sem_cs.at[s])

            @pl.when(has_beside)
            def _():
                arrived(send_f.at[s], sem_cs.at[2 + s])

        @pl.when(owner)
        def _():
            arrived(send_d.at[0 : xy - 1], sem_ds)


def local(gz, xy, volume, measured, view_order):
    blocks = COLS_DEV * xy // 128
    dma = pltpu.SemaphoreType.DMA
    vmem = pltpu.VMEM
    out, resid = pl.pallas_call(
        functools.partial(kernel, gz, xy),
        out_shape=(
            pltpu.VMEM((Z_DEV * X_DEV, NY), F32),
            pltpu.VMEM((VIEWS, ROWS_DEV, COLS_DEV), F32),
        ),
        in_specs=[pl.BlockSpec(memory_space=pl.ANY)] * 3,
        out_specs=(pl.BlockSpec(memory_space=pltpu.VMEM), pl.BlockSpec(memory_space=pltpu.VMEM)),
        scratch_shapes=[
            pltpu.SMEM((ANGLES,), jnp.int32),
            vmem((Z_DEV * X_DEV, NY), F32),
            vmem((VIEWS, ROWS_DEV, SUBSETS, COLS_DEV), F32),
            vmem((SUBSETS, VIEWS, X_DEV, NY), F32),
            vmem((SUBSETS, VIEWS, X_DEV, NY), F32),
            vmem((SUBSETS, VIEWS, X_DEV, NY), F32),
            vmem((SUBSETS, X_DEV, NY), F32),
            vmem((SUBSETS, VIEWS, 2, 8, 128), jnp.int32),
            vmem((SUBSETS, VIEWS, 2, 8, 128), F32),
            vmem((2 * SUBSETS, VIEWS * WIN, HALF * NY), BF16),
            vmem((2, 256, HALF * NY), BF16),
            vmem((VIEWS * 128, 512), BF16),
            vmem((VIEWS * 128, 256), BF16),
            vmem((ROWS, VIEWS * 128), F32),
            vmem((ROWS, 256), BF16),
            vmem((2 * ROWS, 512), BF16),
            vmem((2 * ROWS, 256), BF16),
            vmem((OWNERS, 16, 128), F32),
            vmem((xy, 16, 128), F32),
            vmem((SUBSETS, blocks, 8, 128), F32),
            vmem((SUBSETS, GROUPS, VIEWS, 16, 128), F32),
            vmem((SUBSETS, xy, 16, 128), F32),
            vmem((SUBSETS, 2, VIEWS, 8, 128), F32),
            vmem((SUBSETS, xy, 8, 128), F32),
            vmem((SUBSETS, xy, 8, 128), F32),
            vmem((blocks, 8, 128), F32),
            vmem((SUBSETS, xy, 16, 128), BF16),
            vmem((SUBSETS, OWNERS, 16, 128), BF16),
            vmem((SUBSETS, xy, 8, 128), BF16),
            vmem((SUBSETS, 2, VIEWS, 8, 128), BF16),
            vmem((xy, 8, 128), F32),
            vmem((OWNERS, 8, 128), F32),
            vmem((2, VIEWS * WIN, 128), F32),
            dma(()), dma(()), dma(()), dma(()), dma(()), dma((4,)), dma((2,)), dma((2,)),
            dma((4,)), dma((2,)), dma((2, 2)), dma(()), dma(()),
        ],
        compiler_params=pltpu.CompilerParams(collective_id=0, has_side_effects=True),
    )(view_order, volume.reshape(Z_DEV * X_DEV, NY), measured.transpose(1, 2, 0, 3))
    return out.reshape(Z_DEV, X_DEV, NY), resid


def solution(mesh):
    in_specs = (P("gz", "xy", None), P(None, None, "gz", "xy"), P())
    out_specs = (P("gz", "xy", None), P(None, "gz", "xy"))
    body = functools.partial(local, mesh.shape["gz"], mesh.shape["xy"])
    return jax.shard_map(body, mesh=mesh, in_specs=in_specs, out_specs=out_specs, check_vma=False)
```

```python
import functools
import math

import jax
import jax.numpy as jnp
from jax import lax
from jax.experimental import pallas as pl
from jax.experimental.pallas import tpu as pltpu
from jax.sharding import PartitionSpec as P

Z_DEV = 16
X_DEV = 48
COLS_DEV = 48
NY = 128
VIEWS = 5
SUBSETS = 2
ANGLES = 48
ROWS_DEV = 20
HALF = X_DEV // 2
WIN = 48
GROUPS = 3
SLOTS = 7
SIZES = (7, 7, 6)
OWNERS = VIEWS * GROUPS
SIDE = 4
EDGE = 4
EDGE_SLOT = ROWS_DEV - EDGE - SLOTS * (GROUPS - 1)
ROWS = 16 * GROUPS + 16
MESH = pl.DeviceIdType.MESH
F32 = jnp.float32
BF16 = jnp.bfloat16


def iota(shape, dim):
    return lax.broadcasted_iota(jnp.int32, shape, dim)


def kernel(
    gz, xy, view_hbm, vol_ref, meas_hbm, out_ref, resid_ref,
    views, it, meas, low_id, low_w, high_w, ws, shift, trig, weights, data, window, counted, counted_ahead, count_rows, mixer, smearer,
    send_m, recv_m, meas_rows, send_a, recv_a, send_e, recv_e, starts, total, send_c, recv_c, send_f, recv_f,
    send_d, recv_d, turned,
    sem_view, sem_vol, sem_meas, sem_ms, sem_mr, sem_as, sem_ar, sem_ah, sem_cs, sem_cr, sem_ch, sem_ds, sem_dr,
):
    g = lax.axis_index("gz")
    j = lax.axis_index("xy")
    nx_all, ny_all, dc_all = X_DEV * xy, NY, COLS_DEV * xy
    dr_all, nz_all = ROWS_DEV * gz, Z_DEV * gz
    blocks = dc_all // 128
    chip = lax.div(j, 2)
    owner = jnp.logical_and(lax.rem(j, 2) == 1, chip < OWNERS)
    own_view = lax.rem(lax.div(chip, GROUPS), VIEWS)
    own_group = lax.rem(chip, GROUPS)
    first_group = jnp.logical_and(owner, own_group == 0)
    last_group = jnp.logical_and(owner, own_group == GROUPS - 1)
    below, above = g > 0, g < gz - 1
    give_down = jnp.logical_and(first_group, below)
    give_up = jnp.logical_and(last_group, above)
    has_beside = jnp.logical_or(give_down, give_up)

    view_copy = pltpu.make_async_copy(view_hbm, views, sem_view)
    vol_copy = pltpu.make_async_copy(vol_ref, it, sem_vol)
    meas_copy = pltpu.make_async_copy(meas_hbm, meas, sem_meas)
    view_copy.start()
    vol_copy.start()
    meas_copy.start()

    barrier = pltpu.get_barrier_semaphore()

    def greet(plane, device):
        pl.semaphore_signal(barrier, inc=1, device_id=(plane, device), device_id_type=MESH)

    def greet_all(plane):
        for i in range(xy):
            greet(plane, i)

    def next_owner(t):
        return 2 * lax.rem(chip + t, OWNERS) + 1

    def next_device(t):
        return lax.rem(j + t, xy)

    steps = sorted(
        ((a, b, c) for a in range(SIDE) for b in range(SIDE) for c in (1, 0)),
        key=lambda step: -sum(min(d, SIDE - d) for d in step[:2]),
    )

    def moved_chip(a, b):
        return SIDE * lax.rem(lax.div(chip, SIDE) + a, SIDE) + lax.rem(chip + b, SIDE)

    def moved_device(step):
        return 2 * moved_chip(step[0], step[1]) + lax.rem(j + step[2], 2)

    with jax.named_scope("greet"):
        @pl.when(owner)
        def _():
            for t in range(1, xy):
                greet(g, next_device(t))

        @pl.when(jnp.logical_not(owner))
        def _():
            for t in range(OWNERS):
                greet(g, next_owner(t))

        @pl.when(give_down)
        def _():
            greet_all(g - 1)

        @pl.when(jnp.logical_and(below, jnp.logical_not(first_group)))
        def _():
            for v in range(VIEWS):
                greet(g - 1, 2 * (GROUPS * v + GROUPS - 1) + 1)

        @pl.when(give_up)
        def _():
            greet_all(g + 1)

        @pl.when(jnp.logical_and(above, jnp.logical_not(last_group)))
        def _():
            for v in range(VIEWS):
                greet(g + 1, 2 * GROUPS * v + 1)

    greeted = (
        jnp.where(owner, xy - 1, OWNERS)
        + jnp.where(below, jnp.where(first_group, xy, VIEWS), 0)
        + jnp.where(above, jnp.where(last_group, xy, VIEWS), 0)
    )

    lane = iota((8, 128), 1)
    sub = iota((8, 128), 0)
    lane_f = lane.astype(F32)
    sub_f = sub.astype(F32)
    band = lane // 16
    source = 2.0 * nx_all
    scale = 0.9 * (dc_all / nx_all)
    middle = (dc_all - 1) / 2.0
    x_first = (j * X_DEV).astype(F32)

    def project(x, y, cosine, sine):
        along = x * cosine + y * sine
        depth = y * cosine - x * sine
        return middle + scale * along * source / (source + depth)

    def hat(row, slice_id):
        position = (dr_all - 1) / 2.0 + 0.96 * (dr_all / nz_all) * (slice_id - (nz_all - 1) / 2.0)
        return jnp.maximum(0.0, 1.0 - jnp.abs(position - row) / 2.0)

    def rounded(x):
        return x.astype(BF16).astype(F32)

    def in_two(x):
        high = rounded(x)
        return high, x - high

    def geometry(s):
        for v in range(VIEWS):
            number = jnp.full((8, 128), views[s * VIEWS + v], jnp.int32).astype(F32)
            angle = 2.0 * math.pi * number / ANGLES
            cosine, sine = jnp.cos(angle), jnp.sin(angle)
            trig[s, v, 0] = cosine
            trig[s, v, 1] = sine
            y_low = (band * 16).astype(F32) - (ny_all - 1) / 2.0
            base = []
            for h in range(2):
                x_low = (x_first + HALF * h) - (nx_all - 1) / 2.0
                corners = [
                    project(x, y, cosine, sine)
                    for x in (x_low, x_low + (HALF - 1))
                    for y in (y_low, y_low + 15.0)
                ]
                lowest = jnp.minimum(jnp.minimum(corners[0], corners[1]), jnp.minimum(corners[2], corners[3]))
                start = jnp.floor((lowest - 0.03125) * 0.125) * 8.0
                base.append(start)
                shift[s, v, h] = (start - 256.0 * jnp.floor(start * (1.0 / 256.0))).astype(jnp.int32)
            for block in range(X_DEV // 8):
                x = (x_first + (8.0 * block + sub_f)) - (nx_all - 1) / 2.0
                y = lane_f - (ny_all - 1) / 2.0
                u = project(x, y, cosine, sine)
                low = jnp.floor(u)
                first = rounded(jnp.maximum(0.0, 1.0 - jnp.abs(u - low)))
                second = rounded(jnp.maximum(0.0, 1.0 - jnp.abs(u - (low + 1.0))))
                both = first + second
                rows = slice(8 * block, 8 * block + 8)
                low_id[s, v, rows, :] = low - base[block // (HALF // 8)]
                low_w[s, v, rows, :] = first
                high_w[s, v, rows, :] = second
                ws[s, rows, :] = both if v == 0 else ws[s, rows, :] + both

    window_ids = [(iota((16, 128), 0) + 16 * t).astype(F32).astype(BF16) for t in range(WIN // 16)]
    window_ids_less = [(iota((16, 128), 0) + (16 * t - 1)).astype(F32).astype(BF16) for t in range(WIN // 16)]

    def make_weights(s):
        def one(x, carry):
            for h in range(2):
                for v in range(VIEWS):
                    row = pl.ds(HALF * h + x, 1)
                    at, first, second = (
                        jnp.broadcast_to(ref[s, v, row, :], (16, 128)).astype(BF16) for ref in (low_id, low_w, high_w)
                    )
                    for t in range(WIN // 16):
                        w = jnp.where(window_ids[t] == at, first, jnp.zeros_like(first))
                        w = jnp.where(window_ids_less[t] == at, second, w)
                        weights[2 * s + h, x, v * WIN + 16 * t : v * WIN + 16 * t + 16, :] = w
            return carry

        lax.fori_loop(0, HALF, one, 0)

    band_masks = [(iota((16, 128), 1) // 16 == q).astype(F32).astype(BF16) for q in range(8)]

    def spread(values, h, x):
        values = values.astype(BF16)
        for q in range(8):
            data[h, x, 16 * q : 16 * q + 16, :] = values * band_masks[q]

    def row_tables():
        shape = (ROWS, 128)
        at = iota(shape, 0)
        own = at < 16 * GROUPS
        half = jnp.where(own, (at // 8) % 2, (at // 4) % 2)
        slot = jnp.where(own, at % 8, at % 4)
        edge = jnp.where(at < 16 * GROUPS + 8, -EDGE, ROWS_DEV)
        row = slot + jnp.where(own, SLOTS * (at // 16), edge)
        size = jnp.where(at // 16 == GROUPS - 1, SIZES[-1], SLOTS)
        row_all = g * ROWS_DEV + row
        inside = jnp.logical_and(jnp.logical_and(row_all >= 0, row_all < dr_all), slot < size)
        slice_all = (g * Z_DEV + iota(shape, 1) % 16).astype(F32)
        row_hat = jnp.where(inside, hat(row_all.astype(F32), slice_all), 0.0)
        counts = jnp.where(jnp.logical_and(jnp.logical_and(own, slot == 7), iota(shape, 1) % 16 < 2), 1.0, 0.0)
        for b in range(2):
            mine = half == b
            high, low = in_two(jnp.where(mine, row_hat, 0.0))
            smearer[0:ROWS, 128 * b : 128 * b + 128] = high.astype(BF16)
            smearer[ROWS : 2 * ROWS, 128 * b : 128 * b + 128] = low.astype(BF16)
            for part in range(2):
                columns = slice(256 * b + 128 * part, 256 * b + 128 * part + 128)
                mixer[0:ROWS, columns] = high.astype(BF16)
                mixer[ROWS : 2 * ROWS, columns] = low.astype(BF16)
            count_rows[:, 128 * b : 128 * b + 128] = jnp.where(mine, counts, 0.0).astype(BF16)

    slices = (g * Z_DEV + iota((16, 128), 0)).astype(F32)
    slice_total = jnp.zeros((16, 1), F32)
    for part in range(-(-dr_all // 128)):
        rows = 128 * part + iota((16, 128), 1)
        weight = jnp.where(rows < dr_all, hat(rows.astype(F32), slices), 0.0)
        slice_total = slice_total + jnp.sum(weight, axis=1, keepdims=True)
    slice_total = jnp.broadcast_to(slice_total, (16, 128))
    own_row = (g * ROWS_DEV + own_group * SLOTS + sub).astype(F32)
    ray_row = jnp.zeros((8, 1), F32)
    for part in range(-(-nz_all // 128)):
        ids = 128 * part + lane
        weight = jnp.where(ids < nz_all, hat(own_row, ids.astype(F32)), 0.0)
        ray_row = ray_row + jnp.sum(weight, axis=1, keepdims=True)
    ray_row = jnp.broadcast_to(ray_row, (8, 128))
    own_slot = sub < jnp.where(own_group == GROUPS - 1, SIZES[-1], SLOTS)
    column_ids = [(128 * m + lane).astype(F32) for m in range(blocks)]

    def remote(src, dst, send_sem, recv_sem, plane, device):
        pltpu.make_async_remote_copy(
            src_ref=src, dst_ref=dst, send_sem=send_sem, recv_sem=recv_sem,
            device_id=(plane, device), device_id_type=MESH,
        ).start()

    def arrived(ref, sem):
        pltpu.make_async_copy(ref, ref, sem).wait()

    def to_owners(src, dst, send_sem, recv_sem):
        for a, b, c in steps:
            if c:
                there = moved_chip(a, b)
                wanted = there < OWNERS
                if a == b == 0:
                    wanted = jnp.logical_and(wanted, jnp.logical_not(owner))

                @pl.when(wanted)
                def _():
                    remote(src(there), dst, send_sem, recv_sem, g, 2 * there + 1)

    def with_owners(ref, sem):
        @pl.when(owner)
        def _():
            arrived(ref.at[0 : OWNERS - 1], sem)

        @pl.when(jnp.logical_not(owner))
        def _():
            arrived(ref.at[0:OWNERS], sem)

    def table(x, carry):
        for h in range(2):
            for q in range(8):
                pair = iota((16, 128), 0) < 2
                row = jnp.where(jnp.logical_and(pair, iota((16, 128), 1) // 16 == q), 1.0, 0.0)
                data[h, x, 128 + 16 * q : 128 + 16 * q + 16, :] = row.astype(BF16)
        return carry

    def fill_data(x, carry):
        for h in range(2):
            spread(it[pl.ds(HALF * h + x, 16, stride=X_DEV), :], h, x)
        return carry

    view_copy.wait()
    with jax.named_scope("geom0"):
        geometry(0)
    with jax.named_scope("mw0"):
        make_weights(0)
    with jax.named_scope("tables"):
        row_tables()
        lax.fori_loop(0, HALF, table, 0)
    with jax.named_scope("fill"):
        vol_copy.wait()
        lax.fori_loop(0, HALF, fill_data, 0)

    with jax.named_scope("measured"):
        meas_copy.wait()
        turn = lax.rem(j * COLS_DEV, 128)
        for v in range(VIEWS):
            for k in range(GROUPS):
                o = GROUPS * v + k
                send_m[o] = jnp.zeros((16, 128), F32)
                for s in range(SUBSETS):
                    for slot in range(SIZES[k]):
                        send_m[o, 8 * s + slot, 0:COLS_DEV] = meas[v, SLOTS * k + slot, s, :]
        for o in range(OWNERS):
            send_m[o] = pltpu.roll(send_m[o], turn, 1)

    with jax.named_scope("barrier"):
        pl.semaphore_wait(barrier, greeted)

    def send_measured():
        to_owners(lambda o: send_m.at[o], recv_m.at[j], sem_ms, sem_mr)

        @pl.when(owner)
        def _():
            recv_m[j] = send_m[chip]

    def placed(sums, s, v, part):
        halves = []
        for h in range(2):
            offset = shift[s, v, h]
            rows = [
                sums[h][v * WIN + 8 * i : v * WIN + 8 * i + 8, 128 * part : 128 * part + 128] for i in range(WIN // 8)
            ] + [None] * (32 - WIN // 8)
            for bit in (8, 16, 32, 64, 128):
                moved = (offset & bit) != 0
                step = bit // 8
                new = []
                for i in range(32):
                    old, other = rows[i], rows[(i - step) % 32]
                    if old is None and other is None:
                        new.append(None)
                    elif old is None:
                        new.append(jnp.where(moved, other, 0.0))
                    elif other is None:
                        new.append(jnp.where(moved, 0.0, old))
                    else:
                        new.append(jnp.where(moved, other, old))
                rows = new
            halves.append(rows)
        return [a + b for a, b in zip(*halves)]

    def pairs(pieces):
        for i in range(0, 32, 2):
            yield i // 16, 8 * (i % 16), jnp.concatenate([pieces[i], pieces[i + 1]], axis=0)

    def beside(ref, at, first, count, rows=slice(None)):
        return jnp.concatenate([ref[at, x, rows, :] for x in range(first, first + count)], axis=1)

    def band_sums(s, part):
        rows = slice(0, 256) if part is None else slice(128 * part, 128 * part + 128)
        return [
            lax.dot_general(
                beside(weights, 2 * s + h, 0, HALF), beside(data, h, 0, HALF, rows),
                (((1,), (1,)), ((), ())), preferred_element_type=F32,
            )
            for h in range(2)
        ]

    first_lane = iota((16, 128), 1) % 16 == 0

    def count_columns(s, sums, part):
        for v in range(VIEWS):
            for b, at, value in pairs(placed(sums, s, v, part)):
                high, low = in_two(value)
                counted[128 * v + at : 128 * v + at + 16, 128 * b : 128 * b + 128] = jnp.where(
                    first_lane, high, low
                ).astype(BF16)
        return lax.dot_general(
            count_rows[...], counted[...], (((1,), (1,)), ((), ())), preferred_element_type=F32
        )

    def forward(s, counts):
        with jax.named_scope("f_dot"):
            sums = band_sums(s, None if counts is None else 0)
        with jax.named_scope("f_place"):
            for v in range(VIEWS):
                for b, at, value in pairs(placed(sums, s, v, 0)):
                    high, low = in_two(value)
                    rows = slice(128 * v + at, 128 * v + at + 16)
                    window[rows, 256 * b : 256 * b + 128] = high.astype(BF16)
                    window[rows, 256 * b + 128 : 256 * b + 256] = low.astype(BF16)
        with jax.named_scope("f_mix"):
            if counts is None:
                counts = count_columns(s, sums, 1)
            mixed = lax.dot_general(
                mixer[...], window[...], (((1,), (1,)), ((), ())), preferred_element_type=F32
            )
            mixed = mixed[0:ROWS] + mixed[ROWS : 2 * ROWS] + counts
            for v in range(VIEWS):
                columns = slice(128 * v, 128 * v + 128)
                for k in range(GROUPS):
                    send_a[s, k, v] = mixed[16 * k : 16 * k + 16, columns]
                for e in range(2):
                    at = 16 * GROUPS + 8 * e
                    send_e[s, e, v] = mixed[at : at + 8, columns]
        with jax.named_scope("f_send"):
            for there, plane, e, group in ((below, g - 1, 0, GROUPS - 1), (above, g + 1, 1, 0)):
                @pl.when(there)
                def _():
                    for v in range(VIEWS):
                        remote(
                            send_e.at[s, e, v], recv_e.at[s, j], sem_as.at[2 + s], sem_ah.at[s],
                            plane, 2 * (GROUPS * v + group) + 1,
                        )
            to_owners(
                lambda o: send_a.at[s, lax.rem(o, GROUPS), lax.div(o, GROUPS)],
                recv_a.at[s, j], sem_as.at[s], sem_ar.at[s],
            )

            @pl.when(owner)
            def _():
                recv_a[s, j] = send_a[s, own_group, own_view]

    def prepare_owner():
        arrived(recv_m.at[0 : xy - 1], sem_mr)
        for block in range(blocks):
            first, last = 128 * block, 128 * block + 128
            for s in range(SUBSETS):
                value = jnp.zeros((8, 128), F32)
                for i in range(first // COLS_DEV, min(xy, -(-last // COLS_DEV))):
                    low, high = max(COLS_DEV * i, first) - first, min(COLS_DEV * (i + 1), last) - first
                    piece = recv_m[i, 8 * s : 8 * s + 8, :]
                    value = jnp.where(jnp.logical_and(lane >= low, lane < high), piece, value)
                meas_rows[s, block] = value

    def window_starts(s):
        cosine, sine = trig[s, own_view, 0], trig[s, own_view, 1]

        def one(i, carry):
            x = jnp.full((8, 128), i * X_DEV, jnp.int32).astype(F32) + ((X_DEV - 1) / 2.0 - (nx_all - 1) / 2.0)
            starts[s, i] = jnp.floor(project(x, 0.0, cosine, sine)) - 128.0
            return carry

        lax.fori_loop(0, xy, one, 0)

    def reach(i):
        far = max(abs(X_DEV * i - (nx_all - 1) / 2.0), abs(X_DEV * i + X_DEV - 1 - (nx_all - 1) / 2.0))
        radius = math.hypot(far, (ny_all - 1) / 2.0)
        span = scale * radius / math.sqrt(1.0 - (radius / source) ** 2) + 2.0
        return max(0, int((middle - span) // 128)), min(blocks - 1, int((middle + span) // 128))

    edge_ids = [(256 * m + 128 * (sub // EDGE) + lane).astype(F32) for m in range(blocks // 2)]
    edge_slot = jnp.where(last_group, EDGE_SLOT, 0)

    def within(ids, start):
        return jnp.abs(ids - (start + 127.5)) < 128.0

    def choose(ids, values, candidates, start):
        message = None
        for m in reversed(candidates):
            message = values[m] if message is None else jnp.where(ids[m] >= start, values[m], message)
        return jnp.zeros((8, 128), F32) if message is None else message

    def owner_work(s):
        with jax.named_scope("wait_a"):
            arrived(recv_a.at[s, 0 : xy - 1], sem_ar.at[s])
        with jax.named_scope("o_add"):
            sums = [jnp.zeros((8, 128), F32)] * blocks
            for i in range(xy):
                start = starts[s, i]
                parts = recv_a[s, i, 0:8, :], recv_a[s, i, 8:16, :]
                for m in range(reach(i)[0], reach(i)[1] + 1):
                    sums[m] = sums[m] + jnp.where(within(column_ids[m], start), parts[m % 2], 0.0)
            for m in range(blocks):
                total[m] = sums[m]

        @pl.when(has_beside)
        def _():
            with jax.named_scope("wait_h"):
                arrived(recv_e.at[s], sem_ah.at[s])
            with jax.named_scope("o_addh"):
                sums = [jnp.zeros((8, 128), F32)] * (blocks // 2)
                for i in range(xy):
                    start = starts[s, i]
                    message = recv_e[s, i]
                    for m in range(reach(i)[0] // 2, reach(i)[1] // 2 + 1):
                        sums[m] = sums[m] + jnp.where(within(edge_ids[m], start), message, 0.0)
                for m in range(blocks // 2):
                    low = jnp.where(sub < EDGE, sums[m], 0.0)
                    total[2 * m] = total[2 * m] + pltpu.roll(low, edge_slot, 0)
                    total[2 * m + 1] = total[2 * m + 1] + pltpu.roll(sums[m] - low, edge_slot + EDGE, 0)

        with jax.named_scope("o_give"):
            residuals = []
            for m in range(blocks):
                value = total[m]
                columns = jnp.broadcast_to(value[7:8, :], (8, 128))
                residual = meas_rows[s, m] - value / jnp.maximum(ray_row * columns, 1.0)
                residual = jnp.where(own_slot, residual, 0.0)
                total[m] = residual
                residuals.append(rounded(residual))
            for i in range(xy):
                start = starts[s, i]
                parts = []
                for b in range(2):
                    candidates = [m for m in range(reach(i)[0], reach(i)[1] + 1) if m % 2 == b]
                    parts.append(choose(column_ids, residuals, candidates, start))
                send_c[s, i] = jnp.concatenate(parts, axis=0).astype(BF16)

        @pl.when(has_beside)
        def _():
            with jax.named_scope("o_giveh"):
                back = lax.rem(8 - edge_slot, 8)
                edges = [
                    jnp.where(
                        sub < EDGE,
                        pltpu.roll(rounded(total[2 * m]), back, 0),
                        pltpu.roll(rounded(total[2 * m + 1]), lax.rem(back + EDGE, 8), 0),
                    )
                    for m in range(blocks // 2)
                ]
                for i in range(xy):
                    candidates = list(range(reach(i)[0] // 2, reach(i)[1] // 2 + 1))
                    send_f[s, i] = choose(edge_ids, edges, candidates, starts[s, i]).astype(BF16)
            with jax.named_scope("o_sendh"):
                plane = jnp.where(last_group, g + 1, g - 1)
                slot = jnp.where(last_group, 0, 1)
                for step in steps:
                    i = moved_device(step)
                    remote(
                        send_f.at[s, i], recv_f.at[s, slot, own_view], sem_cs.at[2 + s], sem_ch.at[s, slot], plane, i
                    )

        with jax.named_scope("o_send"):
            for step in steps:
                if step == (0, 0, 0):
                    continue
                i = moved_device(step)
                remote(send_c.at[s, i], recv_c.at[s, chip], sem_cs.at[s], sem_cr.at[s], g, i)
            recv_c[s, chip] = send_c[s, j]

    def owner_give_residual():
        for i in range(xy):
            first = COLS_DEV * i // 128
            message = total[first]
            if first + 1 < blocks:
                message = jnp.where(lane >= COLS_DEV * i % 128, message, total[first + 1])
            send_d[i] = message
        for t in range(1, xy):
            i = next_device(t)
            remote(send_d.at[i], recv_d.at[chip], sem_ds, sem_dr, g, i)
        recv_d[chip] = send_d[j]

    def backward(s):
        @pl.when(jnp.logical_not(below))
        def _():
            recv_f[s, 0] = jnp.zeros((VIEWS, 8, 128), BF16)

        @pl.when(jnp.logical_not(above))
        def _():
            recv_f[s, 1] = jnp.zeros((VIEWS, 8, 128), BF16)

        with jax.named_scope("wait_c"):
            with_owners(recv_c.at[s], sem_cr.at[s])

        with jax.named_scope("wait_ch"):
            @pl.when(below)
            def _():
                arrived(recv_f.at[s, 0], sem_ch.at[s, 0])

            @pl.when(above)
            def _():
                arrived(recv_f.at[s, 1], sem_ch.at[s, 1])

        with jax.named_scope("b_smear"):
            columns = []
            for v in range(VIEWS):
                rows = [recv_c[s, GROUPS * v + k].astype(F32) for k in range(GROUPS)]
                rows = rows + [recv_f[s, e, v].astype(F32) for e in range(2)]
                columns.append(jnp.transpose(jnp.concatenate(rows + rows, axis=0)).astype(BF16))
            smeared = rounded(
                lax.dot_general(
                    jnp.concatenate(columns, axis=0), smearer[...], (((1,), (0,)), ((), ())),
                    preferred_element_type=F32,
                )
            )
            for v in range(VIEWS):
                whole = [
                    smeared[128 * v + 8 * i : 128 * v + 8 * i + 8, 128 * p : 128 * p + 128]
                    for p in range(2)
                    for i in range(16)
                ]
                for h in range(2):
                    offset = shift[s, v, h]
                    now = whole
                    for bit in (128, 64, 32, 16, 8):
                        step = bit // 8
                        moved = (offset & bit) != 0
                        now = [
                            jnp.where(moved, now[(i + step) % 32], now[i]) for i in range(WIN // 8 + step - 1)
                        ]
                    for i in range(WIN // 8):
                        turned[h, v * WIN + 8 * i : v * WIN + 8 * i + 8, :] = now[i]
        with jax.named_scope("b_turn"):
            sides = [jnp.transpose(turned[h]).astype(BF16) for h in range(2)]
        last = s == SUBSETS - 1
        per_step = 2

        bands = jnp.concatenate([band, band], axis=0)

        def one(step):
            for h in range(2):
                back = lax.dot_general(
                    sides[h], beside(weights, 2 * s + h, per_step * step, per_step), (((1,), (0,)), ((), ())),
                    preferred_element_type=F32,
                )
                for part in range(per_step):
                    x = per_step * step + part
                    mine = back[112:128, 128 * part : 128 * part + 128]
                    for q in range(6, -1, -1):
                        mine = jnp.where(
                            bands == q, back[16 * q : 16 * q + 16, 128 * part : 128 * part + 128], mine
                        )
                    norm = slice_total * ws[s, HALF * h + x : HALF * h + x + 1, :]
                    at = pl.ds(HALF * h + x, 16, stride=X_DEV)
                    new = it[at, :] + mine / jnp.maximum(norm, 1.0)
                    if last:
                        out_ref[at, :] = new
                    else:
                        it[at, :] = new
                        spread(new, h, x)

        with jax.named_scope("b_loop"):
            for step in range(HALF // per_step):
                one(step)

    with jax.named_scope("send_m"):
        send_measured()
    forward(0, None)

    @pl.when(owner)
    def _():
        with jax.named_scope("prep"):
            prepare_owner()
            window_starts(0)
        owner_work(0)

    with jax.named_scope("gw1"):
        geometry(1)
        make_weights(1)
        counted_ahead[...] = count_columns(1, band_sums(1, 1), 0)

    @pl.when(owner)
    def _():
        window_starts(1)

    backward(0)
    forward(1, counted_ahead[...])

    @pl.when(owner)
    def _():
        owner_work(1)
        with jax.named_scope("give"):
            owner_give_residual()

    backward(1)

    with jax.named_scope("tail"):
        with_owners(recv_d, sem_dr)
        turn_back = lax.rem(128 - lax.rem(j * COLS_DEV, 128), 128)
        for v in range(VIEWS):
            for k in range(GROUPS):
                message = pltpu.roll(recv_d[GROUPS * v + k], turn_back, 1)
                resid_ref[v, SLOTS * k : SLOTS * k + SIZES[k], :] = message[0 : SIZES[k], 0:COLS_DEV]

        with_owners(send_m, sem_ms)
        for s in range(SUBSETS):
            with_owners(recv_a.at[s], sem_as.at[s])

            @pl.when(below)
            def _():
                arrived(send_e.at[s, 0], sem_as.at[2 + s])

            @pl.when(above)
            def _():
                arrived(send_e.at[s, 1], sem_as.at[2 + s])

            @pl.when(owner)
            def _():
                arrived(send_c.at[s, 0 : xy - 1], sem_cs.at[s])

            @pl.when(has_beside)
            def _():
                arrived(send_f.at[s], sem_cs.at[2 + s])

        @pl.when(owner)
        def _():
            arrived(send_d.at[0 : xy - 1], sem_ds)


def local(gz, xy, volume, measured, view_order):
    blocks = COLS_DEV * xy // 128
    dma = pltpu.SemaphoreType.DMA
    vmem = pltpu.VMEM
    out, resid = pl.pallas_call(
        functools.partial(kernel, gz, xy),
        out_shape=(
            pltpu.VMEM((Z_DEV * X_DEV, NY), F32),
            pltpu.VMEM((VIEWS, ROWS_DEV, COLS_DEV), F32),
        ),
        in_specs=[pl.BlockSpec(memory_space=pl.ANY)] * 3,
        out_specs=(pl.BlockSpec(memory_space=pltpu.VMEM), pl.BlockSpec(memory_space=pltpu.VMEM)),
        scratch_shapes=[
            pltpu.SMEM((ANGLES,), jnp.int32),
            vmem((Z_DEV * X_DEV, NY), F32),
            vmem((VIEWS, ROWS_DEV, SUBSETS, COLS_DEV), F32),
            vmem((SUBSETS, VIEWS, X_DEV, NY), F32),
            vmem((SUBSETS, VIEWS, X_DEV, NY), F32),
            vmem((SUBSETS, VIEWS, X_DEV, NY), F32),
            vmem((SUBSETS, X_DEV, NY), F32),
            vmem((SUBSETS, VIEWS, 2, 8, 128), jnp.int32),
            vmem((SUBSETS, VIEWS, 2, 8, 128), F32),
            vmem((2 * SUBSETS, HALF, VIEWS * WIN, NY), BF16),
            vmem((2, HALF, 256, NY), BF16),
            vmem((VIEWS * 128, 512), BF16),
            vmem((VIEWS * 128, 256), BF16),
            vmem((ROWS, VIEWS * 128), F32),
            vmem((ROWS, 256), BF16),
            vmem((2 * ROWS, 512), BF16),
            vmem((2 * ROWS, 256), BF16),
            vmem((OWNERS, 16, 128), F32),
            vmem((xy, 16, 128), F32),
            vmem((SUBSETS, blocks, 8, 128), F32),
            vmem((SUBSETS, GROUPS, VIEWS, 16, 128), F32),
            vmem((SUBSETS, xy, 16, 128), F32),
            vmem((SUBSETS, 2, VIEWS, 8, 128), F32),
            vmem((SUBSETS, xy, 8, 128), F32),
            vmem((SUBSETS, xy, 8, 128), F32),
            vmem((blocks, 8, 128), F32),
            vmem((SUBSETS, xy, 16, 128), BF16),
            vmem((SUBSETS, OWNERS, 16, 128), BF16),
            vmem((SUBSETS, xy, 8, 128), BF16),
            vmem((SUBSETS, 2, VIEWS, 8, 128), BF16),
            vmem((xy, 8, 128), F32),
            vmem((OWNERS, 8, 128), F32),
            vmem((2, VIEWS * WIN, 128), F32),
            dma(()), dma(()), dma(()), dma(()), dma(()), dma((4,)), dma((2,)), dma((2,)),
            dma((4,)), dma((2,)), dma((2, 2)), dma(()), dma(()),
        ],
        compiler_params=pltpu.CompilerParams(collective_id=0, has_side_effects=True),
    )(view_order, volume.reshape(Z_DEV * X_DEV, NY), measured.transpose(1, 2, 0, 3))
    return out.reshape(Z_DEV, X_DEV, NY), resid


def solution(mesh):
    in_specs = (P("gz", "xy", None), P(None, None, "gz", "xy"), P())
    out_specs = (P("gz", "xy", None), P(None, "gz", "xy"))
    body = functools.partial(local, mesh.shape["gz"], mesh.shape["xy"])
    return jax.shard_map(body, mesh=mesh, in_specs=in_specs, out_specs=out_specs, check_vma=False)
```

```python
import functools
import math

import jax
import jax.numpy as jnp
from jax import lax
from jax.experimental import pallas as pl
from jax.experimental.pallas import tpu as pltpu
from jax.sharding import PartitionSpec as P

Z_DEV = 16
X_DEV = 48
COLS_DEV = 48
NY = 128
VIEWS = 5
SUBSETS = 2
ANGLES = 48
ROWS_DEV = 20
HALF = X_DEV // 2
WIN = 40
DEEP = 208
GROUPS = 3
SLOTS = 7
SIZES = (7, 7, 6)
OWNERS = VIEWS * GROUPS
SIDE = 4
EDGE = 4
EDGE_SLOT = ROWS_DEV - EDGE - SLOTS * (GROUPS - 1)
ROWS = 16 * GROUPS + 16
MESH = pl.DeviceIdType.MESH
F32 = jnp.float32
BF16 = jnp.bfloat16


def iota(shape, dim):
    return lax.broadcasted_iota(jnp.int32, shape, dim)


def kernel(
    gz, xy, view_hbm, vol_ref, meas_hbm, out_ref, resid_ref,
    views, it, meas, up, ws, shift, trig, weights, data, window, counted, counted_ahead, count_rows, mixer, smearer,
    send_m, recv_m, meas_rows, send_a, recv_a, send_e, recv_e, starts, total, send_c, recv_c, send_f, recv_f,
    send_d, recv_d, turned,
    sem_view, sem_vol, sem_meas, sem_ms, sem_mr, sem_as, sem_ar, sem_ah, sem_cs, sem_cr, sem_ch, sem_ds, sem_dr,
):
    g = lax.axis_index("gz")
    j = lax.axis_index("xy")
    nx_all, ny_all, dc_all = X_DEV * xy, NY, COLS_DEV * xy
    dr_all, nz_all = ROWS_DEV * gz, Z_DEV * gz
    blocks = dc_all // 128
    chip = lax.div(j, 2)
    owner = jnp.logical_and(lax.rem(j, 2) == 1, chip < OWNERS)
    own_view = lax.rem(lax.div(chip, GROUPS), VIEWS)
    own_group = lax.rem(chip, GROUPS)
    first_group = jnp.logical_and(owner, own_group == 0)
    last_group = jnp.logical_and(owner, own_group == GROUPS - 1)
    below, above = g > 0, g < gz - 1
    give_down = jnp.logical_and(first_group, below)
    give_up = jnp.logical_and(last_group, above)
    has_beside = jnp.logical_or(give_down, give_up)

    view_copy = pltpu.make_async_copy(view_hbm, views, sem_view)
    vol_copy = pltpu.make_async_copy(vol_ref, it, sem_vol)
    meas_copy = pltpu.make_async_copy(meas_hbm, meas, sem_meas)
    view_copy.start()
    vol_copy.start()
    meas_copy.start()

    barrier = pltpu.get_barrier_semaphore()

    def greet(plane, device):
        pl.semaphore_signal(barrier, inc=1, device_id=(plane, device), device_id_type=MESH)

    def greet_all(plane):
        for i in range(xy):
            greet(plane, i)

    def next_owner(t):
        return 2 * lax.rem(chip + t, OWNERS) + 1

    def next_device(t):
        return lax.rem(j + t, xy)

    steps = sorted(
        ((a, b, c) for a in range(SIDE) for b in range(SIDE) for c in (1, 0)),
        key=lambda step: -sum(min(d, SIDE - d) for d in step[:2]),
    )

    def moved_chip(a, b):
        return SIDE * lax.rem(lax.div(chip, SIDE) + a, SIDE) + lax.rem(chip + b, SIDE)

    def moved_device(step):
        return 2 * moved_chip(step[0], step[1]) + lax.rem(j + step[2], 2)

    with jax.named_scope("greet"):
        @pl.when(owner)
        def _():
            for t in range(1, xy):
                greet(g, next_device(t))

        @pl.when(jnp.logical_not(owner))
        def _():
            for t in range(OWNERS):
                greet(g, next_owner(t))

        @pl.when(give_down)
        def _():
            greet_all(g - 1)

        @pl.when(jnp.logical_and(below, jnp.logical_not(first_group)))
        def _():
            for v in range(VIEWS):
                greet(g - 1, 2 * (GROUPS * v + GROUPS - 1) + 1)

        @pl.when(give_up)
        def _():
            greet_all(g + 1)

        @pl.when(jnp.logical_and(above, jnp.logical_not(last_group)))
        def _():
            for v in range(VIEWS):
                greet(g + 1, 2 * GROUPS * v + 1)

    greeted = (
        jnp.where(owner, xy - 1, OWNERS)
        + jnp.where(below, jnp.where(first_group, xy, VIEWS), 0)
        + jnp.where(above, jnp.where(last_group, xy, VIEWS), 0)
    )

    lane = iota((8, 128), 1)
    sub = iota((8, 128), 0)
    lane_f = lane.astype(F32)
    sub_f = sub.astype(F32)
    band = lane // 16
    source = 2.0 * nx_all
    scale = 0.9 * (dc_all / nx_all)
    middle = (dc_all - 1) / 2.0
    x_first = (j * X_DEV).astype(F32)

    def project(x, y, cosine, sine):
        along = x * cosine + y * sine
        depth = y * cosine - x * sine
        return middle + scale * along * source / (source + depth)

    def hat(row, slice_id):
        position = (dr_all - 1) / 2.0 + 0.96 * (dr_all / nz_all) * (slice_id - (nz_all - 1) / 2.0)
        return jnp.maximum(0.0, 1.0 - jnp.abs(position - row) / 2.0)

    def rounded(x):
        return x.astype(BF16).astype(F32)

    def in_two(x):
        high = rounded(x)
        return high, x - high

    def geometry(s):
        for v in range(VIEWS):
            number = jnp.full((8, 128), views[s * VIEWS + v], jnp.int32).astype(F32)
            angle = 2.0 * math.pi * number / ANGLES
            cosine, sine = jnp.cos(angle), jnp.sin(angle)
            trig[s, v, 0] = cosine
            trig[s, v, 1] = sine
            y_low = (band * 16).astype(F32) - (ny_all - 1) / 2.0
            base = []
            for h in range(2):
                x_low = (x_first + HALF * h) - (nx_all - 1) / 2.0
                corners = [
                    project(x, y, cosine, sine)
                    for x in (x_low, x_low + (HALF - 1))
                    for y in (y_low, y_low + 15.0)
                ]
                lowest = jnp.minimum(jnp.minimum(corners[0], corners[1]), jnp.minimum(corners[2], corners[3]))
                start = jnp.floor((lowest - 0.03125) * 0.125) * 8.0
                base.append(start)
                shift[s, v, h] = (start - 256.0 * jnp.floor(start * (1.0 / 256.0))).astype(jnp.int32)
            for block in range(X_DEV // 8):
                x = (x_first + (8.0 * block + sub_f)) - (nx_all - 1) / 2.0
                y = lane_f - (ny_all - 1) / 2.0
                u = project(x, y, cosine, sine)
                low = jnp.floor(u)
                first = rounded(jnp.maximum(0.0, 1.0 - jnp.abs(u - low)))
                second = rounded(jnp.maximum(0.0, 1.0 - jnp.abs(u - (low + 1.0))))
                both = first + second
                rows = slice(8 * block, 8 * block + 8)
                up[s, v, rows, :] = u - base[block // (HALF // 8)]
                ws[s, rows, :] = both if v == 0 else ws[s, rows, :] + both

    window_ids = [(sub + 8 * i).astype(F32) for i in range(WIN // 8)]

    def weights_row(s, h, x):
        pieces = []
        for v in range(VIEWS):
            u = jnp.broadcast_to(up[s, v, pl.ds(HALF * h + x, 1), :], (8, 128))
            pieces += [jnp.maximum(0.0, 1.0 - jnp.abs(u - ids)) for ids in window_ids]
        pieces.append(jnp.zeros((DEEP - VIEWS * WIN, 128), F32))
        weights[2 * s + h, x] = jnp.concatenate(pieces, axis=0).astype(BF16)

    def make_weights(s):
        def one(x, carry):
            for h in range(2):
                weights_row(s, h, x)
            return carry

        lax.fori_loop(0, HALF, one, 0, unroll=4)

    in_band = [iota((16, 128), 1) // 16 == q for q in range(8)]

    def spread(values, h, x):
        data[h, x, 0:128, :] = jnp.concatenate([jnp.where(mine, values, 0.0) for mine in in_band], axis=0).astype(BF16)

    def row_tables():
        for h in range(2):
            turned[h, VIEWS * WIN : DEEP, :] = jnp.zeros((DEEP - VIEWS * WIN, 128), F32)
        shape = (ROWS, 128)
        at = iota(shape, 0)
        own = at < 16 * GROUPS
        half = jnp.where(own, (at // 8) % 2, (at // 4) % 2)
        slot = jnp.where(own, at % 8, at % 4)
        edge = jnp.where(at < 16 * GROUPS + 8, -EDGE, ROWS_DEV)
        row = slot + jnp.where(own, SLOTS * (at // 16), edge)
        size = jnp.where(at // 16 == GROUPS - 1, SIZES[-1], SLOTS)
        row_all = g * ROWS_DEV + row
        inside = jnp.logical_and(jnp.logical_and(row_all >= 0, row_all < dr_all), slot < size)
        slice_all = (g * Z_DEV + iota(shape, 1) % 16).astype(F32)
        row_hat = jnp.where(inside, hat(row_all.astype(F32), slice_all), 0.0)
        counts = jnp.where(jnp.logical_and(jnp.logical_and(own, slot == 7), iota(shape, 1) % 16 < 2), 1.0, 0.0)
        for b in range(2):
            mine = half == b
            high, low = in_two(jnp.where(mine, row_hat, 0.0))
            smearer[0:ROWS, 128 * b : 128 * b + 128] = high.astype(BF16)
            smearer[ROWS : 2 * ROWS, 128 * b : 128 * b + 128] = low.astype(BF16)
            for part in range(2):
                columns = slice(256 * b + 128 * part, 256 * b + 128 * part + 128)
                mixer[0:ROWS, columns] = high.astype(BF16)
                mixer[ROWS : 2 * ROWS, columns] = low.astype(BF16)
            count_rows[:, 128 * b : 128 * b + 128] = jnp.where(mine, counts, 0.0).astype(BF16)

    slices = (g * Z_DEV + iota((16, 128), 0)).astype(F32)
    slice_total = jnp.zeros((16, 1), F32)
    for part in range(-(-dr_all // 128)):
        rows = 128 * part + iota((16, 128), 1)
        weight = jnp.where(rows < dr_all, hat(rows.astype(F32), slices), 0.0)
        slice_total = slice_total + jnp.sum(weight, axis=1, keepdims=True)
    slice_total = jnp.broadcast_to(slice_total, (16, 128))
    own_row = (g * ROWS_DEV + own_group * SLOTS + sub).astype(F32)
    ray_row = jnp.zeros((8, 1), F32)
    for part in range(-(-nz_all // 128)):
        ids = 128 * part + lane
        weight = jnp.where(ids < nz_all, hat(own_row, ids.astype(F32)), 0.0)
        ray_row = ray_row + jnp.sum(weight, axis=1, keepdims=True)
    ray_row = jnp.broadcast_to(ray_row, (8, 128))
    own_slot = sub < jnp.where(own_group == GROUPS - 1, SIZES[-1], SLOTS)
    column_ids = [(128 * m + lane).astype(F32) for m in range(blocks)]

    def remote(src, dst, send_sem, recv_sem, plane, device):
        pltpu.make_async_remote_copy(
            src_ref=src, dst_ref=dst, send_sem=send_sem, recv_sem=recv_sem,
            device_id=(plane, device), device_id_type=MESH,
        ).start()

    def arrived(ref, sem):
        pltpu.make_async_copy(ref, ref, sem).wait()

    def to_owners(src, dst, send_sem, recv_sem):
        for a, b, c in steps:
            if c:
                there = moved_chip(a, b)
                wanted = there < OWNERS
                if a == b == 0:
                    wanted = jnp.logical_and(wanted, jnp.logical_not(owner))

                @pl.when(wanted)
                def _():
                    remote(src(there), dst, send_sem, recv_sem, g, 2 * there + 1)

    def with_owners(ref, sem):
        @pl.when(owner)
        def _():
            arrived(ref.at[0 : OWNERS - 1], sem)

        @pl.when(jnp.logical_not(owner))
        def _():
            arrived(ref.at[0:OWNERS], sem)

    def table(x, carry):
        for h in range(2):
            for q in range(8):
                pair = iota((16, 128), 0) < 2
                row = jnp.where(jnp.logical_and(pair, iota((16, 128), 1) // 16 == q), 1.0, 0.0)
                data[h, x, 128 + 16 * q : 128 + 16 * q + 16, :] = row.astype(BF16)
        return carry

    def spread_row(h, x):
        spread(it[pl.ds(HALF * h + x, 16, stride=X_DEV), :], h, x)

    def first_half(x, carry):
        weights_row(0, 0, x)
        spread_row(0, x)
        return carry

    with jax.named_scope("tables"):
        row_tables()
        lax.fori_loop(0, HALF, table, 0, unroll=4)
    view_copy.wait()
    with jax.named_scope("geom0"):
        geometry(0)
    with jax.named_scope("fill"):
        vol_copy.wait()
        lax.fori_loop(0, HALF, first_half, 0, unroll=4)

    with jax.named_scope("measured"):
        meas_copy.wait()
        turn = lax.rem(j * COLS_DEV, 128)
        for v in range(VIEWS):
            for k in range(GROUPS):
                o = GROUPS * v + k
                send_m[o] = jnp.zeros((16, 128), F32)
                for s in range(SUBSETS):
                    for slot in range(SIZES[k]):
                        send_m[o, 8 * s + slot, 0:COLS_DEV] = meas[v, SLOTS * k + slot, s, :]
        for o in range(OWNERS):
            send_m[o] = pltpu.roll(send_m[o], turn, 1)

    with jax.named_scope("barrier"):
        pl.semaphore_wait(barrier, greeted)

    def send_measured():
        to_owners(lambda o: send_m.at[o], recv_m.at[j], sem_ms, sem_mr)

        @pl.when(owner)
        def _():
            recv_m[j] = send_m[chip]

    def placed(sums, s, v, part):
        halves = []
        for h in range(2):
            offset = shift[s, v, h]
            rows = [
                sums[h][v * WIN + 8 * i : v * WIN + 8 * i + 8, 128 * part : 128 * part + 128] for i in range(WIN // 8)
            ] + [None] * (32 - WIN // 8)
            for bit in (8, 16, 32, 64, 128):
                moved = (offset & bit) != 0
                step = bit // 8
                new = []
                for i in range(32):
                    old, other = rows[i], rows[(i - step) % 32]
                    if old is None and other is None:
                        new.append(None)
                    elif old is None:
                        new.append(jnp.where(moved, other, 0.0))
                    elif other is None:
                        new.append(jnp.where(moved, 0.0, old))
                    else:
                        new.append(jnp.where(moved, other, old))
                rows = new
            halves.append(rows)
        return [a + b for a, b in zip(*halves)]

    def pairs(pieces):
        for i in range(0, 32, 2):
            yield i // 16, 8 * (i % 16), jnp.concatenate([pieces[i], pieces[i + 1]], axis=0)

    def beside(ref, at, first, count, rows=slice(None)):
        return jnp.concatenate([ref[at, x, rows, :] for x in range(first, first + count)], axis=1)

    def band_sums(s, part, late=()):
        rows = slice(0, 256) if part is None else slice(128 * part, 128 * part + 128)
        sums = []
        for h in range(2):
            sums.append(
                lax.dot_general(
                    beside(weights, 2 * s + h, 0, HALF), beside(data, h, 0, HALF, rows),
                    (((1,), (1,)), ((), ())), preferred_element_type=F32,
                )
            )
            if h == 0:
                for other in late:
                    for x in range(HALF):
                        weights_row(s, other, x)
                        spread_row(other, x)
        return sums

    first_lane = iota((16, 128), 1) % 16 == 0

    def count_columns(s, sums, part):
        for v in range(VIEWS):
            for b, at, value in pairs(placed(sums, s, v, part)):
                high, low = in_two(value)
                counted[128 * v + at : 128 * v + at + 16, 128 * b : 128 * b + 128] = jnp.where(
                    first_lane, high, low
                ).astype(BF16)
        return lax.dot_general(
            count_rows[...], counted[...], (((1,), (1,)), ((), ())), preferred_element_type=F32
        )

    def forward(s, counts):
        with jax.named_scope("f_dot"):
            sums = band_sums(s, None, (1,)) if counts is None else band_sums(s, 0)
        with jax.named_scope("f_place"):
            for v in range(VIEWS):
                for b, at, value in pairs(placed(sums, s, v, 0)):
                    high, low = in_two(value)
                    rows = slice(128 * v + at, 128 * v + at + 16)
                    window[rows, 256 * b : 256 * b + 128] = high.astype(BF16)
                    window[rows, 256 * b + 128 : 256 * b + 256] = low.astype(BF16)
        with jax.named_scope("f_mix"):
            if counts is None:
                counts = count_columns(s, sums, 1)
            mixed = lax.dot_general(
                mixer[...], window[...], (((1,), (1,)), ((), ())), preferred_element_type=F32
            )
            mixed = mixed[0:ROWS] + mixed[ROWS : 2 * ROWS] + counts
            for v in range(VIEWS):
                columns = slice(128 * v, 128 * v + 128)
                for k in range(GROUPS):
                    send_a[s, k, v] = mixed[16 * k : 16 * k + 16, columns]
                for e in range(2):
                    at = 16 * GROUPS + 8 * e
                    send_e[s, e, v] = mixed[at : at + 8, columns]
        with jax.named_scope("f_send"):
            for there, plane, e, group in ((below, g - 1, 0, GROUPS - 1), (above, g + 1, 1, 0)):
                @pl.when(there)
                def _():
                    for v in range(VIEWS):
                        remote(
                            send_e.at[s, e, v], recv_e.at[s, j], sem_as.at[2 + s], sem_ah.at[s],
                            plane, 2 * (GROUPS * v + group) + 1,
                        )
            to_owners(
                lambda o: send_a.at[s, lax.rem(o, GROUPS), lax.div(o, GROUPS)],
                recv_a.at[s, j], sem_as.at[s], sem_ar.at[s],
            )

            @pl.when(owner)
            def _():
                recv_a[s, j] = send_a[s, own_group, own_view]

    def prepare_owner():
        arrived(recv_m.at[0 : xy - 1], sem_mr)
        for block in range(blocks):
            first, last = 128 * block, 128 * block + 128
            for s in range(SUBSETS):
                value = jnp.zeros((8, 128), F32)
                for i in range(first // COLS_DEV, min(xy, -(-last // COLS_DEV))):
                    low, high = max(COLS_DEV * i, first) - first, min(COLS_DEV * (i + 1), last) - first
                    piece = recv_m[i, 8 * s : 8 * s + 8, :]
                    value = jnp.where(jnp.logical_and(lane >= low, lane < high), piece, value)
                meas_rows[s, block] = value

    def window_starts(s):
        cosine, sine = trig[s, own_view, 0], trig[s, own_view, 1]

        def one(i, carry):
            x = jnp.full((8, 128), i * X_DEV, jnp.int32).astype(F32) + ((X_DEV - 1) / 2.0 - (nx_all - 1) / 2.0)
            starts[s, i] = jnp.floor(project(x, 0.0, cosine, sine)) - 128.0
            return carry

        lax.fori_loop(0, xy, one, 0)

    def reach(i):
        far = max(abs(X_DEV * i - (nx_all - 1) / 2.0), abs(X_DEV * i + X_DEV - 1 - (nx_all - 1) / 2.0))
        radius = math.hypot(far, (ny_all - 1) / 2.0)
        span = scale * radius / math.sqrt(1.0 - (radius / source) ** 2) + 2.0
        return max(0, int((middle - span) // 128)), min(blocks - 1, int((middle + span) // 128))

    edge_ids = [(256 * m + 128 * (sub // EDGE) + lane).astype(F32) for m in range(blocks // 2)]
    edge_slot = jnp.where(last_group, EDGE_SLOT, 0)

    def within(ids, start):
        return jnp.abs(ids - (start + 127.5)) < 128.0

    def choose(ids, values, candidates, start):
        message = None
        for m in reversed(candidates):
            message = values[m] if message is None else jnp.where(ids[m] >= start, values[m], message)
        return jnp.zeros((8, 128), F32) if message is None else message

    def owner_work(s):
        with jax.named_scope("wait_a"):
            arrived(recv_a.at[s, 0 : xy - 1], sem_ar.at[s])
        with jax.named_scope("o_add"):
            sums = [jnp.zeros((8, 128), F32)] * blocks
            for i in range(xy):
                start = starts[s, i]
                parts = recv_a[s, i, 0:8, :], recv_a[s, i, 8:16, :]
                for m in range(reach(i)[0], reach(i)[1] + 1):
                    sums[m] = sums[m] + jnp.where(within(column_ids[m], start), parts[m % 2], 0.0)
            for m in range(blocks):
                total[m] = sums[m]

        @pl.when(has_beside)
        def _():
            with jax.named_scope("wait_h"):
                arrived(recv_e.at[s], sem_ah.at[s])
            with jax.named_scope("o_addh"):
                sums = [jnp.zeros((8, 128), F32)] * (blocks // 2)
                for i in range(xy):
                    start = starts[s, i]
                    message = recv_e[s, i]
                    for m in range(reach(i)[0] // 2, reach(i)[1] // 2 + 1):
                        sums[m] = sums[m] + jnp.where(within(edge_ids[m], start), message, 0.0)
                for m in range(blocks // 2):
                    low = jnp.where(sub < EDGE, sums[m], 0.0)
                    total[2 * m] = total[2 * m] + pltpu.roll(low, edge_slot, 0)
                    total[2 * m + 1] = total[2 * m + 1] + pltpu.roll(sums[m] - low, edge_slot + EDGE, 0)

        with jax.named_scope("o_give"):
            residuals = []
            for m in range(blocks):
                value = total[m]
                columns = jnp.broadcast_to(value[7:8, :], (8, 128))
                residual = meas_rows[s, m] - value / jnp.maximum(ray_row * columns, 1.0)
                residual = jnp.where(own_slot, residual, 0.0)
                total[m] = residual
                residuals.append(rounded(residual))
            for i in range(xy):
                start = starts[s, i]
                parts = []
                for b in range(2):
                    candidates = [m for m in range(reach(i)[0], reach(i)[1] + 1) if m % 2 == b]
                    parts.append(choose(column_ids, residuals, candidates, start))
                send_c[s, i] = jnp.concatenate(parts, axis=0).astype(BF16)

        @pl.when(has_beside)
        def _():
            with jax.named_scope("o_giveh"):
                back = lax.rem(8 - edge_slot, 8)
                edges = [
                    jnp.where(
                        sub < EDGE,
                        pltpu.roll(rounded(total[2 * m]), back, 0),
                        pltpu.roll(rounded(total[2 * m + 1]), lax.rem(back + EDGE, 8), 0),
                    )
                    for m in range(blocks // 2)
                ]
                for i in range(xy):
                    candidates = list(range(reach(i)[0] // 2, reach(i)[1] // 2 + 1))
                    send_f[s, i] = choose(edge_ids, edges, candidates, starts[s, i]).astype(BF16)
            with jax.named_scope("o_sendh"):
                plane = jnp.where(last_group, g + 1, g - 1)
                slot = jnp.where(last_group, 0, 1)
                for step in steps:
                    i = moved_device(step)
                    remote(
                        send_f.at[s, i], recv_f.at[s, slot, own_view], sem_cs.at[2 + s], sem_ch.at[s, slot], plane, i
                    )

        with jax.named_scope("o_send"):
            for step in steps:
                if step == (0, 0, 0):
                    continue
                i = moved_device(step)
                remote(send_c.at[s, i], recv_c.at[s, chip], sem_cs.at[s], sem_cr.at[s], g, i)
            recv_c[s, chip] = send_c[s, j]

    def owner_give_residual():
        for i in range(xy):
            first = COLS_DEV * i // 128
            message = total[first]
            if first + 1 < blocks:
                message = jnp.where(lane >= COLS_DEV * i % 128, message, total[first + 1])
            send_d[i] = message
        for t in range(1, xy):
            i = next_device(t)
            remote(send_d.at[i], recv_d.at[chip], sem_ds, sem_dr, g, i)
        recv_d[chip] = send_d[j]

    def backward(s):
        @pl.when(jnp.logical_not(below))
        def _():
            recv_f[s, 0] = jnp.zeros((VIEWS, 8, 128), BF16)

        @pl.when(jnp.logical_not(above))
        def _():
            recv_f[s, 1] = jnp.zeros((VIEWS, 8, 128), BF16)

        with jax.named_scope("wait_c"):
            with_owners(recv_c.at[s], sem_cr.at[s])

        with jax.named_scope("wait_ch"):
            @pl.when(below)
            def _():
                arrived(recv_f.at[s, 0], sem_ch.at[s, 0])

            @pl.when(above)
            def _():
                arrived(recv_f.at[s, 1], sem_ch.at[s, 1])

        with jax.named_scope("b_smear"):
            columns = []
            for v in range(VIEWS):
                rows = [recv_c[s, GROUPS * v + k].astype(F32) for k in range(GROUPS)]
                rows = rows + [recv_f[s, e, v].astype(F32) for e in range(2)]
                columns.append(jnp.transpose(jnp.concatenate(rows + rows, axis=0)).astype(BF16))
            smeared = rounded(
                lax.dot_general(
                    jnp.concatenate(columns, axis=0), smearer[...], (((1,), (0,)), ((), ())),
                    preferred_element_type=F32,
                )
            )
            for v in range(VIEWS):
                whole = [
                    smeared[128 * v + 8 * i : 128 * v + 8 * i + 8, 128 * p : 128 * p + 128]
                    for p in range(2)
                    for i in range(16)
                ]
                for h in range(2):
                    offset = shift[s, v, h]
                    now = whole
                    for bit in (128, 64, 32, 16, 8):
                        step = bit // 8
                        moved = (offset & bit) != 0
                        now = [
                            jnp.where(moved, now[(i + step) % 32], now[i]) for i in range(WIN // 8 + step - 1)
                        ]
                    for i in range(WIN // 8):
                        turned[h, v * WIN + 8 * i : v * WIN + 8 * i + 8, :] = now[i]
        with jax.named_scope("b_turn"):
            sides = [jnp.transpose(turned[h]).astype(BF16) for h in range(2)]
        last = s == SUBSETS - 1
        per_step = 2

        bands = jnp.concatenate([band, band], axis=0)

        def one(step, h):
            if True:
                back = lax.dot_general(
                    sides[h], beside(weights, 2 * s + h, per_step * step, per_step), (((1,), (0,)), ((), ())),
                    preferred_element_type=F32,
                )
                for part in range(per_step):
                    x = per_step * step + part
                    mine = back[112:128, 128 * part : 128 * part + 128]
                    for q in range(6, -1, -1):
                        mine = jnp.where(
                            bands == q, back[16 * q : 16 * q + 16, 128 * part : 128 * part + 128], mine
                        )
                    norm = slice_total * ws[s, HALF * h + x : HALF * h + x + 1, :]
                    at = pl.ds(HALF * h + x, 16, stride=X_DEV)
                    new = it[at, :] + mine / jnp.maximum(norm, 1.0)
                    if last:
                        out_ref[at, :] = new
                    else:
                        it[at, :] = new
                        spread(new, h, x)

        with jax.named_scope("b_loop"):
            for h in range(2):
                for step in range(HALF // per_step):
                    one(step, h)

    with jax.named_scope("send_m"):
        send_measured()
    forward(0, None)

    @pl.when(owner)
    def _():
        with jax.named_scope("prep"):
            prepare_owner()
            window_starts(0)
        owner_work(0)

    with jax.named_scope("gw1"):
        geometry(1)
        make_weights(1)
        counted_ahead[...] = count_columns(1, band_sums(1, 1), 0)

    @pl.when(owner)
    def _():
        window_starts(1)

    backward(0)
    forward(1, counted_ahead[...])

    @pl.when(owner)
    def _():
        owner_work(1)
        with jax.named_scope("give"):
            owner_give_residual()

    backward(1)

    with jax.named_scope("tail"):
        with_owners(recv_d, sem_dr)
        turn_back = lax.rem(128 - lax.rem(j * COLS_DEV, 128), 128)
        for v in range(VIEWS):
            for k in range(GROUPS):
                message = pltpu.roll(recv_d[GROUPS * v + k], turn_back, 1)
                resid_ref[v, SLOTS * k : SLOTS * k + SIZES[k], :] = message[0 : SIZES[k], 0:COLS_DEV]

        with_owners(send_m, sem_ms)
        for s in range(SUBSETS):
            with_owners(recv_a.at[s], sem_as.at[s])

            @pl.when(below)
            def _():
                arrived(send_e.at[s, 0], sem_as.at[2 + s])

            @pl.when(above)
            def _():
                arrived(send_e.at[s, 1], sem_as.at[2 + s])

            @pl.when(owner)
            def _():
                arrived(send_c.at[s, 0 : xy - 1], sem_cs.at[s])

            @pl.when(has_beside)
            def _():
                arrived(send_f.at[s], sem_cs.at[2 + s])

        @pl.when(owner)
        def _():
            arrived(send_d.at[0 : xy - 1], sem_ds)


def local(gz, xy, volume, measured, view_order):
    blocks = COLS_DEV * xy // 128
    dma = pltpu.SemaphoreType.DMA
    vmem = pltpu.VMEM
    out, resid = pl.pallas_call(
        functools.partial(kernel, gz, xy),
        out_shape=(
            pltpu.VMEM((Z_DEV * X_DEV, NY), F32),
            pltpu.VMEM((VIEWS, ROWS_DEV, COLS_DEV), F32),
        ),
        in_specs=[pl.BlockSpec(memory_space=pl.ANY)] * 3,
        out_specs=(pl.BlockSpec(memory_space=pltpu.VMEM), pl.BlockSpec(memory_space=pltpu.VMEM)),
        scratch_shapes=[
            pltpu.SMEM((ANGLES,), jnp.int32),
            vmem((Z_DEV * X_DEV, NY), F32),
            vmem((VIEWS, ROWS_DEV, SUBSETS, COLS_DEV), F32),
            vmem((SUBSETS, VIEWS, X_DEV, NY), F32),
            vmem((SUBSETS, X_DEV, NY), F32),
            vmem((SUBSETS, VIEWS, 2, 8, 128), jnp.int32),
            vmem((SUBSETS, VIEWS, 2, 8, 128), F32),
            vmem((2 * SUBSETS, HALF, DEEP, NY), BF16),
            vmem((2, HALF, 256, NY), BF16),
            vmem((VIEWS * 128, 512), BF16),
            vmem((VIEWS * 128, 256), BF16),
            vmem((ROWS, VIEWS * 128), F32),
            vmem((ROWS, 256), BF16),
            vmem((2 * ROWS, 512), BF16),
            vmem((2 * ROWS, 256), BF16),
            vmem((OWNERS, 16, 128), F32),
            vmem((xy, 16, 128), F32),
            vmem((SUBSETS, blocks, 8, 128), F32),
            vmem((SUBSETS, GROUPS, VIEWS, 16, 128), F32),
            vmem((SUBSETS, xy, 16, 128), F32),
            vmem((SUBSETS, 2, VIEWS, 8, 128), F32),
            vmem((SUBSETS, xy, 8, 128), F32),
            vmem((SUBSETS, xy, 8, 128), F32),
            vmem((blocks, 8, 128), F32),
            vmem((SUBSETS, xy, 16, 128), BF16),
            vmem((SUBSETS, OWNERS, 16, 128), BF16),
            vmem((SUBSETS, xy, 8, 128), BF16),
            vmem((SUBSETS, 2, VIEWS, 8, 128), BF16),
            vmem((xy, 8, 128), F32),
            vmem((OWNERS, 8, 128), F32),
            vmem((2, DEEP, 128), F32),
            dma(()), dma(()), dma(()), dma(()), dma(()), dma((4,)), dma((2,)), dma((2,)),
            dma((4,)), dma((2,)), dma((2, 2)), dma(()), dma(()),
        ],
        compiler_params=pltpu.CompilerParams(collective_id=0, has_side_effects=True),
    )(view_order, volume.reshape(Z_DEV * X_DEV, NY), measured.transpose(1, 2, 0, 3))
    out, resid = pl.pallas_call(
        put_out,
        out_shape=(
            jax.ShapeDtypeStruct((Z_DEV * X_DEV, NY), F32),
            jax.ShapeDtypeStruct((VIEWS, ROWS_DEV, COLS_DEV), F32),
        ),
        in_specs=[pl.BlockSpec(memory_space=pltpu.VMEM)] * 2,
        out_specs=(pl.BlockSpec(memory_space=pl.ANY),) * 2,
        scratch_shapes=[dma(()), dma(())],
    )(pltpu.with_memory_space_constraint(out, pltpu.VMEM), pltpu.with_memory_space_constraint(resid, pltpu.VMEM))
    return out.reshape(Z_DEV, X_DEV, NY), resid


def put_out(a_ref, b_ref, a_out, b_out, a_sem, b_sem):
    copies = [pltpu.make_async_copy(a_ref, a_out, a_sem), pltpu.make_async_copy(b_ref, b_out, b_sem)]
    for copy in copies:
        copy.start()
    for copy in copies:
        copy.wait()


def solution(mesh):
    in_specs = (P("gz", "xy", None), P(None, None, "gz", "xy"), P())
    out_specs = (P("gz", "xy", None), P(None, "gz", "xy"))
    body = functools.partial(local, mesh.shape["gz"], mesh.shape["xy"])
    return jax.shard_map(body, mesh=mesh, in_specs=in_specs, out_specs=out_specs, check_vma=False)
```

```python
import functools
import math

import jax
import jax.numpy as jnp
from jax import lax
from jax.experimental import pallas as pl
from jax.experimental.pallas import tpu as pltpu
from jax.sharding import PartitionSpec as P

Z_DEV = 16
X_DEV = 48
COLS_DEV = 48
NY = 128
VIEWS = 5
SUBSETS = 2
ANGLES = 48
ROWS_DEV = 20
HALF = X_DEV // 2
WIN = 40
DEEP = 208
GROUPS = 3
SLOTS = 7
SIZES = (7, 7, 6)
OWNERS = VIEWS * GROUPS
SIDE = 4
EDGE = 4
EDGE_SLOT = ROWS_DEV - EDGE - SLOTS * (GROUPS - 1)
ROWS = 16 * GROUPS + 16
MESH = pl.DeviceIdType.MESH
F32 = jnp.float32
BF16 = jnp.bfloat16


def iota(shape, dim):
    return lax.broadcasted_iota(jnp.int32, shape, dim)


def kernel(
    gz, xy, view_hbm, vol_ref, meas_hbm, out_ref, resid_ref,
    views, it, meas, up, ws, shift, trig, weights, data, window, counted, counted_ahead, count_rows, mixer, smearer,
    send_m, recv_m, meas_rows, send_a, recv_a, send_e, recv_e, starts, total, send_c, recv_c, send_f, recv_f,
    send_d, recv_d, turned,
    sem_view, sem_vol, sem_meas, sem_ms, sem_mr, sem_as, sem_ar, sem_ah, sem_cs, sem_cr, sem_ch, sem_ds, sem_dr,
):
    g = lax.axis_index("gz")
    j = lax.axis_index("xy")
    nx_all, ny_all, dc_all = X_DEV * xy, NY, COLS_DEV * xy
    dr_all, nz_all = ROWS_DEV * gz, Z_DEV * gz
    blocks = dc_all // 128
    chip = lax.div(j, 2)
    owner = jnp.logical_and(lax.rem(j, 2) == 1, chip < OWNERS)
    own_view = lax.rem(lax.div(chip, GROUPS), VIEWS)
    own_group = lax.rem(chip, GROUPS)
    first_group = jnp.logical_and(owner, own_group == 0)
    last_group = jnp.logical_and(owner, own_group == GROUPS - 1)
    below, above = g > 0, g < gz - 1
    give_down = jnp.logical_and(first_group, below)
    give_up = jnp.logical_and(last_group, above)
    has_beside = jnp.logical_or(give_down, give_up)

    view_copy = pltpu.make_async_copy(view_hbm, views, sem_view)
    vol_copy = pltpu.make_async_copy(vol_ref, it, sem_vol)
    meas_copy = pltpu.make_async_copy(meas_hbm, meas, sem_meas)
    view_copy.start()
    vol_copy.start()
    meas_copy.start()

    barrier = pltpu.get_barrier_semaphore()

    def greet(plane, device):
        pl.semaphore_signal(barrier, inc=1, device_id=(plane, device), device_id_type=MESH)

    def greet_all(plane):
        for i in range(xy):
            greet(plane, i)

    def next_owner(t):
        return 2 * lax.rem(chip + t, OWNERS) + 1

    def next_device(t):
        return lax.rem(j + t, xy)

    steps = sorted(
        ((a, b, c) for a in range(SIDE) for b in range(SIDE) for c in (1, 0)),
        key=lambda step: -sum(min(d, SIDE - d) for d in step[:2]),
    )

    def moved_chip(a, b):
        return SIDE * lax.rem(lax.div(chip, SIDE) + a, SIDE) + lax.rem(chip + b, SIDE)

    def moved_device(step):
        return 2 * moved_chip(step[0], step[1]) + lax.rem(j + step[2], 2)

    with jax.named_scope("greet"):
        @pl.when(owner)
        def _():
            for t in range(1, xy):
                greet(g, next_device(t))

        @pl.when(jnp.logical_not(owner))
        def _():
            for t in range(OWNERS):
                greet(g, next_owner(t))

        @pl.when(give_down)
        def _():
            greet_all(g - 1)

        @pl.when(jnp.logical_and(below, jnp.logical_not(first_group)))
        def _():
            for v in range(VIEWS):
                greet(g - 1, 2 * (GROUPS * v + GROUPS - 1) + 1)

        @pl.when(give_up)
        def _():
            greet_all(g + 1)

        @pl.when(jnp.logical_and(above, jnp.logical_not(last_group)))
        def _():
            for v in range(VIEWS):
                greet(g + 1, 2 * GROUPS * v + 1)

    greeted = (
        jnp.where(owner, xy - 1, OWNERS)
        + jnp.where(below, jnp.where(first_group, xy, VIEWS), 0)
        + jnp.where(above, jnp.where(last_group, xy, VIEWS), 0)
    )

    lane = iota((8, 128), 1)
    sub = iota((8, 128), 0)
    lane_f = lane.astype(F32)
    sub_f = sub.astype(F32)
    band = lane // 16
    source = 2.0 * nx_all
    scale = 0.9 * (dc_all / nx_all)
    middle = (dc_all - 1) / 2.0
    x_first = (j * X_DEV).astype(F32)

    def project(x, y, cosine, sine):
        along = x * cosine + y * sine
        depth = y * cosine - x * sine
        return middle + scale * along * source / (source + depth)

    def hat(row, slice_id):
        position = (dr_all - 1) / 2.0 + 0.96 * (dr_all / nz_all) * (slice_id - (nz_all - 1) / 2.0)
        return jnp.maximum(0.0, 1.0 - jnp.abs(position - row) / 2.0)

    def rounded(x):
        return x.astype(BF16).astype(F32)

    def in_two(x):
        high = rounded(x)
        return high, x - high

    def geometry(s):
        for v in range(VIEWS):
            number = jnp.full((8, 128), views[s * VIEWS + v], jnp.int32).astype(F32)
            angle = 2.0 * math.pi * number / ANGLES
            cosine, sine = jnp.cos(angle), jnp.sin(angle)
            trig[s, v, 0] = cosine
            trig[s, v, 1] = sine
            y_low = (band * 16).astype(F32) - (ny_all - 1) / 2.0
            base = []
            for h in range(2):
                x_low = (x_first + HALF * h) - (nx_all - 1) / 2.0
                corners = [
                    project(x, y, cosine, sine)
                    for x in (x_low, x_low + (HALF - 1))
                    for y in (y_low, y_low + 15.0)
                ]
                lowest = jnp.minimum(jnp.minimum(corners[0], corners[1]), jnp.minimum(corners[2], corners[3]))
                start = jnp.floor((lowest - 0.03125) * 0.125) * 8.0
                base.append(start)
                shift[s, v, h] = (start - 256.0 * jnp.floor(start * (1.0 / 256.0))).astype(jnp.int32)
            for block in range(X_DEV // 8):
                x = (x_first + (8.0 * block + sub_f)) - (nx_all - 1) / 2.0
                y = lane_f - (ny_all - 1) / 2.0
                u = project(x, y, cosine, sine)
                low = jnp.floor(u)
                first = rounded(jnp.maximum(0.0, 1.0 - jnp.abs(u - low)))
                second = rounded(jnp.maximum(0.0, 1.0 - jnp.abs(u - (low + 1.0))))
                both = first + second
                rows = slice(8 * block, 8 * block + 8)
                up[s, v, rows, :] = u - base[block // (HALF // 8)]
                ws[s, rows, :] = both if v == 0 else ws[s, rows, :] + both

    window_ids = [(sub + 8 * i).astype(F32) for i in range(WIN // 8)]

    def weights_row(s, h, x):
        pieces = []
        for v in range(VIEWS):
            u = jnp.broadcast_to(up[s, v, pl.ds(HALF * h + x, 1), :], (8, 128))
            pieces += [jnp.maximum(0.0, 1.0 - jnp.abs(u - ids)) for ids in window_ids]
        pieces.append(jnp.zeros((DEEP - VIEWS * WIN, 128), F32))
        weights[2 * s + h, x] = jnp.concatenate(pieces, axis=0).astype(BF16)

    def make_weights(s):
        def one(x, carry):
            for h in range(2):
                weights_row(s, h, x)
            return carry

        lax.fori_loop(0, HALF, one, 0, unroll=4)

    in_band = [iota((16, 128), 1) // 16 == q for q in range(8)]

    def spread(values, h, x):
        data[h, x, 0:128, :] = jnp.concatenate([jnp.where(mine, values, 0.0) for mine in in_band], axis=0).astype(BF16)

    def row_tables():
        for h in range(2):
            turned[h, VIEWS * WIN : DEEP, :] = jnp.zeros((DEEP - VIEWS * WIN, 128), F32)
        shape = (ROWS, 128)
        at = iota(shape, 0)
        own = at < 16 * GROUPS
        half = jnp.where(own, (at // 8) % 2, (at // 4) % 2)
        slot = jnp.where(own, at % 8, at % 4)
        edge = jnp.where(at < 16 * GROUPS + 8, -EDGE, ROWS_DEV)
        row = slot + jnp.where(own, SLOTS * (at // 16), edge)
        size = jnp.where(at // 16 == GROUPS - 1, SIZES[-1], SLOTS)
        row_all = g * ROWS_DEV + row
        inside = jnp.logical_and(jnp.logical_and(row_all >= 0, row_all < dr_all), slot < size)
        slice_all = (g * Z_DEV + iota(shape, 1) % 16).astype(F32)
        row_hat = jnp.where(inside, hat(row_all.astype(F32), slice_all), 0.0)
        counts = jnp.where(jnp.logical_and(jnp.logical_and(own, slot == 7), iota(shape, 1) % 16 < 2), 1.0, 0.0)
        for b in range(2):
            mine = half == b
            high, low = in_two(jnp.where(mine, row_hat, 0.0))
            smearer[0:ROWS, 128 * b : 128 * b + 128] = high.astype(BF16)
            smearer[ROWS : 2 * ROWS, 128 * b : 128 * b + 128] = low.astype(BF16)
            for part in range(2):
                columns = slice(256 * b + 128 * part, 256 * b + 128 * part + 128)
                mixer[0:ROWS, columns] = high.astype(BF16)
                mixer[ROWS : 2 * ROWS, columns] = low.astype(BF16)
            count_rows[:, 128 * b : 128 * b + 128] = jnp.where(mine, counts, 0.0).astype(BF16)

    slices = (g * Z_DEV + iota((16, 128), 0)).astype(F32)
    slice_total = jnp.zeros((16, 1), F32)
    for part in range(-(-dr_all // 128)):
        rows = 128 * part + iota((16, 128), 1)
        weight = jnp.where(rows < dr_all, hat(rows.astype(F32), slices), 0.0)
        slice_total = slice_total + jnp.sum(weight, axis=1, keepdims=True)
    slice_total = jnp.broadcast_to(slice_total, (16, 128))
    own_row = (g * ROWS_DEV + own_group * SLOTS + sub).astype(F32)
    ray_row = jnp.zeros((8, 1), F32)
    for part in range(-(-nz_all // 128)):
        ids = 128 * part + lane
        weight = jnp.where(ids < nz_all, hat(own_row, ids.astype(F32)), 0.0)
        ray_row = ray_row + jnp.sum(weight, axis=1, keepdims=True)
    ray_row = jnp.broadcast_to(ray_row, (8, 128))
    own_slot = sub < jnp.where(own_group == GROUPS - 1, SIZES[-1], SLOTS)
    column_ids = [(128 * m + lane).astype(F32) for m in range(blocks)]

    def remote(src, dst, send_sem, recv_sem, plane, device):
        pltpu.make_async_remote_copy(
            src_ref=src, dst_ref=dst, send_sem=send_sem, recv_sem=recv_sem,
            device_id=(plane, device), device_id_type=MESH,
        ).start()

    def arrived(ref, sem):
        pltpu.make_async_copy(ref, ref, sem).wait()

    def to_owners(src, dst, send_sem, recv_sem):
        for a, b, c in steps:
            if c:
                there = moved_chip(a, b)
                wanted = there < OWNERS
                if a == b == 0:
                    wanted = jnp.logical_and(wanted, jnp.logical_not(owner))

                @pl.when(wanted)
                def _():
                    remote(src(there), dst, send_sem, recv_sem, g, 2 * there + 1)

    def with_owners(ref, sem):
        @pl.when(owner)
        def _():
            arrived(ref.at[0 : OWNERS - 1], sem)

        @pl.when(jnp.logical_not(owner))
        def _():
            arrived(ref.at[0:OWNERS], sem)

    def table(x, carry):
        for h in range(2):
            for q in range(8):
                pair = iota((16, 128), 0) < 2
                row = jnp.where(jnp.logical_and(pair, iota((16, 128), 1) // 16 == q), 1.0, 0.0)
                data[h, x, 128 + 16 * q : 128 + 16 * q + 16, :] = row.astype(BF16)
        return carry

    def spread_row(h, x):
        spread(it[pl.ds(HALF * h + x, 16, stride=X_DEV), :], h, x)

    def first_half(x, carry):
        weights_row(0, 0, x)
        spread_row(0, x)
        return carry

    with jax.named_scope("tables"):
        row_tables()
        lax.fori_loop(0, HALF, table, 0, unroll=4)
    view_copy.wait()
    with jax.named_scope("geom0"):
        geometry(0)
    with jax.named_scope("fill"):
        vol_copy.wait()
        lax.fori_loop(0, HALF, first_half, 0, unroll=4)

    with jax.named_scope("measured"):
        meas_copy.wait()
        turn = lax.rem(j * COLS_DEV, 128)
        for v in range(VIEWS):
            for k in range(GROUPS):
                o = GROUPS * v + k
                send_m[o] = jnp.zeros((16, 128), F32)
                for s in range(SUBSETS):
                    for slot in range(SIZES[k]):
                        send_m[o, 8 * s + slot, 0:COLS_DEV] = meas[v, SLOTS * k + slot, s, :]
        for o in range(OWNERS):
            send_m[o] = pltpu.roll(send_m[o], turn, 1)

    def send_measured():
        to_owners(lambda o: send_m.at[o], recv_m.at[j], sem_ms, sem_mr)

        @pl.when(owner)
        def _():
            recv_m[j] = send_m[chip]

    def placed(sums, s, v, part):
        halves = []
        for h in range(2):
            offset = shift[s, v, h]
            rows = [
                sums[h][v * WIN + 8 * i : v * WIN + 8 * i + 8, 128 * part : 128 * part + 128] for i in range(WIN // 8)
            ] + [None] * (32 - WIN // 8)
            for bit in (8, 16, 32, 64, 128):
                moved = (offset & bit) != 0
                step = bit // 8
                new = []
                for i in range(32):
                    old, other = rows[i], rows[(i - step) % 32]
                    if old is None and other is None:
                        new.append(None)
                    elif old is None:
                        new.append(jnp.where(moved, other, 0.0))
                    elif other is None:
                        new.append(jnp.where(moved, 0.0, old))
                    else:
                        new.append(jnp.where(moved, other, old))
                rows = new
            halves.append(rows)
        return [a + b for a, b in zip(*halves)]

    def pairs(pieces):
        for i in range(0, 32, 2):
            yield i // 16, 8 * (i % 16), jnp.concatenate([pieces[i], pieces[i + 1]], axis=0)

    def beside(ref, at, first, count, rows=slice(None)):
        return jnp.concatenate([ref[at, x, rows, :] for x in range(first, first + count)], axis=1)

    def band_sums(s, part, late=()):
        rows = slice(0, 256) if part is None else slice(128 * part, 128 * part + 128)
        sums = []
        for h in range(2):
            sums.append(
                lax.dot_general(
                    beside(weights, 2 * s + h, 0, HALF), beside(data, h, 0, HALF, rows),
                    (((1,), (1,)), ((), ())), preferred_element_type=F32,
                )
            )
            if h == 0:
                for other in late:
                    for x in range(HALF):
                        weights_row(s, other, x)
                        spread_row(other, x)
        return sums

    first_lane = iota((16, 128), 1) % 16 == 0

    def count_columns(s, sums, part):
        for v in range(VIEWS):
            for b, at, value in pairs(placed(sums, s, v, part)):
                high, low = in_two(value)
                counted[128 * v + at : 128 * v + at + 16, 128 * b : 128 * b + 128] = jnp.where(
                    first_lane, high, low
                ).astype(BF16)
        return lax.dot_general(
            count_rows[...], counted[...], (((1,), (1,)), ((), ())), preferred_element_type=F32
        )

    def forward(s, counts):
        with jax.named_scope("f_dot"):
            sums = band_sums(s, None, (1,)) if counts is None else band_sums(s, 0)
        if s == 0:
            with jax.named_scope("barrier"):
                pl.semaphore_wait(barrier, greeted)
            with jax.named_scope("send_m"):
                send_measured()
        with jax.named_scope("f_place"):
            for v in range(VIEWS):
                for b, at, value in pairs(placed(sums, s, v, 0)):
                    high, low = in_two(value)
                    rows = slice(128 * v + at, 128 * v + at + 16)
                    window[rows, 256 * b : 256 * b + 128] = high.astype(BF16)
                    window[rows, 256 * b + 128 : 256 * b + 256] = low.astype(BF16)
        with jax.named_scope("f_mix"):
            if counts is None:
                counts = count_columns(s, sums, 1)
            mixed = lax.dot_general(
                mixer[...], window[...], (((1,), (1,)), ((), ())), preferred_element_type=F32
            )
            mixed = mixed[0:ROWS] + mixed[ROWS : 2 * ROWS] + counts
            for v in range(VIEWS):
                columns = slice(128 * v, 128 * v + 128)
                for k in range(GROUPS):
                    send_a[s, k, v] = mixed[16 * k : 16 * k + 16, columns]
                for e in range(2):
                    at = 16 * GROUPS + 8 * e
                    send_e[s, e, v] = mixed[at : at + 8, columns]
        with jax.named_scope("f_send"):
            for there, plane, e, group in ((below, g - 1, 0, GROUPS - 1), (above, g + 1, 1, 0)):
                @pl.when(there)
                def _():
                    for v in range(VIEWS):
                        remote(
                            send_e.at[s, e, v], recv_e.at[s, j], sem_as.at[2 + s], sem_ah.at[s],
                            plane, 2 * (GROUPS * v + group) + 1,
                        )
            to_owners(
                lambda o: send_a.at[s, lax.rem(o, GROUPS), lax.div(o, GROUPS)],
                recv_a.at[s, j], sem_as.at[s], sem_ar.at[s],
            )

            @pl.when(owner)
            def _():
                recv_a[s, j] = send_a[s, own_group, own_view]

    def prepare_owner():
        arrived(recv_m.at[0 : xy - 1], sem_mr)
        for block in range(blocks):
            first, last = 128 * block, 128 * block + 128
            for s in range(SUBSETS):
                value = jnp.zeros((8, 128), F32)
                for i in range(first // COLS_DEV, min(xy, -(-last // COLS_DEV))):
                    low, high = max(COLS_DEV * i, first) - first, min(COLS_DEV * (i + 1), last) - first
                    piece = recv_m[i, 8 * s : 8 * s + 8, :]
                    value = jnp.where(jnp.logical_and(lane >= low, lane < high), piece, value)
                meas_rows[s, block] = value

    def window_starts(s):
        cosine, sine = trig[s, own_view, 0], trig[s, own_view, 1]

        def one(i, carry):
            x = jnp.full((8, 128), i * X_DEV, jnp.int32).astype(F32) + ((X_DEV - 1) / 2.0 - (nx_all - 1) / 2.0)
            starts[s, i] = jnp.floor(project(x, 0.0, cosine, sine)) - 128.0
            return carry

        lax.fori_loop(0, xy, one, 0)

    def reach(i):
        far = max(abs(X_DEV * i - (nx_all - 1) / 2.0), abs(X_DEV * i + X_DEV - 1 - (nx_all - 1) / 2.0))
        radius = math.hypot(far, (ny_all - 1) / 2.0)
        span = scale * radius / math.sqrt(1.0 - (radius / source) ** 2) + 2.0
        return max(0, int((middle - span) // 128)), min(blocks - 1, int((middle + span) // 128))

    edge_ids = [(256 * m + 128 * (sub // EDGE) + lane).astype(F32) for m in range(blocks // 2)]
    edge_slot = jnp.where(last_group, EDGE_SLOT, 0)

    def within(ids, start):
        return jnp.abs(ids - (start + 127.5)) < 128.0

    def choose(ids, values, candidates, start):
        message = None
        for m in reversed(candidates):
            message = values[m] if message is None else jnp.where(ids[m] >= start, values[m], message)
        return jnp.zeros((8, 128), F32) if message is None else message

    def owner_work(s):
        with jax.named_scope("wait_a"):
            arrived(recv_a.at[s, 0 : xy - 1], sem_ar.at[s])
        with jax.named_scope("o_add"):
            sums = [jnp.zeros((8, 128), F32)] * blocks
            for i in range(xy):
                start = starts[s, i]
                parts = recv_a[s, i, 0:8, :], recv_a[s, i, 8:16, :]
                for m in range(reach(i)[0], reach(i)[1] + 1):
                    sums[m] = sums[m] + jnp.where(within(column_ids[m], start), parts[m % 2], 0.0)
            for m in range(blocks):
                total[m] = sums[m]

        @pl.when(has_beside)
        def _():
            with jax.named_scope("wait_h"):
                arrived(recv_e.at[s], sem_ah.at[s])
            with jax.named_scope("o_addh"):
                sums = [jnp.zeros((8, 128), F32)] * (blocks // 2)
                for i in range(xy):
                    start = starts[s, i]
                    message = recv_e[s, i]
                    for m in range(reach(i)[0] // 2, reach(i)[1] // 2 + 1):
                        sums[m] = sums[m] + jnp.where(within(edge_ids[m], start), message, 0.0)
                for m in range(blocks // 2):
                    low = jnp.where(sub < EDGE, sums[m], 0.0)
                    total[2 * m] = total[2 * m] + pltpu.roll(low, edge_slot, 0)
                    total[2 * m + 1] = total[2 * m + 1] + pltpu.roll(sums[m] - low, edge_slot + EDGE, 0)

        with jax.named_scope("o_give"):
            residuals = []
            for m in range(blocks):
                value = total[m]
                columns = jnp.broadcast_to(value[7:8, :], (8, 128))
                residual = meas_rows[s, m] - value / jnp.maximum(ray_row * columns, 1.0)
                residual = jnp.where(own_slot, residual, 0.0)
                total[m] = residual
                residuals.append(rounded(residual))
            for i in range(xy):
                start = starts[s, i]
                parts = []
                for b in range(2):
                    candidates = [m for m in range(reach(i)[0], reach(i)[1] + 1) if m % 2 == b]
                    parts.append(choose(column_ids, residuals, candidates, start))
                send_c[s, i] = jnp.concatenate(parts, axis=0).astype(BF16)

        @pl.when(has_beside)
        def _():
            with jax.named_scope("o_giveh"):
                back = lax.rem(8 - edge_slot, 8)
                edges = [
                    jnp.where(
                        sub < EDGE,
                        pltpu.roll(rounded(total[2 * m]), back, 0),
                        pltpu.roll(rounded(total[2 * m + 1]), lax.rem(back + EDGE, 8), 0),
                    )
                    for m in range(blocks // 2)
                ]
                for i in range(xy):
                    candidates = list(range(reach(i)[0] // 2, reach(i)[1] // 2 + 1))
                    send_f[s, i] = choose(edge_ids, edges, candidates, starts[s, i]).astype(BF16)
            with jax.named_scope("o_sendh"):
                plane = jnp.where(last_group, g + 1, g - 1)
                slot = jnp.where(last_group, 0, 1)
                for step in steps:
                    i = moved_device(step)
                    remote(
                        send_f.at[s, i], recv_f.at[s, slot, own_view], sem_cs.at[2 + s], sem_ch.at[s, slot], plane, i
                    )

        with jax.named_scope("o_send"):
            for step in steps:
                if step == (0, 0, 0):
                    continue
                i = moved_device(step)
                remote(send_c.at[s, i], recv_c.at[s, chip], sem_cs.at[s], sem_cr.at[s], g, i)
            recv_c[s, chip] = send_c[s, j]

    def owner_give_residual():
        for i in range(xy):
            first = COLS_DEV * i // 128
            message = total[first]
            if first + 1 < blocks:
                message = jnp.where(lane >= COLS_DEV * i % 128, message, total[first + 1])
            send_d[i] = message
        for t in range(1, xy):
            i = next_device(t)
            remote(send_d.at[i], recv_d.at[chip], sem_ds, sem_dr, g, i)
        recv_d[chip] = send_d[j]

    def backward(s):
        @pl.when(jnp.logical_not(below))
        def _():
            recv_f[s, 0] = jnp.zeros((VIEWS, 8, 128), BF16)

        @pl.when(jnp.logical_not(above))
        def _():
            recv_f[s, 1] = jnp.zeros((VIEWS, 8, 128), BF16)

        with jax.named_scope("wait_c"):
            with_owners(recv_c.at[s], sem_cr.at[s])

        with jax.named_scope("wait_ch"):
            @pl.when(below)
            def _():
                arrived(recv_f.at[s, 0], sem_ch.at[s, 0])

            @pl.when(above)
            def _():
                arrived(recv_f.at[s, 1], sem_ch.at[s, 1])

        with jax.named_scope("b_smear"):
            columns = []
            for v in range(VIEWS):
                rows = [recv_c[s, GROUPS * v + k].astype(F32) for k in range(GROUPS)]
                rows = rows + [recv_f[s, e, v].astype(F32) for e in range(2)]
                columns.append(jnp.transpose(jnp.concatenate(rows + rows, axis=0)).astype(BF16))
            smeared = rounded(
                lax.dot_general(
                    jnp.concatenate(columns, axis=0), smearer[...], (((1,), (0,)), ((), ())),
                    preferred_element_type=F32,
                )
            )
            for v in range(VIEWS):
                whole = [
                    smeared[128 * v + 8 * i : 128 * v + 8 * i + 8, 128 * p : 128 * p + 128]
                    for p in range(2)
                    for i in range(16)
                ]
                for h in range(2):
                    offset = shift[s, v, h]
                    now = whole
                    for bit in (128, 64, 32, 16, 8):
                        step = bit // 8
                        moved = (offset & bit) != 0
                        now = [
                            jnp.where(moved, now[(i + step) % 32], now[i]) for i in range(WIN // 8 + step - 1)
                        ]
                    for i in range(WIN // 8):
                        turned[h, v * WIN + 8 * i : v * WIN + 8 * i + 8, :] = now[i]
        with jax.named_scope("b_turn"):
            sides = [jnp.transpose(turned[h]).astype(BF16) for h in range(2)]
        last = s == SUBSETS - 1
        per_step = 2

        bands = jnp.concatenate([band, band], axis=0)

        def one(step, h):
            if True:
                back = lax.dot_general(
                    sides[h], beside(weights, 2 * s + h, per_step * step, per_step), (((1,), (0,)), ((), ())),
                    preferred_element_type=F32,
                )
                for part in range(per_step):
                    x = per_step * step + part
                    mine = back[112:128, 128 * part : 128 * part + 128]
                    for q in range(6, -1, -1):
                        mine = jnp.where(
                            bands == q, back[16 * q : 16 * q + 16, 128 * part : 128 * part + 128], mine
                        )
                    norm = slice_total * ws[s, HALF * h + x : HALF * h + x + 1, :]
                    at = pl.ds(HALF * h + x, 16, stride=X_DEV)
                    new = it[at, :] + mine / jnp.maximum(norm, 1.0)
                    if last:
                        out_ref[at, :] = new
                    else:
                        it[at, :] = new
                        spread(new, h, x)

        with jax.named_scope("b_loop"):
            for h in range(2):
                for step in range(HALF // per_step):
                    one(step, h)

    forward(0, None)

    @pl.when(owner)
    def _():
        with jax.named_scope("prep"):
            prepare_owner()
            window_starts(0)
        owner_work(0)

    with jax.named_scope("gw1"):
        geometry(1)
        make_weights(1)
        counted_ahead[...] = count_columns(1, band_sums(1, 1), 0)

    @pl.when(owner)
    def _():
        window_starts(1)

    backward(0)
    forward(1, counted_ahead[...])

    @pl.when(owner)
    def _():
        owner_work(1)
        with jax.named_scope("give"):
            owner_give_residual()

    backward(1)

    with jax.named_scope("tail"):
        with_owners(recv_d, sem_dr)
        turn_back = lax.rem(128 - lax.rem(j * COLS_DEV, 128), 128)
        for v in range(VIEWS):
            for k in range(GROUPS):
                message = pltpu.roll(recv_d[GROUPS * v + k], turn_back, 1)
                resid_ref[v, SLOTS * k : SLOTS * k + SIZES[k], :] = message[0 : SIZES[k], 0:COLS_DEV]

        with_owners(send_m, sem_ms)
        for s in range(SUBSETS):
            with_owners(recv_a.at[s], sem_as.at[s])

            @pl.when(below)
            def _():
                arrived(send_e.at[s, 0], sem_as.at[2 + s])

            @pl.when(above)
            def _():
                arrived(send_e.at[s, 1], sem_as.at[2 + s])

            @pl.when(owner)
            def _():
                arrived(send_c.at[s, 0 : xy - 1], sem_cs.at[s])

            @pl.when(has_beside)
            def _():
                arrived(send_f.at[s], sem_cs.at[2 + s])

        @pl.when(owner)
        def _():
            arrived(send_d.at[0 : xy - 1], sem_ds)


def local(gz, xy, volume, measured, view_order):
    blocks = COLS_DEV * xy // 128
    dma = pltpu.SemaphoreType.DMA
    vmem = pltpu.VMEM
    out, resid = pl.pallas_call(
        functools.partial(kernel, gz, xy),
        out_shape=(
            pltpu.VMEM((Z_DEV * X_DEV, NY), F32),
            pltpu.VMEM((VIEWS, ROWS_DEV, COLS_DEV), F32),
        ),
        in_specs=[pl.BlockSpec(memory_space=pl.ANY)] * 3,
        out_specs=(pl.BlockSpec(memory_space=pltpu.VMEM), pl.BlockSpec(memory_space=pltpu.VMEM)),
        scratch_shapes=[
            pltpu.SMEM((ANGLES,), jnp.int32),
            vmem((Z_DEV * X_DEV, NY), F32),
            vmem((VIEWS, ROWS_DEV, SUBSETS, COLS_DEV), F32),
            vmem((SUBSETS, VIEWS, X_DEV, NY), F32),
            vmem((SUBSETS, X_DEV, NY), F32),
            vmem((SUBSETS, VIEWS, 2, 8, 128), jnp.int32),
            vmem((SUBSETS, VIEWS, 2, 8, 128), F32),
            vmem((2 * SUBSETS, HALF, DEEP, NY), BF16),
            vmem((2, HALF, 256, NY), BF16),
            vmem((VIEWS * 128, 512), BF16),
            vmem((VIEWS * 128, 256), BF16),
            vmem((ROWS, VIEWS * 128), F32),
            vmem((ROWS, 256), BF16),
            vmem((2 * ROWS, 512), BF16),
            vmem((2 * ROWS, 256), BF16),
            vmem((OWNERS, 16, 128), F32),
            vmem((xy, 16, 128), F32),
            vmem((SUBSETS, blocks, 8, 128), F32),
            vmem((SUBSETS, GROUPS, VIEWS, 16, 128), F32),
            vmem((SUBSETS, xy, 16, 128), F32),
            vmem((SUBSETS, 2, VIEWS, 8, 128), F32),
            vmem((SUBSETS, xy, 8, 128), F32),
            vmem((SUBSETS, xy, 8, 128), F32),
            vmem((blocks, 8, 128), F32),
            vmem((SUBSETS, xy, 16, 128), BF16),
            vmem((SUBSETS, OWNERS, 16, 128), BF16),
            vmem((SUBSETS, xy, 8, 128), BF16),
            vmem((SUBSETS, 2, VIEWS, 8, 128), BF16),
            vmem((xy, 8, 128), F32),
            vmem((OWNERS, 8, 128), F32),
            vmem((2, DEEP, 128), F32),
            dma(()), dma(()), dma(()), dma(()), dma(()), dma((4,)), dma((2,)), dma((2,)),
            dma((4,)), dma((2,)), dma((2, 2)), dma(()), dma(()),
        ],
        compiler_params=pltpu.CompilerParams(collective_id=0, has_side_effects=True),
    )(view_order, volume.reshape(Z_DEV * X_DEV, NY), measured.transpose(1, 2, 0, 3))
    out, resid = pl.pallas_call(
        put_out,
        out_shape=(
            jax.ShapeDtypeStruct((Z_DEV * X_DEV, NY), F32),
            jax.ShapeDtypeStruct((VIEWS, ROWS_DEV, COLS_DEV), F32),
        ),
        in_specs=[pl.BlockSpec(memory_space=pltpu.VMEM)] * 2,
        out_specs=(pl.BlockSpec(memory_space=pl.ANY),) * 2,
        scratch_shapes=[dma(()), dma(())],
    )(pltpu.with_memory_space_constraint(out, pltpu.VMEM), pltpu.with_memory_space_constraint(resid, pltpu.VMEM))
    return out.reshape(Z_DEV, X_DEV, NY), resid


def put_out(a_ref, b_ref, a_out, b_out, a_sem, b_sem):
    copies = [pltpu.make_async_copy(a_ref, a_out, a_sem), pltpu.make_async_copy(b_ref, b_out, b_sem)]
    for copy in copies:
        copy.start()
    for copy in copies:
        copy.wait()


def solution(mesh):
    in_specs = (P("gz", "xy", None), P(None, None, "gz", "xy"), P())
    out_specs = (P("gz", "xy", None), P(None, "gz", "xy"))
    body = functools.partial(local, mesh.shape["gz"], mesh.shape["xy"])
    return jax.shard_map(body, mesh=mesh, in_specs=in_specs, out_specs=out_specs, check_vma=False)
```

```python
import functools
import math

import jax
import jax.numpy as jnp
from jax import lax
from jax.experimental import pallas as pl
from jax.experimental.pallas import tpu as pltpu
from jax.sharding import PartitionSpec as P

Z_DEV = 16
X_DEV = 48
COLS_DEV = 48
NY = 128
VIEWS = 5
SUBSETS = 2
ANGLES = 48
ROWS_DEV = 20
HALF = X_DEV // 2
WIN = 40
DEEP = 208
GROUPS = 3
SLOTS = 7
SIZES = (7, 7, 6)
OWNERS = VIEWS * GROUPS
SIDE = 4
EDGE = 4
EDGE_SLOT = ROWS_DEV - EDGE - SLOTS * (GROUPS - 1)
ROWS = 16 * GROUPS + 16
MESH = pl.DeviceIdType.MESH
F32 = jnp.float32
BF16 = jnp.bfloat16


def iota(shape, dim):
    return lax.broadcasted_iota(jnp.int32, shape, dim)


def kernel(
    gz, xy, view_hbm, vol_ref, meas_hbm, out_ref, resid_ref,
    views, it, meas, up, ws, shift, trig, weights, data, window, counted, counted_ahead, count_rows, mixer, smearer,
    send_m, recv_m, meas_rows, send_a, recv_a, send_e, recv_e, starts, total, send_c, recv_c, send_f, recv_f,
    send_d, recv_d, turned,
    sem_view, sem_vol, sem_meas, sem_ms, sem_mr, sem_as, sem_ar, sem_ah, sem_cs, sem_cr, sem_ch, sem_ds, sem_dr,
):
    g = lax.axis_index("gz")
    j = lax.axis_index("xy")
    nx_all, ny_all, dc_all = X_DEV * xy, NY, COLS_DEV * xy
    dr_all, nz_all = ROWS_DEV * gz, Z_DEV * gz
    blocks = dc_all // 128
    chip = lax.div(j, 2)
    owner = jnp.logical_and(lax.rem(j, 2) == 1, chip < OWNERS)
    own_view = lax.rem(lax.div(chip, GROUPS), VIEWS)
    own_group = lax.rem(chip, GROUPS)
    first_group = jnp.logical_and(owner, own_group == 0)
    last_group = jnp.logical_and(owner, own_group == GROUPS - 1)
    below, above = g > 0, g < gz - 1
    give_down = jnp.logical_and(first_group, below)
    give_up = jnp.logical_and(last_group, above)
    has_beside = jnp.logical_or(give_down, give_up)

    view_copy = pltpu.make_async_copy(view_hbm, views, sem_view)
    vol_copy = pltpu.make_async_copy(vol_ref, it, sem_vol)
    meas_copy = pltpu.make_async_copy(meas_hbm, meas, sem_meas)
    view_copy.start()
    vol_copy.start()
    meas_copy.start()

    barrier = pltpu.get_barrier_semaphore()

    def greet(plane, device):
        pl.semaphore_signal(barrier, inc=1, device_id=(plane, device), device_id_type=MESH)

    def greet_all(plane):
        for i in range(xy):
            greet(plane, i)

    def next_owner(t):
        return 2 * lax.rem(chip + t, OWNERS) + 1

    def next_device(t):
        return lax.rem(j + t, xy)

    steps = sorted(
        ((a, b, c) for a in range(SIDE) for b in range(SIDE) for c in (1, 0)),
        key=lambda step: -sum(min(d, SIDE - d) for d in step[:2]),
    )

    def moved_chip(a, b):
        return SIDE * lax.rem(lax.div(chip, SIDE) + a, SIDE) + lax.rem(chip + b, SIDE)

    def moved_device(step):
        return 2 * moved_chip(step[0], step[1]) + lax.rem(j + step[2], 2)

    with jax.named_scope("greet"):
        @pl.when(owner)
        def _():
            for t in range(1, xy):
                greet(g, next_device(t))

        @pl.when(jnp.logical_not(owner))
        def _():
            for t in range(OWNERS):
                greet(g, next_owner(t))

        @pl.when(give_down)
        def _():
            greet_all(g - 1)

        @pl.when(jnp.logical_and(below, jnp.logical_not(first_group)))
        def _():
            for v in range(VIEWS):
                greet(g - 1, 2 * (GROUPS * v + GROUPS - 1) + 1)

        @pl.when(give_up)
        def _():
            greet_all(g + 1)

        @pl.when(jnp.logical_and(above, jnp.logical_not(last_group)))
        def _():
            for v in range(VIEWS):
                greet(g + 1, 2 * GROUPS * v + 1)

    greeted = (
        jnp.where(owner, xy - 1, OWNERS)
        + jnp.where(below, jnp.where(first_group, xy, VIEWS), 0)
        + jnp.where(above, jnp.where(last_group, xy, VIEWS), 0)
    )

    lane = iota((8, 128), 1)
    sub = iota((8, 128), 0)
    lane_f = lane.astype(F32)
    sub_f = sub.astype(F32)
    band = lane // 16
    source = 2.0 * nx_all
    scale = 0.9 * (dc_all / nx_all)
    middle = (dc_all - 1) / 2.0
    x_first = (j * X_DEV).astype(F32)

    def project(x, y, cosine, sine):
        along = x * cosine + y * sine
        depth = y * cosine - x * sine
        return middle + scale * along * source / (source + depth)

    def hat(row, slice_id):
        position = (dr_all - 1) / 2.0 + 0.96 * (dr_all / nz_all) * (slice_id - (nz_all - 1) / 2.0)
        return jnp.maximum(0.0, 1.0 - jnp.abs(position - row) / 2.0)

    def rounded(x):
        return x.astype(BF16).astype(F32)

    def in_two(x):
        high = rounded(x)
        return high, x - high

    def geometry(s):
        for v in range(VIEWS):
            number = jnp.full((8, 128), views[s * VIEWS + v], jnp.int32).astype(F32)
            angle = 2.0 * math.pi * number / ANGLES
            cosine, sine = jnp.cos(angle), jnp.sin(angle)
            trig[s, v, 0] = cosine
            trig[s, v, 1] = sine
            y_low = (band * 16).astype(F32) - (ny_all - 1) / 2.0
            x = x_first + (HALF * (sub // 4) + (HALF - 1) * ((sub // 2) % 2)).astype(F32) - (nx_all - 1) / 2.0
            corners = project(x, y_low + (15 * (sub % 2)).astype(F32), cosine, sine)
            lowest = jnp.minimum(corners, pltpu.roll(corners, 7, 0))
            lowest = jnp.minimum(lowest, pltpu.roll(lowest, 6, 0))
            begin = jnp.floor((lowest - 0.03125) * 0.125) * 8.0
            base = []
            for h in range(2):
                start = jnp.broadcast_to(begin[4 * h : 4 * h + 1, :], (8, 128))
                base.append(start)
                shift[s, v, h] = (start - 256.0 * jnp.floor(start * (1.0 / 256.0))).astype(jnp.int32)
            for block in range(X_DEV // 8):
                x = (x_first + (8.0 * block + sub_f)) - (nx_all - 1) / 2.0
                y = lane_f - (ny_all - 1) / 2.0
                u = project(x, y, cosine, sine)
                low = jnp.floor(u)
                first = rounded(jnp.maximum(0.0, 1.0 - jnp.abs(u - low)))
                second = rounded(jnp.maximum(0.0, 1.0 - jnp.abs(u - (low + 1.0))))
                both = first + second
                rows = slice(8 * block, 8 * block + 8)
                up[s, v, rows, :] = u - base[block // (HALF // 8)]
                ws[s, rows, :] = both if v == 0 else ws[s, rows, :] + both

    window_ids = [(sub + 8 * i).astype(F32) for i in range(WIN // 8)]

    def weights_row(s, h, x):
        pieces = []
        for v in range(VIEWS):
            u = jnp.broadcast_to(up[s, v, pl.ds(HALF * h + x, 1), :], (8, 128))
            pieces += [jnp.maximum(0.0, 1.0 - jnp.abs(u - ids)) for ids in window_ids]
        pieces.append(jnp.zeros((DEEP - VIEWS * WIN, 128), F32))
        weights[2 * s + h, x] = jnp.concatenate(pieces, axis=0).astype(BF16)

    def make_weights(s):
        def one(x, carry):
            for h in range(2):
                weights_row(s, h, x)
            return carry

        lax.fori_loop(0, HALF, one, 0, unroll=4)

    in_band = [iota((16, 128), 1) // 16 == q for q in range(8)]

    def spread(values, h, x):
        data[h, x, 0:128, :] = jnp.concatenate([jnp.where(mine, values, 0.0) for mine in in_band], axis=0).astype(BF16)

    def row_tables():
        for h in range(2):
            turned[h, VIEWS * WIN : DEEP, :] = jnp.zeros((DEEP - VIEWS * WIN, 128), F32)
        shape = (ROWS, 128)
        at = iota(shape, 0)
        own = at < 16 * GROUPS
        half = jnp.where(own, (at // 8) % 2, (at // 4) % 2)
        slot = jnp.where(own, at % 8, at % 4)
        edge = jnp.where(at < 16 * GROUPS + 8, -EDGE, ROWS_DEV)
        row = slot + jnp.where(own, SLOTS * (at // 16), edge)
        size = jnp.where(at // 16 == GROUPS - 1, SIZES[-1], SLOTS)
        row_all = g * ROWS_DEV + row
        inside = jnp.logical_and(jnp.logical_and(row_all >= 0, row_all < dr_all), slot < size)
        slice_all = (g * Z_DEV + iota(shape, 1) % 16).astype(F32)
        row_hat = jnp.where(inside, hat(row_all.astype(F32), slice_all), 0.0)
        counts = jnp.where(jnp.logical_and(jnp.logical_and(own, slot == 7), iota(shape, 1) % 16 < 2), 1.0, 0.0)
        for b in range(2):
            mine = half == b
            high, low = in_two(jnp.where(mine, row_hat, 0.0))
            smearer[0:ROWS, 128 * b : 128 * b + 128] = high.astype(BF16)
            smearer[ROWS : 2 * ROWS, 128 * b : 128 * b + 128] = low.astype(BF16)
            for part in range(2):
                columns = slice(256 * b + 128 * part, 256 * b + 128 * part + 128)
                mixer[0:ROWS, columns] = high.astype(BF16)
                mixer[ROWS : 2 * ROWS, columns] = low.astype(BF16)
            count_rows[:, 128 * b : 128 * b + 128] = jnp.where(mine, counts, 0.0).astype(BF16)

    slices = (g * Z_DEV + iota((16, 128), 0)).astype(F32)
    slice_total = jnp.zeros((16, 1), F32)
    for part in range(-(-dr_all // 128)):
        rows = 128 * part + iota((16, 128), 1)
        weight = jnp.where(rows < dr_all, hat(rows.astype(F32), slices), 0.0)
        slice_total = slice_total + jnp.sum(weight, axis=1, keepdims=True)
    slice_total = jnp.broadcast_to(slice_total, (16, 128))
    own_row = (g * ROWS_DEV + own_group * SLOTS + sub).astype(F32)
    ray_row = jnp.zeros((8, 1), F32)
    for part in range(-(-nz_all // 128)):
        ids = 128 * part + lane
        weight = jnp.where(ids < nz_all, hat(own_row, ids.astype(F32)), 0.0)
        ray_row = ray_row + jnp.sum(weight, axis=1, keepdims=True)
    ray_row = jnp.broadcast_to(ray_row, (8, 128))
    own_slot = sub < jnp.where(own_group == GROUPS - 1, SIZES[-1], SLOTS)
    column_ids = [(128 * m + lane).astype(F32) for m in range(blocks)]

    def remote(src, dst, send_sem, recv_sem, plane, device):
        pltpu.make_async_remote_copy(
            src_ref=src, dst_ref=dst, send_sem=send_sem, recv_sem=recv_sem,
            device_id=(plane, device), device_id_type=MESH,
        ).start()

    def arrived(ref, sem):
        pltpu.make_async_copy(ref, ref, sem).wait()

    def to_owners(src, dst, send_sem, recv_sem):
        for a, b, c in steps:
            if c:
                there = moved_chip(a, b)
                wanted = there < OWNERS
                if a == b == 0:
                    wanted = jnp.logical_and(wanted, jnp.logical_not(owner))

                @pl.when(wanted)
                def _():
                    remote(src(there), dst, send_sem, recv_sem, g, 2 * there + 1)

    def with_owners(ref, sem):
        @pl.when(owner)
        def _():
            arrived(ref.at[0 : OWNERS - 1], sem)

        @pl.when(jnp.logical_not(owner))
        def _():
            arrived(ref.at[0:OWNERS], sem)

    def table(x, carry):
        for h in range(2):
            for q in range(8):
                pair = iota((16, 128), 0) < 2
                row = jnp.where(jnp.logical_and(pair, iota((16, 128), 1) // 16 == q), 1.0, 0.0)
                data[h, x, 128 + 16 * q : 128 + 16 * q + 16, :] = row.astype(BF16)
        return carry

    def spread_row(h, x):
        spread(it[pl.ds(HALF * h + x, 16, stride=X_DEV), :], h, x)

    def first_half(x, carry):
        weights_row(0, 0, x)
        spread_row(0, x)
        return carry

    with jax.named_scope("tables"):
        row_tables()
        lax.fori_loop(0, HALF, table, 0, unroll=4)
    view_copy.wait()
    with jax.named_scope("geom0"):
        geometry(0)
    with jax.named_scope("fill"):
        vol_copy.wait()
        lax.fori_loop(0, HALF, first_half, 0, unroll=4)

    with jax.named_scope("measured"):
        meas_copy.wait()
        turn = lax.rem(j * COLS_DEV, 128)
        for v in range(VIEWS):
            for k in range(GROUPS):
                o = GROUPS * v + k
                send_m[o] = jnp.zeros((16, 128), F32)
                for s in range(SUBSETS):
                    for slot in range(SIZES[k]):
                        send_m[o, 8 * s + slot, 0:COLS_DEV] = meas[v, SLOTS * k + slot, s, :]
        for o in range(OWNERS):
            send_m[o] = pltpu.roll(send_m[o], turn, 1)

    def send_measured():
        to_owners(lambda o: send_m.at[o], recv_m.at[j], sem_ms, sem_mr)

        @pl.when(owner)
        def _():
            recv_m[j] = send_m[chip]

    def placed(sums, s, v, part):
        halves = []
        for h in range(2):
            offset = shift[s, v, h]
            rows = [
                sums[h][v * WIN + 8 * i : v * WIN + 8 * i + 8, 128 * part : 128 * part + 128] for i in range(WIN // 8)
            ] + [None] * (32 - WIN // 8)
            for bit in (8, 16, 32, 64, 128):
                moved = (offset & bit) != 0
                step = bit // 8
                new = []
                for i in range(32):
                    old, other = rows[i], rows[(i - step) % 32]
                    if old is None and other is None:
                        new.append(None)
                    elif old is None:
                        new.append(jnp.where(moved, other, 0.0))
                    elif other is None:
                        new.append(jnp.where(moved, 0.0, old))
                    else:
                        new.append(jnp.where(moved, other, old))
                rows = new
            halves.append(rows)
        return [a + b for a, b in zip(*halves)]

    def pairs(pieces):
        for i in range(0, 32, 2):
            yield i // 16, 8 * (i % 16), jnp.concatenate([pieces[i], pieces[i + 1]], axis=0)

    def beside(ref, at, first, count, rows=slice(None)):
        return jnp.concatenate([ref[at, x, rows, :] for x in range(first, first + count)], axis=1)

    def band_sums(s, part, late=()):
        rows = slice(0, 256) if part is None else slice(128 * part, 128 * part + 128)
        sums = []
        for h in range(2):
            sums.append(
                lax.dot_general(
                    beside(weights, 2 * s + h, 0, HALF), beside(data, h, 0, HALF, rows),
                    (((1,), (1,)), ((), ())), preferred_element_type=F32,
                )
            )
            if h == 0:
                for other in late:
                    for x in range(HALF):
                        weights_row(s, other, x)
                        spread_row(other, x)
        return sums

    first_lane = iota((16, 128), 1) % 16 == 0

    def count_columns(s, sums, part):
        for v in range(VIEWS):
            for b, at, value in pairs(placed(sums, s, v, part)):
                high, low = in_two(value)
                counted[128 * v + at : 128 * v + at + 16, 128 * b : 128 * b + 128] = jnp.where(
                    first_lane, high, low
                ).astype(BF16)
        return lax.dot_general(
            count_rows[...], counted[...], (((1,), (1,)), ((), ())), preferred_element_type=F32
        )

    def forward(s, counts):
        with jax.named_scope("f_dot"):
            sums = band_sums(s, None, (1,)) if counts is None else band_sums(s, 0)
        with jax.named_scope("f_place"):
            for v in range(VIEWS):
                for b, at, value in pairs(placed(sums, s, v, 0)):
                    high, low = in_two(value)
                    rows = slice(128 * v + at, 128 * v + at + 16)
                    window[rows, 256 * b : 256 * b + 128] = high.astype(BF16)
                    window[rows, 256 * b + 128 : 256 * b + 256] = low.astype(BF16)
        with jax.named_scope("f_mix"):
            if counts is None:
                counts = count_columns(s, sums, 1)
            mixed = lax.dot_general(
                mixer[...], window[...], (((1,), (1,)), ((), ())), preferred_element_type=F32
            )
            mixed = mixed[0:ROWS] + mixed[ROWS : 2 * ROWS] + counts
            for v in range(VIEWS):
                columns = slice(128 * v, 128 * v + 128)
                for k in range(GROUPS):
                    send_a[s, k, v] = mixed[16 * k : 16 * k + 16, columns]
                for e in range(2):
                    at = 16 * GROUPS + 8 * e
                    send_e[s, e, v] = mixed[at : at + 8, columns]
        if s == 0:
            with jax.named_scope("barrier"):
                pl.semaphore_wait(barrier, greeted)
            with jax.named_scope("send_m"):
                send_measured()
        with jax.named_scope("f_send"):
            for there, plane, e, group in ((below, g - 1, 0, GROUPS - 1), (above, g + 1, 1, 0)):
                @pl.when(there)
                def _():
                    for v in range(VIEWS):
                        remote(
                            send_e.at[s, e, v], recv_e.at[s, j], sem_as.at[2 + s], sem_ah.at[s],
                            plane, 2 * (GROUPS * v + group) + 1,
                        )
            to_owners(
                lambda o: send_a.at[s, lax.rem(o, GROUPS), lax.div(o, GROUPS)],
                recv_a.at[s, j], sem_as.at[s], sem_ar.at[s],
            )

            @pl.when(owner)
            def _():
                recv_a[s, j] = send_a[s, own_group, own_view]

    def prepare_owner():
        arrived(recv_m.at[0 : xy - 1], sem_mr)
        for block in range(blocks):
            first, last = 128 * block, 128 * block + 128
            for s in range(SUBSETS):
                value = jnp.zeros((8, 128), F32)
                for i in range(first // COLS_DEV, min(xy, -(-last // COLS_DEV))):
                    low, high = max(COLS_DEV * i, first) - first, min(COLS_DEV * (i + 1), last) - first
                    piece = recv_m[i, 8 * s : 8 * s + 8, :]
                    value = jnp.where(jnp.logical_and(lane >= low, lane < high), piece, value)
                meas_rows[s, block] = value

    def window_starts(s):
        cosine, sine = trig[s, own_view, 0], trig[s, own_view, 1]

        def one(i, carry):
            x = jnp.full((8, 128), i * X_DEV, jnp.int32).astype(F32) + ((X_DEV - 1) / 2.0 - (nx_all - 1) / 2.0)
            starts[s, i] = jnp.floor(project(x, 0.0, cosine, sine)) - 128.0
            return carry

        lax.fori_loop(0, xy, one, 0)

    def reach(i):
        far = max(abs(X_DEV * i - (nx_all - 1) / 2.0), abs(X_DEV * i + X_DEV - 1 - (nx_all - 1) / 2.0))
        radius = math.hypot(far, (ny_all - 1) / 2.0)
        span = scale * radius / math.sqrt(1.0 - (radius / source) ** 2) + 2.0
        return max(0, int((middle - span) // 128)), min(blocks - 1, int((middle + span) // 128))

    edge_ids = [(256 * m + 128 * (sub // EDGE) + lane).astype(F32) for m in range(blocks // 2)]
    edge_slot = jnp.where(last_group, EDGE_SLOT, 0)

    def within(ids, start):
        return jnp.abs(ids - (start + 127.5)) < 128.0

    def choose(ids, values, candidates, start):
        message = None
        for m in reversed(candidates):
            message = values[m] if message is None else jnp.where(ids[m] >= start, values[m], message)
        return jnp.zeros((8, 128), F32) if message is None else message

    def owner_work(s):
        with jax.named_scope("wait_a"):
            arrived(recv_a.at[s, 0 : xy - 1], sem_ar.at[s])
        with jax.named_scope("o_add"):
            sums = [jnp.zeros((8, 128), F32)] * blocks
            for i in range(xy):
                start = starts[s, i]
                parts = recv_a[s, i, 0:8, :], recv_a[s, i, 8:16, :]
                for m in range(reach(i)[0], reach(i)[1] + 1):
                    sums[m] = sums[m] + jnp.where(within(column_ids[m], start), parts[m % 2], 0.0)
            for m in range(blocks):
                total[m] = sums[m]

        @pl.when(has_beside)
        def _():
            with jax.named_scope("wait_h"):
                arrived(recv_e.at[s], sem_ah.at[s])
            with jax.named_scope("o_addh"):
                sums = [jnp.zeros((8, 128), F32)] * (blocks // 2)
                for i in range(xy):
                    start = starts[s, i]
                    message = recv_e[s, i]
                    for m in range(reach(i)[0] // 2, reach(i)[1] // 2 + 1):
                        sums[m] = sums[m] + jnp.where(within(edge_ids[m], start), message, 0.0)
                for m in range(blocks // 2):
                    low = jnp.where(sub < EDGE, sums[m], 0.0)
                    total[2 * m] = total[2 * m] + pltpu.roll(low, edge_slot, 0)
                    total[2 * m + 1] = total[2 * m + 1] + pltpu.roll(sums[m] - low, edge_slot + EDGE, 0)

        with jax.named_scope("o_give"):
            residuals = []
            for m in range(blocks):
                value = total[m]
                columns = jnp.broadcast_to(value[7:8, :], (8, 128))
                residual = meas_rows[s, m] - value / jnp.maximum(ray_row * columns, 1.0)
                residual = jnp.where(own_slot, residual, 0.0)
                total[m] = residual
                residuals.append(rounded(residual))
            for i in range(xy):
                start = starts[s, i]
                parts = []
                for b in range(2):
                    candidates = [m for m in range(reach(i)[0], reach(i)[1] + 1) if m % 2 == b]
                    parts.append(choose(column_ids, residuals, candidates, start))
                send_c[s, i] = jnp.concatenate(parts, axis=0).astype(BF16)

        @pl.when(has_beside)
        def _():
            with jax.named_scope("o_giveh"):
                back = lax.rem(8 - edge_slot, 8)
                edges = [
                    jnp.where(
                        sub < EDGE,
                        pltpu.roll(rounded(total[2 * m]), back, 0),
                        pltpu.roll(rounded(total[2 * m + 1]), lax.rem(back + EDGE, 8), 0),
                    )
                    for m in range(blocks // 2)
                ]
                for i in range(xy):
                    candidates = list(range(reach(i)[0] // 2, reach(i)[1] // 2 + 1))
                    send_f[s, i] = choose(edge_ids, edges, candidates, starts[s, i]).astype(BF16)
            with jax.named_scope("o_sendh"):
                plane = jnp.where(last_group, g + 1, g - 1)
                slot = jnp.where(last_group, 0, 1)
                for step in steps:
                    i = moved_device(step)
                    remote(
                        send_f.at[s, i], recv_f.at[s, slot, own_view], sem_cs.at[2 + s], sem_ch.at[s, slot], plane, i
                    )

        with jax.named_scope("o_send"):
            for step in steps:
                if step == (0, 0, 0):
                    continue
                i = moved_device(step)
                remote(send_c.at[s, i], recv_c.at[s, chip], sem_cs.at[s], sem_cr.at[s], g, i)
            recv_c[s, chip] = send_c[s, j]

    def owner_give_residual():
        for i in range(xy):
            first = COLS_DEV * i // 128
            message = total[first]
            if first + 1 < blocks:
                message = jnp.where(lane >= COLS_DEV * i % 128, message, total[first + 1])
            send_d[i] = message
        for t in range(1, xy):
            i = next_device(t)
            remote(send_d.at[i], recv_d.at[chip], sem_ds, sem_dr, g, i)
        recv_d[chip] = send_d[j]

    def backward(s):
        @pl.when(jnp.logical_not(below))
        def _():
            recv_f[s, 0] = jnp.zeros((VIEWS, 8, 128), BF16)

        @pl.when(jnp.logical_not(above))
        def _():
            recv_f[s, 1] = jnp.zeros((VIEWS, 8, 128), BF16)

        with jax.named_scope("wait_c"):
            with_owners(recv_c.at[s], sem_cr.at[s])

        with jax.named_scope("wait_ch"):
            @pl.when(below)
            def _():
                arrived(recv_f.at[s, 0], sem_ch.at[s, 0])

            @pl.when(above)
            def _():
                arrived(recv_f.at[s, 1], sem_ch.at[s, 1])

        with jax.named_scope("b_smear"):
            columns = []
            for v in range(VIEWS):
                rows = [recv_c[s, GROUPS * v + k].astype(F32) for k in range(GROUPS)]
                rows = rows + [recv_f[s, e, v].astype(F32) for e in range(2)]
                columns.append(jnp.transpose(jnp.concatenate(rows + rows, axis=0)).astype(BF16))
            smeared = rounded(
                lax.dot_general(
                    jnp.concatenate(columns, axis=0), smearer[...], (((1,), (0,)), ((), ())),
                    preferred_element_type=F32,
                )
            )
            for v in range(VIEWS):
                whole = [
                    smeared[128 * v + 8 * i : 128 * v + 8 * i + 8, 128 * p : 128 * p + 128]
                    for p in range(2)
                    for i in range(16)
                ]
                for h in range(2):
                    offset = shift[s, v, h]
                    now = whole
                    for bit in (128, 64, 32, 16, 8):
                        step = bit // 8
                        moved = (offset & bit) != 0
                        now = [
                            jnp.where(moved, now[(i + step) % 32], now[i]) for i in range(WIN // 8 + step - 1)
                        ]
                    for i in range(WIN // 8):
                        turned[h, v * WIN + 8 * i : v * WIN + 8 * i + 8, :] = now[i]
        with jax.named_scope("b_turn"):
            sides = [jnp.transpose(turned[h]).astype(BF16) for h in range(2)]
        last = s == SUBSETS - 1
        per_step = 2

        bands = jnp.concatenate([band, band], axis=0)

        def one(step, h):
            if True:
                back = lax.dot_general(
                    sides[h], beside(weights, 2 * s + h, per_step * step, per_step), (((1,), (0,)), ((), ())),
                    preferred_element_type=F32,
                )
                for part in range(per_step):
                    x = per_step * step + part
                    mine = back[112:128, 128 * part : 128 * part + 128]
                    for q in range(6, -1, -1):
                        mine = jnp.where(
                            bands == q, back[16 * q : 16 * q + 16, 128 * part : 128 * part + 128], mine
                        )
                    norm = slice_total * ws[s, HALF * h + x : HALF * h + x + 1, :]
                    at = pl.ds(HALF * h + x, 16, stride=X_DEV)
                    new = it[at, :] + mine / jnp.maximum(norm, 1.0)
                    if last:
                        out_ref[at, :] = new
                    else:
                        it[at, :] = new
                        spread(new, h, x)

        with jax.named_scope("b_loop"):
            for h in range(2):
                for step in range(HALF // per_step):
                    one(step, h)

    forward(0, None)

    @pl.when(owner)
    def _():
        with jax.named_scope("prep"):
            prepare_owner()
            window_starts(0)
        owner_work(0)

    with jax.named_scope("gw1"):
        geometry(1)
        make_weights(1)
        counted_ahead[...] = count_columns(1, band_sums(1, 1), 0)

    @pl.when(owner)
    def _():
        window_starts(1)

    backward(0)
    forward(1, counted_ahead[...])

    @pl.when(owner)
    def _():
        owner_work(1)
        with jax.named_scope("give"):
            owner_give_residual()

    backward(1)

    with jax.named_scope("tail"):
        with_owners(recv_d, sem_dr)
        turn_back = lax.rem(128 - lax.rem(j * COLS_DEV, 128), 128)
        for v in range(VIEWS):
            for k in range(GROUPS):
                message = pltpu.roll(recv_d[GROUPS * v + k], turn_back, 1)
                resid_ref[v, SLOTS * k : SLOTS * k + SIZES[k], :] = message[0 : SIZES[k], 0:COLS_DEV]

        with_owners(send_m, sem_ms)
        for s in range(SUBSETS):
            with_owners(recv_a.at[s], sem_as.at[s])

            @pl.when(below)
            def _():
                arrived(send_e.at[s, 0], sem_as.at[2 + s])

            @pl.when(above)
            def _():
                arrived(send_e.at[s, 1], sem_as.at[2 + s])

            @pl.when(owner)
            def _():
                arrived(send_c.at[s, 0 : xy - 1], sem_cs.at[s])

            @pl.when(has_beside)
            def _():
                arrived(send_f.at[s], sem_cs.at[2 + s])

        @pl.when(owner)
        def _():
            arrived(send_d.at[0 : xy - 1], sem_ds)


def local(gz, xy, volume, measured, view_order):
    blocks = COLS_DEV * xy // 128
    dma = pltpu.SemaphoreType.DMA
    vmem = pltpu.VMEM
    out, resid = pl.pallas_call(
        functools.partial(kernel, gz, xy),
        out_shape=(
            pltpu.VMEM((Z_DEV * X_DEV, NY), F32),
            pltpu.VMEM((VIEWS, ROWS_DEV, COLS_DEV), F32),
        ),
        in_specs=[pl.BlockSpec(memory_space=pl.ANY)] * 3,
        out_specs=(pl.BlockSpec(memory_space=pltpu.VMEM), pl.BlockSpec(memory_space=pltpu.VMEM)),
        scratch_shapes=[
            pltpu.SMEM((ANGLES,), jnp.int32),
            vmem((Z_DEV * X_DEV, NY), F32),
            vmem((VIEWS, ROWS_DEV, SUBSETS, COLS_DEV), F32),
            vmem((SUBSETS, VIEWS, X_DEV, NY), F32),
            vmem((SUBSETS, X_DEV, NY), F32),
            vmem((SUBSETS, VIEWS, 2, 8, 128), jnp.int32),
            vmem((SUBSETS, VIEWS, 2, 8, 128), F32),
            vmem((2 * SUBSETS, HALF, DEEP, NY), BF16),
            vmem((2, HALF, 256, NY), BF16),
            vmem((VIEWS * 128, 512), BF16),
            vmem((VIEWS * 128, 256), BF16),
            vmem((ROWS, VIEWS * 128), F32),
            vmem((ROWS, 256), BF16),
            vmem((2 * ROWS, 512), BF16),
            vmem((2 * ROWS, 256), BF16),
            vmem((OWNERS, 16, 128), F32),
            vmem((xy, 16, 128), F32),
            vmem((SUBSETS, blocks, 8, 128), F32),
            vmem((SUBSETS, GROUPS, VIEWS, 16, 128), F32),
            vmem((SUBSETS, xy, 16, 128), F32),
            vmem((SUBSETS, 2, VIEWS, 8, 128), F32),
            vmem((SUBSETS, xy, 8, 128), F32),
            vmem((SUBSETS, xy, 8, 128), F32),
            vmem((blocks, 8, 128), F32),
            vmem((SUBSETS, xy, 16, 128), BF16),
            vmem((SUBSETS, OWNERS, 16, 128), BF16),
            vmem((SUBSETS, xy, 8, 128), BF16),
            vmem((SUBSETS, 2, VIEWS, 8, 128), BF16),
            vmem((xy, 8, 128), F32),
            vmem((OWNERS, 8, 128), F32),
            vmem((2, DEEP, 128), F32),
            dma(()), dma(()), dma(()), dma(()), dma(()), dma((4,)), dma((2,)), dma((2,)),
            dma((4,)), dma((2,)), dma((2, 2)), dma(()), dma(()),
        ],
        compiler_params=pltpu.CompilerParams(collective_id=0, has_side_effects=True),
    )(view_order, volume.reshape(Z_DEV * X_DEV, NY), measured.transpose(1, 2, 0, 3))
    out, resid = pl.pallas_call(
        put_out,
        out_shape=(
            jax.ShapeDtypeStruct((Z_DEV * X_DEV, NY), F32),
            jax.ShapeDtypeStruct((VIEWS, ROWS_DEV, COLS_DEV), F32),
        ),
        in_specs=[pl.BlockSpec(memory_space=pltpu.VMEM)] * 2,
        out_specs=(pl.BlockSpec(memory_space=pl.ANY),) * 2,
        scratch_shapes=[dma(()), dma(())],
    )(pltpu.with_memory_space_constraint(out, pltpu.VMEM), pltpu.with_memory_space_constraint(resid, pltpu.VMEM))
    return out.reshape(Z_DEV, X_DEV, NY), resid


def put_out(a_ref, b_ref, a_out, b_out, a_sem, b_sem):
    copies = [pltpu.make_async_copy(a_ref, a_out, a_sem), pltpu.make_async_copy(b_ref, b_out, b_sem)]
    for copy in copies:
        copy.start()
    for copy in copies:
        copy.wait()


def solution(mesh):
    in_specs = (P("gz", "xy", None), P(None, None, "gz", "xy"), P())
    out_specs = (P("gz", "xy", None), P(None, "gz", "xy"))
    body = functools.partial(local, mesh.shape["gz"], mesh.shape["xy"])
    return jax.shard_map(body, mesh=mesh, in_specs=in_specs, out_specs=out_specs, check_vma=False)
```
